8 devices in a mesh: dp: 1 (over z), tx: 2 (over y), tyz: 4 (over x, core).
Axes of the slice: x: 2, y: 2, z: 1, core: 2. Of those that a mesh axis runs over, the one named last changes fastest.
Arguments:
- hidden: bfloat16 [64, 64, 2048], P('dp', None, ('tx', 'tyz'))
- lengths: int32 [64], P(('dp', 'tx', 'tyz'))
- k_cache: bfloat16 [64, 2048, 128], P(('dp', 'tx', 'tyz'))
- v_cache: bfloat16 [64, 2048, 128], P(('dp', 'tx', 'tyz'))
- ln_gain: float32 [2048], P(('tx', 'tyz'))
- w_query: bfloat16 [2048, 2048], P('tx', 'tyz')
- w_key: bfloat16 [2048, 128], P('tx')
- w_value: bfloat16 [2048, 128], P('tx')
- w_gate: bfloat16 [2048, 8192], P('tx', 'tyz')
- w_up: bfloat16 [2048, 8192], P('tx', 'tyz')
- w_down: bfloat16 [8192, 2048], P('tyz', 'tx')
- w_out: bfloat16 [2048, 2048], P('tyz', 'tx')
Outputs:
- output 1: bfloat16 [64, 64, 2048], P('dp', None, ('tx', 'tyz'))
- output 2: bfloat16 [64, 2048, 128], P(('dp', 'tx', 'tyz'))
- output 3: bfloat16 [64, 2048, 128], P(('dp', 'tx', 'tyz'))
All inputs are finite; a program needn't handle non-finite values.
Results may differ from the reference program's by a relative error of at most 0.00443472.
Values are sent between devices in bfloat16 or wider.
A program may use at most 1 GiB of HBM per device.

```python
import jax
import jax.numpy as jnp
from jax import lax

TOKENS = 64
CACHE = 2048
EMBED = 2048
HEADS = 16
HEAD = 128
FF = 8192
BATCH = 64


def rope_tables(positions):
    half_dim = HEAD // 2
    inv_freq = 10000.0 ** (-2.0 * jnp.arange(half_dim, dtype=jnp.float32) / HEAD)
    angles = positions.astype(jnp.float32)[..., None] * inv_freq
    return jnp.cos(angles), jnp.sin(angles)


def apply_rope(tensor, cos_t, sin_t):
    half_dim = HEAD // 2
    first_half = tensor[..., :half_dim].astype(jnp.float32)
    second_half = tensor[..., half_dim:].astype(jnp.float32)
    rotated = jnp.concatenate([first_half * cos_t - second_half * sin_t, second_half * cos_t + first_half * sin_t], axis=-1)
    return rotated.astype(jnp.bfloat16)


def draw_lengths(len_key):
    len_max = CACHE - TOKENS
    len_low = len_max // 2
    key_base, key_first, key_shift = jax.random.split(len_key, 3)
    drawn_len = jax.random.randint(key_base, (BATCH,), len_low, len_max + 1, dtype=jnp.int32)
    first_row = jax.random.randint(key_first, (), 0, BATCH, dtype=jnp.int32)
    other_row = (first_row + 1 + jax.random.randint(key_shift, (), 0, BATCH - 1, dtype=jnp.int32)) % BATCH
    return drawn_len.at[first_row].set(len_max).at[other_row].set(len_low)


def setup_inputs(seed: int = 0, part: int = 0) -> dict:
    part_key = jax.random.fold_in(jax.random.key(seed), part)
    key_hidden, key_len, key_kc, key_vc = jax.random.split(part_key, 4)
    shared = jax.random.split(jax.random.key(seed + 1), 8)
    q_width = HEADS * HEAD
    hidden = jax.random.normal(key_hidden, (BATCH, TOKENS, EMBED), jnp.float32)
    k_cache = jax.random.normal(key_kc, (BATCH, CACHE, HEAD), jnp.float32)
    v_cache = jax.random.normal(key_vc, (BATCH, CACHE, HEAD), jnp.float32)
    ln_gain = 1.0 + 0.4 * jax.random.normal(shared[0], (EMBED,), jnp.float32)
    w_query = 1.5 * EMBED ** -0.5 * jax.random.normal(shared[1], (EMBED, q_width), jnp.float32)
    w_key = EMBED ** -0.5 * jax.random.normal(shared[2], (EMBED, HEAD), jnp.float32)
    w_value = EMBED ** -0.5 * jax.random.normal(shared[3], (EMBED, HEAD), jnp.float32)
    w_gate = EMBED ** -0.5 * jax.random.normal(shared[4], (EMBED, FF), jnp.float32)
    w_up = EMBED ** -0.5 * jax.random.normal(shared[5], (EMBED, FF), jnp.float32)
    w_down = FF ** -0.5 * jax.random.normal(shared[6], (FF, EMBED), jnp.float32)
    w_out = 0.2 * (CACHE / q_width) ** 0.5 * jax.random.normal(shared[7], (q_width, EMBED), jnp.float32)
    return {
        "hidden": hidden.astype(jnp.bfloat16),
        "lengths": draw_lengths(key_len),
        "k_cache": k_cache.astype(jnp.bfloat16),
        "v_cache": v_cache.astype(jnp.bfloat16),
        "ln_gain": ln_gain,
        "w_query": w_query.astype(jnp.bfloat16),
        "w_key": w_key.astype(jnp.bfloat16),
        "w_value": w_value.astype(jnp.bfloat16),
        "w_gate": w_gate.astype(jnp.bfloat16),
        "w_up": w_up.astype(jnp.bfloat16),
        "w_down": w_down.astype(jnp.bfloat16),
        "w_out": w_out.astype(jnp.bfloat16),
    }


def reference(hidden, lengths, k_cache, v_cache, ln_gain, w_query, w_key, w_value, w_gate, w_up, w_down, w_out):
    def one_row(row_args):
        hidden_row, row_length, k_old, v_old = row_args
        x_f32 = hidden_row.astype(jnp.float32)
        row_mean = jnp.mean(x_f32, axis=-1, keepdims=True)
        row_var = jnp.mean(x_f32 * x_f32, axis=-1, keepdims=True) - row_mean * row_mean
        normed = ((x_f32 - row_mean) * lax.rsqrt(row_var + 1e-6) * ln_gain).astype(jnp.bfloat16)
        gate_proj = jnp.dot(normed, w_gate, preferred_element_type=jnp.float32)
        up_proj = jnp.dot(normed, w_up, preferred_element_type=jnp.float32)
        act_rows = (jax.nn.silu(gate_proj) * up_proj).astype(jnp.bfloat16)
        query_lin = jnp.dot(normed, w_query, preferred_element_type=jnp.float32).astype(jnp.bfloat16).reshape(TOKENS, HEADS, HEAD)
        key_lin = jnp.dot(normed, w_key, preferred_element_type=jnp.float32).astype(jnp.bfloat16)
        value_new = jnp.dot(normed, w_value, preferred_element_type=jnp.float32).astype(jnp.bfloat16)
        positions = row_length + jnp.arange(TOKENS, dtype=jnp.int32)
        cos_t, sin_t = rope_tables(positions)
        query_rot = apply_rope(query_lin, cos_t[:, None, :], sin_t[:, None, :])
        key_rot = apply_rope(key_lin, cos_t, sin_t)
        k_row = lax.dynamic_update_slice_in_dim(k_old, key_rot, row_length, axis=0)
        v_row = lax.dynamic_update_slice_in_dim(v_old, value_new, row_length, axis=0)
        scores = jnp.einsum("chd,jd->chj", query_rot.astype(jnp.float32), k_row.astype(jnp.float32)) * HEAD ** -0.5
        visible = jnp.arange(CACHE, dtype=jnp.int32)[None, None, :] <= positions[:, None, None]
        scores = jnp.where(visible, scores, -1e30)
        prob_rows = jax.nn.softmax(scores, axis=-1).astype(jnp.bfloat16)
        attn_out = jnp.einsum("chj,jd->chd", prob_rows.astype(jnp.float32), v_row.astype(jnp.float32)).astype(jnp.bfloat16)
        mixed_sum = jnp.dot(act_rows, w_down, preferred_element_type=jnp.float32) + jnp.dot(attn_out.reshape(TOKENS, HEADS * HEAD), w_out, preferred_element_type=jnp.float32)
        out_row = (x_f32 + mixed_sum).astype(jnp.bfloat16)
        return out_row, k_row, v_row

    out_rows, k_next, v_next = lax.map(one_row, (hidden, lengths, k_cache, v_cache))
    return out_rows, k_next, v_next
```

```python
import functools

import jax
import jax.numpy as jnp
from jax import lax
from jax.experimental import pallas as pl
from jax.experimental.pallas import tpu as pltpu
from jax.sharding import PartitionSpec as P

LN_EPS = 1e-6
ROPE_BASE = 10000.0
BF16 = jnp.bfloat16
F32 = jnp.float32


def swap(axis, pairs):
    return lambda a: lax.ppermute(a, axis, pairs)


swap_y = swap("tx", [(0, 1), (1, 0)])
swap_x = swap("tyz", [(0, 2), (2, 0), (1, 3), (3, 1)])
swap_c = swap("tyz", [(0, 1), (1, 0), (2, 3), (3, 2)])


def pick(arr, index):
    return lax.dynamic_index_in_dim(arr, index, axis=0, keepdims=False)


def norm_kernel(offs_ref, *refs):
    pieces, gain_ref, out_ref = refs[:8], refs[8], refs[9]
    width = pieces[0].shape[1]
    total = 8 * width
    xs = [p[...].astype(F32) for p in pieces]
    s1 = sum(jnp.sum(v, axis=-1, keepdims=True) for v in xs)
    s2 = sum(jnp.sum(v * v, axis=-1, keepdims=True) for v in xs)
    mean = s1 / total
    var = s2 / total - mean * mean
    inv = lax.rsqrt(var + LN_EPS)
    for i, v in enumerate(xs):
        off = pl.multiple_of(offs_ref[i], width)
        out_ref[:, pl.ds(off, width)] = ((v - mean) * inv * gain_ref[i : i + 1, :]).astype(BF16)


def layer_norm(pieces, gains, offs):
    tokens, width = pieces[0].shape
    blk = 256
    return pl.pallas_call(
        norm_kernel,
        grid_spec=pltpu.PrefetchScalarGridSpec(
            num_scalar_prefetch=1,
            grid=(tokens // blk,),
            in_specs=[pl.BlockSpec((blk, width), lambda i, o: (i, 0))] * 8 + [pl.BlockSpec((8, width), lambda i, o: (0, 0))],
            out_specs=pl.BlockSpec((blk, 8 * width), lambda i, o: (i, 0)),
        ),
        out_shape=jax.ShapeDtypeStruct((tokens, 8 * width), BF16),
        cost_estimate=pl.CostEstimate(flops=20 * tokens * 8 * width, bytes_accessed=32 * tokens * width, transcendentals=tokens),
        name="norm",
    )(offs, *pieces, gains)


def rope(t, cos_t, sin_t):
    t = t.astype(F32)
    return (t * cos_t + pltpu.roll(t, t.shape[-1] // 2, 1) * sin_t).astype(BF16)


def attn_kernel(len_ref, q0, q1, q2, q3, kv_ref, cos_ref, sin_ref, kc_ref, vc_ref, o0, o1, o2, o3, kn_ref, vn_ref, qs):
    new = kv_ref.shape[0]
    cache = kc_ref.shape[1]
    dim = kc_ref.shape[2]
    length = len_ref[pl.program_id(0)]
    cos_t, sin_t = cos_ref[...], sin_ref[...]
    win = new + 32
    kn_ref[...] = kc_ref[...]
    vn_ref[...] = vc_ref[...]
    base = pl.multiple_of(jnp.minimum((length // 16) * 16, cache - win), 16)
    rows = lax.broadcasted_iota(jnp.int32, (win, new), 0) + (base - length)
    hot = (rows == lax.broadcasted_iota(jnp.int32, (win, new), 1)).astype(BF16)
    key_rot = rope(kv_ref[:, :dim], cos_t, sin_t)
    r = lax.broadcasted_iota(jnp.int32, (win, dim), 0) + (base - length)
    fresh = (r >= 0) & (r < new)
    k_win = jnp.dot(hot, key_rot, preferred_element_type=F32)
    v_win = jnp.dot(hot, kv_ref[:, dim:], preferred_element_type=F32)
    sl = pl.ds(base, win)
    kn_ref[0, sl, :] = jnp.where(fresh, k_win, kc_ref[0, sl, :].astype(F32)).astype(BF16)
    vn_ref[0, sl, :] = jnp.where(fresh, v_win, vc_ref[0, sl, :].astype(F32)).astype(BF16)

    q_refs, o_refs = (q0, q1, q2, q3), (o0, o1, o2, o3)
    hpg = q0.shape[1] // dim
    for g in range(4):
        for h in range(hpg):
            qs[g * hpg * new + h * new : g * hpg * new + (h + 1) * new, :] = rope(q_refs[g][:, h * dim : (h + 1) * dim], cos_t, sin_t)

    def attend(keys):
        @pl.loop(0, 4)
        def _(g):
            group = pl.ds(pl.multiple_of(g * hpg * new, hpg * new), hpg * new)
            q = qs[group, :]
            s = lax.dot_general(q, kn_ref[0, :keys, :], (((1,), (1,)), ((), ())), preferred_element_type=F32)
            s = s * (dim ** -0.5)
            tok = lax.broadcasted_iota(jnp.int32, (hpg * new, keys), 0) % new
            pos = lax.broadcasted_iota(jnp.int32, (hpg * new, keys), 1)
            s = jnp.where(pos - tok <= length, s, -1e30)
            e = jnp.exp(s - jnp.max(s, axis=-1, keepdims=True))
            p = (e * (1.0 / jnp.sum(e, axis=-1, keepdims=True))).astype(BF16)
            qs[group, :] = jnp.dot(p, vn_ref[0, :keys, :], preferred_element_type=F32).astype(BF16)

    step = 256
    need = (length + new + step - 1) // step
    sizes = list(range(5, cache // step + 1))
    for n in sizes:
        cond = need <= n if n == sizes[0] else need == n
        pl.when(cond)(functools.partial(attend, n * step))
    for g in range(4):
        for h in range(hpg):
            o_refs[g][:, h * dim : (h + 1) * dim] = qs[(g * hpg + h) * new : (g * hpg + h + 1) * new, :]


def attention(lengths, qs, kv, cos_t, sin_t, k_cache, v_cache):
    rows, cache, dim = k_cache.shape
    new = kv.shape[0] // rows
    qw = qs[0].shape[1]
    tok = lambda w: pl.BlockSpec((new, w), lambda b, L: (b, 0))
    row = pl.BlockSpec((1, cache, dim), lambda b, L: (b, 0, 0))
    heads = 4 * qw // dim
    return pl.pallas_call(
        attn_kernel,
        grid_spec=pltpu.PrefetchScalarGridSpec(
            num_scalar_prefetch=1,
            grid=(rows,),
            in_specs=[tok(qw)] * 4 + [tok(2 * dim), tok(dim), tok(dim), row, row],
            out_specs=[tok(qw)] * 4 + [row, row],
            scratch_shapes=[pltpu.VMEM((heads * new, dim), BF16)],
        ),
        out_shape=[jax.ShapeDtypeStruct((rows * new, qw), BF16)] * 4 + [jax.ShapeDtypeStruct(k_cache.shape, BF16)] * 2,
        cost_estimate=pl.CostEstimate(
            flops=8 * rows * heads * new * cache * dim, bytes_accessed=8 * rows * cache * dim, transcendentals=rows * heads * new * cache
        ),
        name="attn",
    )(lengths, *qs, kv, cos_t, sin_t, k_cache, v_cache)


def solution(mesh):
    def local_layer(hidden, lengths, k_cache, v_cache, ln_gain, w_query, w_key, w_value, w_gate, w_up, w_down, w_out):
        batch, new, width = hidden.shape
        rows_own, cache_len, dim = k_cache.shape
        yi = lax.axis_index("tx")
        ti = lax.axis_index("tyz")
        xi, ci = ti // 2, ti % 2
        half = batch * new // 2
        own_tok = rows_own * new

        g = ln_gain.reshape(1, width)
        g = jnp.concatenate([g, swap_y(g)], 0)
        g = jnp.concatenate([g, swap_x(g)], 0)
        g = jnp.concatenate([g, swap_c(g)], 0)
        hid2 = hidden.reshape(2, half, width)
        mine, other = pick(hid2, yi), pick(hid2, 1 - yi)
        from_y = swap_y(other)
        mine_x = swap_x(mine)
        from_yx = swap_x(from_y)
        near = [mine, from_y, mine_x, from_yx]
        far = [swap_c(p) for p in near]
        offs = []
        for cr in range(2):
            for xr in range(2):
                for yr in range(2):
                    offs.append(width * (4 * yr + 2 * (xr ^ xi) + (cr ^ ci)))
        h = layer_norm(near + far, g, jnp.stack(offs).astype(jnp.int32))

        w_kv = jnp.concatenate([w_key, w_value], axis=1)
        w_kv = jnp.concatenate([w_kv, swap_y(w_kv)], 0)
        w_q = jnp.concatenate([w_query, swap_y(w_query)], 0)

        h_own = lax.dynamic_slice_in_dim(h, ti * own_tok, own_tok, 0)
        kv = jnp.dot(h_own, w_kv, preferred_element_type=F32).astype(BF16)
        q = jnp.dot(h, w_q, preferred_element_type=F32).astype(BF16)

        q4 = q.reshape(2, 2, own_tok, q.shape[1])
        q_x = [pick(q4, xi), swap_x(pick(q4, 1 - xi))]
        q_c = [pick(v, ci) for v in q_x] + [swap_c(pick(v, 1 - ci)) for v in q_x]

        half_dim = dim // 2
        inv_freq = ROPE_BASE ** (-2.0 * jnp.arange(half_dim, dtype=F32) / dim)
        positions = (lengths[:, None] + jnp.arange(new, dtype=jnp.int32)[None, :]).reshape(own_tok)
        angles = positions.astype(F32)[:, None] * inv_freq
        cos_t, sin_t = jnp.cos(angles), jnp.sin(angles)
        cos_t = jnp.concatenate([cos_t, cos_t], -1)
        sin_t = jnp.concatenate([-sin_t, sin_t], -1)
        o0, o1, o2, o3, k_next, v_next = attention(lengths, q_c, kv, cos_t, sin_t, k_cache, v_cache)

        keep = [o0, swap_c(o2)]
        send = swap_x(jnp.stack([o1, swap_c(o3)]))
        flip = lambda pair, i: jnp.where(i == 0, jnp.stack(pair), jnp.stack(pair[::-1]))
        o_rows = flip([flip(keep, ci), jnp.where(ci == 0, send, send[::-1])], xi)
        o_own = o_rows.reshape(half, -1)
        o_oth = swap_c(o_own)

        chunks = 4
        ff = w_gate.shape[1]
        cw = ff // chunks
        a_own, a_oth = [], []
        for j in range(chunks):
            wg, wu = w_gate[:, j * cw : (j + 1) * cw], w_up[:, j * cw : (j + 1) * cw]
            wg = jnp.concatenate([wg, swap_y(wg)], 0)
            wu = jnp.concatenate([wu, swap_y(wu)], 0)
            gate = jnp.dot(h, wg, preferred_element_type=F32)
            up = jnp.dot(h, wu, preferred_element_type=F32)
            act = (jax.nn.silu(gate) * up).astype(BF16)
            a_own.append(act)
            a_oth.append(swap_c(act))
        lhs = jnp.concatenate(a_own + a_oth + [o_own, o_oth], axis=1)

        w_do = jnp.concatenate([w_down, w_out], axis=0).reshape(-1, 2, 2, width)
        w_do = w_do.transpose(1, 2, 0, 3)
        nd = w_down.shape[0]

        def product(cols):
            mine_c, other_c = pick(cols, ci), swap_c(pick(cols, 1 - ci))
            w = jnp.concatenate([mine_c[:nd], other_c[:nd], mine_c[nd:], other_c[nd:]], 0)
            return jnp.dot(lhs, w, preferred_element_type=F32)

        cols_same, cols_cross = pick(w_do, xi), pick(w_do, 1 - xi)
        y_cross = swap_y(cols_cross)
        y_same = swap_y(cols_same)
        r_own = swap_x(product(cols_cross))
        r_oth = swap_x(product(y_cross))
        out_own = (mine.astype(F32) + (product(cols_same) + r_own)).astype(BF16)
        out_oth = (from_y.astype(F32) + (product(y_same) + r_oth)).astype(BF16)
        out_far = swap_y(out_oth)
        out = jnp.where(yi == 0, jnp.stack([out_own, out_far]), jnp.stack([out_far, out_own]))
        return out.reshape(batch, new, width), k_next, v_next

    row_spec = P("dp", None, ("tx", "tyz"))
    batch_spec = P(("dp", "tx", "tyz"), None, None)
    in_specs = (row_spec, P(("dp", "tx", "tyz")), batch_spec, batch_spec, P(("tx", "tyz")), P("tx", "tyz"), P("tx", None), P("tx", None), P("tx", "tyz"), P("tx", "tyz"), P("tyz", "tx"), P("tyz", "tx"))
    out_specs = (row_spec, batch_spec, batch_spec)
    return jax.shard_map(local_layer, mesh=mesh, in_specs=in_specs, out_specs=out_specs, check_vma=False)
```

```python
import functools

import jax
import jax.numpy as jnp
from jax import lax
from jax.experimental import pallas as pl
from jax.experimental.pallas import tpu as pltpu
from jax.sharding import PartitionSpec as P

LN_EPS = 1e-6
ROPE_BASE = 10000.0
BF16 = jnp.bfloat16
F32 = jnp.float32


def swap(axis, pairs):
    return lambda a: lax.ppermute(a, axis, pairs)


swap_y = swap("tx", [(0, 1), (1, 0)])
swap_x = swap("tyz", [(0, 2), (2, 0), (1, 3), (3, 1)])
swap_c = swap("tyz", [(0, 1), (1, 0), (2, 3), (3, 2)])


def pick(arr, index):
    return lax.dynamic_index_in_dim(arr, index, axis=0, keepdims=False)


def norm_kernel(offs_ref, *refs):
    pieces, gain_ref, out_ref = refs[:8], refs[8], refs[9]
    width = pieces[0].shape[1]
    total = 8 * width
    xs = [p[...].astype(F32) for p in pieces]
    s1 = sum(jnp.sum(v, axis=-1, keepdims=True) for v in xs)
    s2 = sum(jnp.sum(v * v, axis=-1, keepdims=True) for v in xs)
    mean = s1 / total
    var = s2 / total - mean * mean
    inv = lax.rsqrt(var + LN_EPS)
    for i, v in enumerate(xs):
        off = pl.multiple_of(offs_ref[i], width)
        out_ref[:, pl.ds(off, width)] = ((v - mean) * inv * gain_ref[i : i + 1, :]).astype(BF16)


def layer_norm(pieces, gains, offs):
    tokens, width = pieces[0].shape
    blk = 256
    return pl.pallas_call(
        norm_kernel,
        grid_spec=pltpu.PrefetchScalarGridSpec(
            num_scalar_prefetch=1,
            grid=(tokens // blk,),
            in_specs=[pl.BlockSpec((blk, width), lambda i, o: (i, 0))] * 8 + [pl.BlockSpec((8, width), lambda i, o: (0, 0))],
            out_specs=pl.BlockSpec((blk, 8 * width), lambda i, o: (i, 0)),
        ),
        out_shape=jax.ShapeDtypeStruct((tokens, 8 * width), BF16),
        cost_estimate=pl.CostEstimate(flops=20 * tokens * 8 * width, bytes_accessed=32 * tokens * width, transcendentals=tokens),
        name="norm",
    )(offs, *pieces, gains)


def rope(t, cos_t, sin_t):
    t = t.astype(F32)
    return (t * cos_t + pltpu.roll(t, t.shape[-1] // 2, 1) * sin_t).astype(BF16)


def attn_kernel(len_ref, q0, q1, q2, q3, kv_ref, cos_ref, sin_ref, kc_ref, vc_ref, o0, o1, o2, o3, kn_ref, vn_ref, qs):
    new = kv_ref.shape[0]
    cache = kc_ref.shape[1]
    dim = kc_ref.shape[2]
    length = len_ref[pl.program_id(0)]
    cos_t, sin_t = cos_ref[...], sin_ref[...]
    win = new + 32
    kn_ref[...] = kc_ref[...]
    vn_ref[...] = vc_ref[...]
    base = pl.multiple_of(jnp.minimum((length // 16) * 16, cache - win), 16)
    rows = lax.broadcasted_iota(jnp.int32, (win, new), 0) + (base - length)
    hot = (rows == lax.broadcasted_iota(jnp.int32, (win, new), 1)).astype(BF16)
    key_rot = rope(kv_ref[:, :dim], cos_t, sin_t)
    r = lax.broadcasted_iota(jnp.int32, (win, dim), 0) + (base - length)
    fresh = (r >= 0) & (r < new)
    k_win = jnp.dot(hot, key_rot, preferred_element_type=F32)
    v_win = jnp.dot(hot, kv_ref[:, dim:], preferred_element_type=F32)
    sl = pl.ds(base, win)
    kn_ref[0, sl, :] = jnp.where(fresh, k_win, kc_ref[0, sl, :].astype(F32)).astype(BF16)
    vn_ref[0, sl, :] = jnp.where(fresh, v_win, vc_ref[0, sl, :].astype(F32)).astype(BF16)

    q_refs, o_refs = (q0, q1, q2, q3), (o0, o1, o2, o3)
    hpg = q0.shape[1] // dim
    for g in range(4):
        for h in range(hpg):
            qs[g * hpg * new + h * new : g * hpg * new + (h + 1) * new, :] = rope(q_refs[g][:, h * dim : (h + 1) * dim], cos_t, sin_t)

    def attend(keys):
        @pl.loop(0, 4)
        def _(g):
            group = pl.ds(pl.multiple_of(g * hpg * new, hpg * new), hpg * new)
            q = qs[group, :]
            s = lax.dot_general(q, kn_ref[0, :keys, :], (((1,), (1,)), ((), ())), preferred_element_type=F32)
            s = s * (dim ** -0.5)
            tok = lax.broadcasted_iota(jnp.int32, (hpg * new, keys), 0) % new
            pos = lax.broadcasted_iota(jnp.int32, (hpg * new, keys), 1)
            s = jnp.where(pos - tok <= length, s, -1e30)
            e = jnp.exp(s - jnp.max(s, axis=-1, keepdims=True))
            p = (e * (1.0 / jnp.sum(e, axis=-1, keepdims=True))).astype(BF16)
            qs[group, :] = jnp.dot(p, vn_ref[0, :keys, :], preferred_element_type=F32).astype(BF16)

    step = 256
    need = (length + new + step - 1) // step
    sizes = list(range(5, cache // step + 1))
    for n in sizes:
        cond = need <= n if n == sizes[0] else need == n
        pl.when(cond)(functools.partial(attend, n * step))
    for g in range(4):
        for h in range(hpg):
            o_refs[g][:, h * dim : (h + 1) * dim] = qs[(g * hpg + h) * new : (g * hpg + h + 1) * new, :]


def attention(lengths, qs, kv, cos_t, sin_t, k_cache, v_cache):
    rows, cache, dim = k_cache.shape
    new = kv.shape[0] // rows
    qw = qs[0].shape[1]
    tok = lambda w: pl.BlockSpec((new, w), lambda b, L: (b, 0))
    row = pl.BlockSpec((1, cache, dim), lambda b, L: (b, 0, 0))
    heads = 4 * qw // dim
    return pl.pallas_call(
        attn_kernel,
        grid_spec=pltpu.PrefetchScalarGridSpec(
            num_scalar_prefetch=1,
            grid=(rows,),
            in_specs=[tok(qw)] * 4 + [tok(2 * dim), tok(dim), tok(dim), row, row],
            out_specs=[tok(qw)] * 4 + [row, row],
            scratch_shapes=[pltpu.VMEM((heads * new, dim), BF16)],
        ),
        out_shape=[jax.ShapeDtypeStruct((rows * new, qw), BF16)] * 4 + [jax.ShapeDtypeStruct(k_cache.shape, BF16)] * 2,
        cost_estimate=pl.CostEstimate(
            flops=8 * rows * heads * new * cache * dim, bytes_accessed=8 * rows * cache * dim, transcendentals=rows * heads * new * cache
        ),
        name="attn",
    )(lengths, *qs, kv, cos_t, sin_t, k_cache, v_cache)


def glu_kernel(h_ref, go, gf, uo, uf, a_ref):
    depth = go.shape[0]
    near, far = h_ref[:, :depth], h_ref[:, depth:]
    gate = jnp.dot(near, go[...], preferred_element_type=F32) + jnp.dot(far, gf[...], preferred_element_type=F32)
    up = jnp.dot(near, uo[...], preferred_element_type=F32) + jnp.dot(far, uf[...], preferred_element_type=F32)
    a_ref[...] = (gate / (1.0 + jnp.exp(-gate)) * up).astype(BF16)


def glu(h, go, gf, uo, uf):
    tokens, depth = h.shape
    cols = go.shape[1]
    blk = 512
    w = pl.BlockSpec((depth // 2, cols), lambda i: (0, 0))
    return pl.pallas_call(
        glu_kernel,
        grid=(tokens // blk,),
        in_specs=[pl.BlockSpec((blk, depth), lambda i: (i, 0)), w, w, w, w],
        out_specs=pl.BlockSpec((blk, cols), lambda i: (i, 0)),
        out_shape=jax.ShapeDtypeStruct((tokens, cols), BF16),
        cost_estimate=pl.CostEstimate(flops=4 * tokens * depth * cols, bytes_accessed=2 * tokens * (depth + cols) + 4 * depth * cols, transcendentals=tokens * cols),
        name="glu",
    )(h, go, gf, uo, uf)


def mix_kernel(n_lhs, n_w, n_add, *refs):
    lhs, ws, adds, out_ref = refs[:n_lhs], refs[n_lhs : n_lhs + n_w], refs[n_lhs + n_w : n_lhs + n_w + n_add], refs[-1]
    total = None
    i, row = 0, 0
    for l in lhs:
        k = l.shape[1]
        part = jnp.dot(l[...], ws[i][row : row + k, :], preferred_element_type=F32)
        total = part if total is None else total + part
        row += k
        if row == ws[i].shape[0]:
            i, row = i + 1, 0
    for t in adds:
        total = total + t[...].astype(F32)
    out_ref[...] = total.astype(out_ref.dtype)


def mix(lhs, ws, adds=(), dtype=F32, start=0, tokens=None):
    tokens = lhs[0].shape[0] if tokens is None else tokens
    cols = ws[0].shape[1]
    blk = 256
    first = start // blk
    tok = lambda w: pl.BlockSpec((blk, w), lambda i: (i + first, 0))
    depth = sum(l.shape[1] for l in lhs)
    add_specs = [tok(cols) if t.shape[0] != tokens else pl.BlockSpec((blk, cols), lambda i: (i, 0)) for t in adds]
    return pl.pallas_call(
        functools.partial(mix_kernel, len(lhs), len(ws), len(adds)),
        grid=(tokens // blk,),
        in_specs=[tok(l.shape[1]) for l in lhs] + [pl.BlockSpec(w.shape, lambda i: (0, 0)) for w in ws] + add_specs,
        out_specs=pl.BlockSpec((blk, cols), lambda i: (i, 0)),
        out_shape=jax.ShapeDtypeStruct((tokens, cols), dtype),
        cost_estimate=pl.CostEstimate(flops=2 * tokens * depth * cols, bytes_accessed=2 * depth * (tokens + cols), transcendentals=0),
        name="mix",
    )(*lhs, *ws, *adds)


def tie(value, *others):
    return lax.optimization_barrier((value, *others))[0]


def solution(mesh):
    def local_layer(hidden, lengths, k_cache, v_cache, ln_gain, w_query, w_key, w_value, w_gate, w_up, w_down, w_out):
        batch, new, width = hidden.shape
        rows_own, cache_len, dim = k_cache.shape
        yi = lax.axis_index("tx")
        ti = lax.axis_index("tyz")
        xi, ci = ti // 2, ti % 2
        half = batch * new // 2
        own_tok = rows_own * new

        g = ln_gain.reshape(1, width)
        g = jnp.concatenate([g, swap_y(g)], 0)
        g = jnp.concatenate([g, swap_x(g)], 0)
        g = jnp.concatenate([g, swap_c(g)], 0)
        hid2 = hidden.reshape(2, half, width)
        mine, other = pick(hid2, yi), pick(hid2, 1 - yi)
        from_y = swap_y(other)
        mine_x = swap_x(mine)
        from_yx = swap_x(from_y)
        near = [mine, from_y, mine_x, from_yx]
        far = [swap_c(p) for p in near]
        offs = []
        for cr in range(2):
            for xr in range(2):
                for yr in range(2):
                    offs.append(width * (4 * yr + 2 * (xr ^ xi) + (cr ^ ci)))
        h = layer_norm(near + far, g, jnp.stack(offs).astype(jnp.int32))

        kv_rows = w_key.shape[0] // 2
        w_kv = jnp.concatenate([w_key, w_value], axis=1)
        kv_part = swap_y(lax.dynamic_slice_in_dim(w_kv, ci * kv_rows, kv_rows, 0))
        kv_pair = jnp.stack([kv_part, swap_c(kv_part)])
        kv_far = jnp.where(ci == 0, kv_pair, kv_pair[::-1]).reshape(w_kv.shape)
        q_far = swap_y(w_query)
        depth = w_query.shape[0]

        q = mix([h], [jnp.concatenate([w_query, q_far], 0)], dtype=BF16)
        h_own = lax.dynamic_slice_in_dim(h, ti * own_tok, own_tok, 0)
        kv = jnp.dot(h_own, jnp.concatenate([w_kv, kv_far], 0), preferred_element_type=F32).astype(BF16)

        q4 = q.reshape(2, 2, own_tok, q.shape[1])
        q_x = [pick(q4, xi), swap_x(pick(q4, 1 - xi))]
        q_c = [pick(v, ci) for v in q_x] + [swap_c(pick(v, 1 - ci)) for v in q_x]

        half_dim = dim // 2
        inv_freq = ROPE_BASE ** (-2.0 * jnp.arange(half_dim, dtype=F32) / dim)
        positions = (lengths[:, None] + jnp.arange(new, dtype=jnp.int32)[None, :]).reshape(own_tok)
        angles = positions.astype(F32)[:, None] * inv_freq
        cos_t, sin_t = jnp.cos(angles), jnp.sin(angles)
        cos_t = jnp.concatenate([cos_t, cos_t], -1)
        sin_t = jnp.concatenate([-sin_t, sin_t], -1)
        o0, o1, o2, o3, k_next, v_next = attention(lengths, q_c, kv, cos_t, sin_t, k_cache, v_cache)

        keep = [o0, swap_c(o2)]
        send = swap_x(jnp.stack([o1, swap_c(o3)]))
        flip = lambda pair, i: jnp.where(i == 0, jnp.stack(pair), jnp.stack(pair[::-1]))
        o_rows = flip([flip(keep, ci), jnp.where(ci == 0, send, send[::-1])], xi)
        o_own = o_rows.reshape(half, -1)
        o_far = swap_c(o_own)

        chunks = 4
        cw = w_gate.shape[1] // chunks
        gates = [from_y, h, q, o0]
        a_own, a_far = [], []
        for j in range(chunks):
            wg, wu = (tie(w[:, j * cw : (j + 1) * cw], gates[j]) for w in (w_gate, w_up))
            gf, uf = swap_y(wg), swap_y(wu)
            if j == 0:
                gf = tie(gf, o0)
            a_own.append(glu(h, wg, gf, wu, uf))
            a_far.append(swap_c(a_own[-1]))
        lhs = a_own + a_far + [o_own, o_far]

        def cols_of(w, i, n):
            return lax.dynamic_slice_in_dim(w, i * n, n, 1)

        def both_cores(pair):
            mine_c = [cols_of(w, ci, width) for w in pair]
            far_c = [swap_c(cols_of(w, 1 - ci, width)) for w in pair]
            return [mine_c[0], far_c[0], mine_c[1], far_c[1]]

        own_w = tie(w_down, q), tie(w_out, q)
        same = [cols_of(w, xi, 2 * width) for w in own_w]
        cross = [cols_of(w, 1 - xi, 2 * width) for w in own_w]
        y_cross = [swap_y(tie(w, a_own[0])) for w in cross]
        y_same = [swap_y(tie(w, a_own[1])) for w in same]
        w_cross, w_same = both_cores(cross), both_cores(same)
        p_own = mix(lhs, w_cross)
        r_own = swap_x(p_own)
        out_own = mix(lhs, [tie(w_same[0], p_own), *w_same[1:]], [mine, r_own], BF16)
        p_far = mix(lhs, both_cores([tie(w, p_own) for w in y_cross]))
        r_far = swap_x(p_far)
        w_last = both_cores([tie(w, p_far) for w in y_same])
        parts = 2
        size = half // parts
        out_far = []
        for i in range(parts):
            out_far.append(swap_y(mix(lhs, w_last, [from_y, r_far], BF16, i * size, size)))
        out_far = jnp.concatenate(out_far, 0)
        out = jnp.where(yi == 0, jnp.stack([out_own, out_far]), jnp.stack([out_far, out_own]))
        return out.reshape(batch, new, width), k_next, v_next

    row_spec = P("dp", None, ("tx", "tyz"))
    batch_spec = P(("dp", "tx", "tyz"), None, None)
    in_specs = (row_spec, P(("dp", "tx", "tyz")), batch_spec, batch_spec, P(("tx", "tyz")), P("tx", "tyz"), P("tx", None), P("tx", None), P("tx", "tyz"), P("tx", "tyz"), P("tyz", "tx"), P("tyz", "tx"))
    out_specs = (row_spec, batch_spec, batch_spec)
    return jax.shard_map(local_layer, mesh=mesh, in_specs=in_specs, out_specs=out_specs, check_vma=False)
```

```python
import functools

import jax
import jax.numpy as jnp
from jax import lax
from jax.experimental import pallas as pl
from jax.experimental.pallas import tpu as pltpu
from jax.sharding import PartitionSpec as P

LN_EPS = 1e-6
ROPE_BASE = 10000.0
BF16 = jnp.bfloat16
F32 = jnp.float32


def swap(axis, pairs):
    return lambda a: lax.ppermute(a, axis, pairs)


swap_y = swap("tx", [(0, 1), (1, 0)])
swap_x = swap("tyz", [(0, 2), (2, 0), (1, 3), (3, 1)])
swap_c = swap("tyz", [(0, 1), (1, 0), (2, 3), (3, 2)])


def pick(arr, index):
    return lax.dynamic_index_in_dim(arr, index, axis=0, keepdims=False)


def norm_kernel(offs_ref, *refs):
    pieces, gain_ref, out_ref = refs[:8], refs[8], refs[9]
    width = pieces[0].shape[1]
    total = 8 * width
    xs = [p[...].astype(F32) for p in pieces]
    s1 = sum(jnp.sum(v, axis=-1, keepdims=True) for v in xs)
    s2 = sum(jnp.sum(v * v, axis=-1, keepdims=True) for v in xs)
    mean = s1 / total
    var = s2 / total - mean * mean
    inv = lax.rsqrt(var + LN_EPS)
    for i, v in enumerate(xs):
        off = pl.multiple_of(offs_ref[i], width)
        out_ref[:, pl.ds(off, width)] = ((v - mean) * inv * gain_ref[i : i + 1, :]).astype(BF16)


def layer_norm(pieces, gains, offs):
    tokens, width = pieces[0].shape
    blk = 256
    return pl.pallas_call(
        norm_kernel,
        grid_spec=pltpu.PrefetchScalarGridSpec(
            num_scalar_prefetch=1,
            grid=(tokens // blk,),
            in_specs=[pl.BlockSpec((blk, width), lambda i, o: (i, 0))] * 8 + [pl.BlockSpec((8, width), lambda i, o: (0, 0))],
            out_specs=pl.BlockSpec((blk, 8 * width), lambda i, o: (i, 0)),
        ),
        out_shape=jax.ShapeDtypeStruct((tokens, 8 * width), BF16),
        cost_estimate=pl.CostEstimate(flops=20 * tokens * 8 * width, bytes_accessed=32 * tokens * width, transcendentals=tokens),
        name="norm",
    )(offs, *pieces, gains)


def rope(t, cos_t, sin_t):
    t = t.astype(F32)
    return (t * cos_t + pltpu.roll(t, t.shape[-1] // 2, 1) * sin_t).astype(BF16)


def attn_kernel(len_ref, q0, q1, q2, q3, kv_ref, cos_ref, sin_ref, kc_ref, vc_ref, o0, o1, o2, o3, kn_ref, vn_ref, qs):
    new = kv_ref.shape[0]
    cache = kc_ref.shape[1]
    dim = kc_ref.shape[2]
    length = len_ref[pl.program_id(0)]
    cos_t, sin_t = cos_ref[...], sin_ref[...]
    win = new + 32
    kn_ref[...] = kc_ref[...]
    vn_ref[...] = vc_ref[...]
    base = pl.multiple_of(jnp.minimum((length // 16) * 16, cache - win), 16)
    rows = lax.broadcasted_iota(jnp.int32, (win, new), 0) + (base - length)
    hot = (rows == lax.broadcasted_iota(jnp.int32, (win, new), 1)).astype(BF16)
    key_rot = rope(kv_ref[:, :dim], cos_t, sin_t)
    r = lax.broadcasted_iota(jnp.int32, (win, dim), 0) + (base - length)
    fresh = (r >= 0) & (r < new)
    k_win = jnp.dot(hot, key_rot, preferred_element_type=F32)
    v_win = jnp.dot(hot, kv_ref[:, dim:], preferred_element_type=F32)
    sl = pl.ds(base, win)
    kn_ref[0, sl, :] = jnp.where(fresh, k_win, kc_ref[0, sl, :].astype(F32)).astype(BF16)
    vn_ref[0, sl, :] = jnp.where(fresh, v_win, vc_ref[0, sl, :].astype(F32)).astype(BF16)

    q_refs, o_refs = (q0, q1, q2, q3), (o0, o1, o2, o3)
    hpg = q0.shape[1] // dim
    for g in range(4):
        for h in range(hpg):
            qs[g * hpg * new + h * new : g * hpg * new + (h + 1) * new, :] = rope(q_refs[g][:, h * dim : (h + 1) * dim], cos_t, sin_t)

    def attend(keys):
        @pl.loop(0, 4)
        def _(g):
            group = pl.ds(pl.multiple_of(g * hpg * new, hpg * new), hpg * new)
            q = qs[group, :]
            s = lax.dot_general(q, kn_ref[0, :keys, :], (((1,), (1,)), ((), ())), preferred_element_type=F32)
            s = s * (dim ** -0.5)
            tok = lax.broadcasted_iota(jnp.int32, (hpg * new, keys), 0) % new
            pos = lax.broadcasted_iota(jnp.int32, (hpg * new, keys), 1)
            s = jnp.where(pos - tok <= length, s, -1e30)
            e = jnp.exp(s - jnp.max(s, axis=-1, keepdims=True))
            p = (e * (1.0 / jnp.sum(e, axis=-1, keepdims=True))).astype(BF16)
            qs[group, :] = jnp.dot(p, vn_ref[0, :keys, :], preferred_element_type=F32).astype(BF16)

    step = 256
    need = (length + new + step - 1) // step
    sizes = list(range(5, cache // step + 1))
    for n in sizes:
        cond = need <= n if n == sizes[0] else need == n
        pl.when(cond)(functools.partial(attend, n * step))
    for g in range(4):
        for h in range(hpg):
            o_refs[g][:, h * dim : (h + 1) * dim] = qs[(g * hpg + h) * new : (g * hpg + h + 1) * new, :]


def attention(lengths, qs, kv, cos_t, sin_t, k_cache, v_cache):
    rows, cache, dim = k_cache.shape
    new = kv.shape[0] // rows
    qw = qs[0].shape[1]
    tok = lambda w: pl.BlockSpec((new, w), lambda b, L: (b, 0))
    row = pl.BlockSpec((1, cache, dim), lambda b, L: (b, 0, 0))
    heads = 4 * qw // dim
    return pl.pallas_call(
        attn_kernel,
        grid_spec=pltpu.PrefetchScalarGridSpec(
            num_scalar_prefetch=1,
            grid=(rows,),
            in_specs=[tok(qw)] * 4 + [tok(2 * dim), tok(dim), tok(dim), row, row],
            out_specs=[tok(qw)] * 4 + [row, row],
            scratch_shapes=[pltpu.VMEM((heads * new, dim), BF16)],
        ),
        out_shape=[jax.ShapeDtypeStruct((rows * new, qw), BF16)] * 4 + [jax.ShapeDtypeStruct(k_cache.shape, BF16)] * 2,
        cost_estimate=pl.CostEstimate(
            flops=8 * rows * heads * new * cache * dim, bytes_accessed=8 * rows * cache * dim, transcendentals=rows * heads * new * cache
        ),
        name="attn",
    )(lengths, *qs, kv, cos_t, sin_t, k_cache, v_cache)


def glu_kernel(h_ref, near_w, far_w, a_ref):
    depth = near_w.shape[1]
    near, far = h_ref[:, :depth], h_ref[:, depth:]
    gate = jnp.dot(near, near_w[0], preferred_element_type=F32) + jnp.dot(far, far_w[0], preferred_element_type=F32)
    up = jnp.dot(near, near_w[1], preferred_element_type=F32) + jnp.dot(far, far_w[1], preferred_element_type=F32)
    a_ref[...] = (gate / (1.0 + jnp.exp(-gate)) * up).astype(BF16)


def glu(h, near_w, far_w):
    tokens, depth = h.shape
    cols = near_w.shape[2]
    blk = 512
    w = pl.BlockSpec(near_w.shape, lambda i: (0, 0, 0))
    return pl.pallas_call(
        glu_kernel,
        grid=(tokens // blk,),
        in_specs=[pl.BlockSpec((blk, depth), lambda i: (i, 0)), w, w],
        out_specs=pl.BlockSpec((blk, cols), lambda i: (i, 0)),
        out_shape=jax.ShapeDtypeStruct((tokens, cols), BF16),
        cost_estimate=pl.CostEstimate(flops=4 * tokens * depth * cols, bytes_accessed=2 * tokens * (depth + cols) + 4 * depth * cols, transcendentals=tokens * cols),
        name="glu",
    )(h, near_w, far_w)


def mix_kernel(n_lhs, n_w, n_add, *refs):
    lhs, ws, adds, out_ref = refs[:n_lhs], refs[n_lhs : n_lhs + n_w], refs[n_lhs + n_w : n_lhs + n_w + n_add], refs[-1]
    total = None
    i, row = 0, 0
    for l in lhs:
        k = l.shape[1]
        part = jnp.dot(l[...], ws[i][row : row + k, :], preferred_element_type=F32)
        total = part if total is None else total + part
        row += k
        if row == ws[i].shape[0]:
            i, row = i + 1, 0
    for t in adds:
        total = total + t[...].astype(F32)
    out_ref[...] = total.astype(out_ref.dtype)


def mix(lhs, ws, adds=(), dtype=F32, start=0, tokens=None):
    tokens = lhs[0].shape[0] if tokens is None else tokens
    cols = ws[0].shape[1]
    blk = 512
    first = start // blk
    tok = lambda w: pl.BlockSpec((blk, w), lambda i: (i + first, 0))
    depth = sum(l.shape[1] for l in lhs)
    add_specs = [tok(cols) if t.shape[0] != tokens else pl.BlockSpec((blk, cols), lambda i: (i, 0)) for t in adds]
    return pl.pallas_call(
        functools.partial(mix_kernel, len(lhs), len(ws), len(adds)),
        grid=(tokens // blk,),
        in_specs=[tok(l.shape[1]) for l in lhs] + [pl.BlockSpec(w.shape, lambda i: (0, 0)) for w in ws] + add_specs,
        out_specs=pl.BlockSpec((blk, cols), lambda i: (i, 0)),
        out_shape=jax.ShapeDtypeStruct((tokens, cols), dtype),
        cost_estimate=pl.CostEstimate(flops=2 * tokens * depth * cols, bytes_accessed=2 * depth * (tokens + cols), transcendentals=0),
        name="mix",
    )(*lhs, *ws, *adds)


BLOCK_ORDER = [(1, 1), (1, 0), (0, 1), (0, 0)]


def tie(value, *others):
    return lax.optimization_barrier((value, *others))[0]


def solution(mesh):
    def local_layer(hidden, lengths, k_cache, v_cache, ln_gain, w_query, w_key, w_value, w_gate, w_up, w_down, w_out):
        batch, new, width = hidden.shape
        rows_own, _, dim = k_cache.shape
        yi = lax.axis_index("tx")
        ti = lax.axis_index("tyz")
        xi, ci = ti // 2, ti % 2
        half = batch * new // 2
        own_tok = rows_own * new

        g = ln_gain.reshape(1, width)
        g = jnp.concatenate([g, swap_y(g)], 0)
        g = jnp.concatenate([g, swap_x(g)], 0)
        g = jnp.concatenate([g, swap_c(g)], 0)
        hid2 = hidden.reshape(2, half, width)
        mine, other = pick(hid2, yi), pick(hid2, 1 - yi)
        from_y = swap_y(other)
        mine_x = swap_x(mine)
        from_yx = swap_x(from_y)
        near = [mine, from_y, mine_x, from_yx]
        far = [swap_c(p) for p in near]
        offs = []
        for cr in range(2):
            for xr in range(2):
                for yr in range(2):
                    offs.append(width * (4 * yr + 2 * (xr ^ xi) + (cr ^ ci)))
        h = layer_norm(near + far, g, jnp.stack(offs).astype(jnp.int32))

        kv_rows = w_key.shape[0] // 2
        w_kv = jnp.concatenate([w_key, w_value], axis=1)
        kv_part = swap_y(lax.dynamic_slice_in_dim(w_kv, ci * kv_rows, kv_rows, 0))
        kv_pair = jnp.stack([kv_part, swap_c(kv_part)])
        kv_far = jnp.where(ci == 0, kv_pair, kv_pair[::-1]).reshape(w_kv.shape)
        q_far = swap_y(w_query)

        q = mix([h], [jnp.concatenate([w_query, q_far], 0)], dtype=BF16)
        h_own = lax.dynamic_slice_in_dim(h, ti * own_tok, own_tok, 0)
        kv = jnp.dot(h_own, jnp.concatenate([w_kv, kv_far], 0), preferred_element_type=F32).astype(BF16)

        q4 = q.reshape(2, 2, own_tok, q.shape[1])
        q_x = [pick(q4, xi), swap_x(pick(q4, 1 - xi))]
        q_c = [pick(v, ci) for v in q_x] + [swap_c(pick(v, 1 - ci)) for v in q_x]

        half_dim = dim // 2
        inv_freq = ROPE_BASE ** (-2.0 * jnp.arange(half_dim, dtype=F32) / dim)
        positions = (lengths[:, None] + jnp.arange(new, dtype=jnp.int32)[None, :]).reshape(own_tok)
        angles = positions.astype(F32)[:, None] * inv_freq
        cos_t, sin_t = jnp.cos(angles), jnp.sin(angles)
        cos_t = jnp.concatenate([cos_t, cos_t], -1)
        sin_t = jnp.concatenate([-sin_t, sin_t], -1)
        o0, o1, o2, o3, k_next, v_next = attention(lengths, q_c, kv, cos_t, sin_t, k_cache, v_cache)

        keep = [o0, swap_c(o2)]
        send = swap_x(jnp.stack([o1, swap_c(o3)]))
        flip = lambda pair, i: jnp.where(i == 0, jnp.stack(pair), jnp.stack(pair[::-1]))
        o_rows = flip([flip(keep, ci), jnp.where(ci == 0, send, send[::-1])], xi)
        o_own = o_rows.reshape(half, -1)
        o_far = swap_c(o_own)

        chunks = 4
        cw = w_gate.shape[1] // chunks
        a_own, a_far = [], []
        for j in range(chunks):
            near_w = jnp.stack([w[:, j * cw : (j + 1) * cw] for w in (w_gate, w_up)])
            far_w = swap_y(near_w)
            if j > 0:
                far_w = tie(far_w, a_own[-1], o0)
            a_own.append(glu(h, near_w, far_w))
            a_far.append(swap_c(a_own[-1]))
        lhs_near, lhs_far = a_own + [o_own], a_far + [swap_c(o_own)]

        def block(xr, cr):
            col = (2 * (xi ^ xr) + (ci ^ cr)) * width
            return jnp.concatenate([lax.dynamic_slice_in_dim(w, col, width, 1) for w in (w_down, w_out)], 0)

        blocks = [[block(xr, cr) for cr in range(2)] for xr in range(2)]
        other_y = [[None, None], [None, None]]
        for xr, cr in BLOCK_ORDER:
            other_y[xr][cr] = swap_y(blocks[xr][cr])

        def product(pair, adds=(), dtype=F32):
            return mix(lhs_near + lhs_far, [pair[0], swap_c(pair[1])], adds, dtype)

        p_own = product(blocks[1])
        r_own = swap_x(p_own)
        p_far = product([tie(w, p_own) for w in other_y[1]])
        r_far = swap_x(p_far)
        out_own = product([blocks[0][0], tie(blocks[0][1], p_far)], [mine, r_own], BF16)
        base = mix(lhs_far, [swap_c(tie(other_y[0][1], p_far))], [from_y, tie(r_far, out_own)])
        last = tie(other_y[0][0], base)
        parts = 2
        size = half // parts
        out_far = [swap_y(mix(lhs_near, [last], [base], BF16, i * size, size)) for i in range(parts)]
        out_far = jnp.concatenate(out_far, 0)
        out = jnp.where(yi == 0, jnp.stack([out_own, out_far]), jnp.stack([out_far, out_own]))
        return out.reshape(batch, new, width), k_next, v_next

    row_spec = P("dp", None, ("tx", "tyz"))
    batch_spec = P(("dp", "tx", "tyz"), None, None)
    in_specs = (row_spec, P(("dp", "tx", "tyz")), batch_spec, batch_spec, P(("tx", "tyz")), P("tx", "tyz"), P("tx", None), P("tx", None), P("tx", "tyz"), P("tx", "tyz"), P("tyz", "tx"), P("tyz", "tx"))
    out_specs = (row_spec, batch_spec, batch_spec)

    return jax.shard_map(local_layer, mesh=mesh, in_specs=in_specs, out_specs=out_specs, check_vma=False)
```

```python
import functools

import jax
import jax.numpy as jnp
from jax import lax
from jax.experimental import pallas as pl
from jax.experimental.pallas import tpu as pltpu
from jax.sharding import PartitionSpec as P

LN_EPS = 1e-6
ROPE_BASE = 10000.0
BF16 = jnp.bfloat16
F32 = jnp.float32


def swap(axis, pairs):
    return lambda a: lax.ppermute(a, axis, pairs)


swap_y = swap("tx", [(0, 1), (1, 0)])
swap_x = swap("tyz", [(0, 2), (2, 0), (1, 3), (3, 1)])
swap_c = swap("tyz", [(0, 1), (1, 0), (2, 3), (3, 2)])


def pick(arr, index):
    return lax.dynamic_index_in_dim(arr, index, axis=0, keepdims=False)


def norm_kernel(offs_ref, *refs):
    pieces, gain_ref, out_ref = refs[:8], refs[8], refs[9]
    width = pieces[0].shape[1]
    total = 8 * width
    xs = [p[...].astype(F32) for p in pieces]
    s1 = sum(jnp.sum(v, axis=-1, keepdims=True) for v in xs)
    s2 = sum(jnp.sum(v * v, axis=-1, keepdims=True) for v in xs)
    mean = s1 / total
    var = s2 / total - mean * mean
    inv = lax.rsqrt(var + LN_EPS)
    for i, v in enumerate(xs):
        off = pl.multiple_of(offs_ref[i], width)
        out_ref[:, pl.ds(off, width)] = ((v - mean) * inv * gain_ref[i : i + 1, :]).astype(BF16)


def layer_norm(pieces, gains, offs):
    tokens, width = pieces[0].shape
    blk = 256
    return pl.pallas_call(
        norm_kernel,
        grid_spec=pltpu.PrefetchScalarGridSpec(
            num_scalar_prefetch=1,
            grid=(tokens // blk,),
            in_specs=[pl.BlockSpec((blk, width), lambda i, o: (i, 0))] * 8 + [pl.BlockSpec((8, width), lambda i, o: (0, 0))],
            out_specs=pl.BlockSpec((blk, 8 * width), lambda i, o: (i, 0)),
        ),
        out_shape=jax.ShapeDtypeStruct((tokens, 8 * width), BF16),
        cost_estimate=pl.CostEstimate(flops=20 * tokens * 8 * width, bytes_accessed=32 * tokens * width, transcendentals=tokens),
        name="norm",
    )(offs, *pieces, gains)


def rope(t, cos_t, sin_t):
    t = t.astype(F32)
    return (t * cos_t + pltpu.roll(t, t.shape[-1] // 2, 1) * sin_t).astype(BF16)


def attn_kernel(len_ref, q0, q1, q2, q3, kv_ref, cos_ref, sin_ref, kc_ref, vc_ref, o0, o1, o2, o3, kn_ref, vn_ref, qs):
    new = kv_ref.shape[0]
    cache = kc_ref.shape[1]
    dim = kc_ref.shape[2]
    length = len_ref[pl.program_id(0)]
    cos_t, sin_t = cos_ref[...], sin_ref[...]
    win = new + 32
    kn_ref[...] = kc_ref[...]
    vn_ref[...] = vc_ref[...]
    base = pl.multiple_of(jnp.minimum((length // 16) * 16, cache - win), 16)
    rows = lax.broadcasted_iota(jnp.int32, (win, new), 0) + (base - length)
    hot = (rows == lax.broadcasted_iota(jnp.int32, (win, new), 1)).astype(BF16)
    key_rot = rope(kv_ref[:, :dim], cos_t, sin_t)
    r = lax.broadcasted_iota(jnp.int32, (win, dim), 0) + (base - length)
    fresh = (r >= 0) & (r < new)
    k_win = jnp.dot(hot, key_rot, preferred_element_type=F32)
    v_win = jnp.dot(hot, kv_ref[:, dim:], preferred_element_type=F32)
    sl = pl.ds(base, win)
    kn_ref[0, sl, :] = jnp.where(fresh, k_win, kc_ref[0, sl, :].astype(F32)).astype(BF16)
    vn_ref[0, sl, :] = jnp.where(fresh, v_win, vc_ref[0, sl, :].astype(F32)).astype(BF16)

    q_refs, o_refs = (q0, q1, q2, q3), (o0, o1, o2, o3)
    hpg = q0.shape[1] // dim
    for g in range(4):
        for h in range(hpg):
            qs[g * hpg * new + h * new : g * hpg * new + (h + 1) * new, :] = rope(q_refs[g][:, h * dim : (h + 1) * dim], cos_t, sin_t)

    def attend(keys):
        @pl.loop(0, 4)
        def _(g):
            group = pl.ds(pl.multiple_of(g * hpg * new, hpg * new), hpg * new)
            q = qs[group, :]
            s = lax.dot_general(q, kn_ref[0, :keys, :], (((1,), (1,)), ((), ())), preferred_element_type=F32)
            s = s * (dim ** -0.5)
            tok = lax.broadcasted_iota(jnp.int32, (hpg * new, keys), 0) % new
            pos = lax.broadcasted_iota(jnp.int32, (hpg * new, keys), 1)
            s = jnp.where(pos - tok <= length, s, -1e30)
            e = jnp.exp(s - jnp.max(s, axis=-1, keepdims=True))
            p = (e * (1.0 / jnp.sum(e, axis=-1, keepdims=True))).astype(BF16)
            qs[group, :] = jnp.dot(p, vn_ref[0, :keys, :], preferred_element_type=F32).astype(BF16)

    step = 256
    need = (length + new + step - 1) // step
    sizes = list(range(5, cache // step + 1))
    for n in sizes:
        cond = need <= n if n == sizes[0] else need == n
        pl.when(cond)(functools.partial(attend, n * step))
    for g in range(4):
        for h in range(hpg):
            o_refs[g][:, h * dim : (h + 1) * dim] = qs[(g * hpg + h) * new : (g * hpg + h + 1) * new, :]


def attention(lengths, qs, kv, cos_t, sin_t, k_cache, v_cache):
    rows, cache, dim = k_cache.shape
    new = kv.shape[0] // rows
    qw = qs[0].shape[1]
    tok = lambda w: pl.BlockSpec((new, w), lambda b, L: (b, 0))
    row = pl.BlockSpec((1, cache, dim), lambda b, L: (b, 0, 0))
    heads = 4 * qw // dim
    return pl.pallas_call(
        attn_kernel,
        grid_spec=pltpu.PrefetchScalarGridSpec(
            num_scalar_prefetch=1,
            grid=(rows,),
            in_specs=[tok(qw)] * 4 + [tok(2 * dim), tok(dim), tok(dim), row, row],
            out_specs=[tok(qw)] * 4 + [row, row],
            scratch_shapes=[pltpu.VMEM((heads * new, dim), BF16)],
        ),
        out_shape=[jax.ShapeDtypeStruct((rows * new, qw), BF16)] * 4 + [jax.ShapeDtypeStruct(k_cache.shape, BF16)] * 2,
        cost_estimate=pl.CostEstimate(
            flops=8 * rows * heads * new * cache * dim, bytes_accessed=8 * rows * cache * dim, transcendentals=rows * heads * new * cache
        ),
        name="attn",
    )(lengths, *qs, kv, cos_t, sin_t, k_cache, v_cache)


def glu_kernel(h_ref, near_w, far_w, a_ref):
    depth = near_w.shape[1]
    near, far = h_ref[:, :depth], h_ref[:, depth:]
    gate = jnp.dot(near, near_w[0], preferred_element_type=F32) + jnp.dot(far, far_w[0], preferred_element_type=F32)
    up = jnp.dot(near, near_w[1], preferred_element_type=F32) + jnp.dot(far, far_w[1], preferred_element_type=F32)
    a_ref[...] = (gate / (1.0 + jnp.exp(-gate)) * up).astype(BF16)


def glu(h, near_w, far_w):
    tokens, depth = h.shape
    cols = near_w.shape[2]
    blk = 512
    w = pl.BlockSpec(near_w.shape, lambda i: (0, 0, 0))
    return pl.pallas_call(
        glu_kernel,
        grid=(tokens // blk,),
        in_specs=[pl.BlockSpec((blk, depth), lambda i: (i, 0)), w, w],
        out_specs=pl.BlockSpec((blk, cols), lambda i: (i, 0)),
        out_shape=jax.ShapeDtypeStruct((tokens, cols), BF16),
        cost_estimate=pl.CostEstimate(flops=4 * tokens * depth * cols, bytes_accessed=2 * tokens * (depth + cols) + 4 * depth * cols, transcendentals=tokens * cols),
        name="glu",
    )(h, near_w, far_w)


def mix_kernel(plan, n_lhs, n_w, *refs):
    lhs, ws, adds, out_ref = refs[:n_lhs], refs[n_lhs : n_lhs + n_w], refs[n_lhs + n_w : -1], refs[-1]
    total = None
    for l, (w, row) in zip(lhs, plan):
        part = jnp.dot(l[...], ws[w][row : row + l.shape[1], :], preferred_element_type=F32)
        total = part if total is None else total + part
    for t in adds:
        total = total + t[...].astype(F32)
    out_ref[...] = total.astype(out_ref.dtype)


def mix(terms, adds=(), dtype=F32, start=0, tokens=None):
    ws, plan = [], []
    for _, w, row in terms:
        found = [i for i, v in enumerate(ws) if v is w]
        if not found:
            ws.append(w)
        plan.append((found[0] if found else len(ws) - 1, row))
    lhs = [t[0] for t in terms]
    tokens = lhs[0].shape[0] if tokens is None else tokens
    cols = ws[0].shape[1]
    blk = 512
    first = start // blk
    tok = lambda w: pl.BlockSpec((blk, w), lambda i: (i + first, 0))
    depth = sum(l.shape[1] for l in lhs)
    add_specs = [tok(cols) if t.shape[0] != tokens else pl.BlockSpec((blk, cols), lambda i: (i, 0)) for t in adds]
    return pl.pallas_call(
        functools.partial(mix_kernel, plan, len(lhs), len(ws)),
        grid=(tokens // blk,),
        in_specs=[tok(l.shape[1]) for l in lhs] + [pl.BlockSpec(w.shape, lambda i: (0, 0)) for w in ws] + add_specs,
        out_specs=pl.BlockSpec((blk, cols), lambda i: (i, 0)),
        out_shape=jax.ShapeDtypeStruct((tokens, cols), dtype),
        cost_estimate=pl.CostEstimate(flops=2 * tokens * depth * cols, bytes_accessed=2 * depth * (tokens + cols), transcendentals=0),
        name="mix",
    )(*lhs, *ws, *adds)


BLOCK_ORDER = [(1, 1), (1, 0), (0, 1), (0, 0)]


def tie(value, *others):
    return lax.optimization_barrier((value, *others))[0]


def solution(mesh):
    def local_layer(hidden, lengths, k_cache, v_cache, ln_gain, w_query, w_key, w_value, w_gate, w_up, w_down, w_out):
        batch, new, width = hidden.shape
        rows_own, _, dim = k_cache.shape
        yi = lax.axis_index("tx")
        ti = lax.axis_index("tyz")
        xi, ci = ti // 2, ti % 2
        half = batch * new // 2
        own_tok = rows_own * new

        g = ln_gain.reshape(1, width)
        g = jnp.concatenate([g, swap_y(g)], 0)
        g = jnp.concatenate([g, swap_x(g)], 0)
        g = jnp.concatenate([g, swap_c(g)], 0)
        hid2 = hidden.reshape(2, half, width)
        mine, other = pick(hid2, yi), pick(hid2, 1 - yi)
        from_y = swap_y(other)
        mine_x = swap_x(mine)
        from_yx = swap_x(from_y)
        near = [mine, from_y, mine_x, from_yx]
        far = [swap_c(p) for p in near]
        offs = []
        for cr in range(2):
            for xr in range(2):
                for yr in range(2):
                    offs.append(width * (4 * yr + 2 * (xr ^ xi) + (cr ^ ci)))
        h = layer_norm(near + far, g, jnp.stack(offs).astype(jnp.int32))

        kv_rows = w_key.shape[0] // 2
        w_kv = jnp.concatenate([w_key, w_value], axis=1)
        kv_part = swap_y(lax.dynamic_slice_in_dim(w_kv, ci * kv_rows, kv_rows, 0))
        kv_pair = jnp.stack([kv_part, swap_c(kv_part)])
        kv_far = jnp.where(ci == 0, kv_pair, kv_pair[::-1]).reshape(w_kv.shape)
        q_far = swap_y(w_query)

        q = mix([(h, jnp.concatenate([w_query, q_far], 0), 0)], dtype=BF16)
        h_own = lax.dynamic_slice_in_dim(h, ti * own_tok, own_tok, 0)
        kv = jnp.dot(h_own, jnp.concatenate([w_kv, kv_far], 0), preferred_element_type=F32).astype(BF16)

        q4 = q.reshape(2, 2, own_tok, q.shape[1])
        q_x = [pick(q4, xi), swap_x(pick(q4, 1 - xi))]
        q_c = [pick(v, ci) for v in q_x] + [swap_c(pick(v, 1 - ci)) for v in q_x]

        half_dim = dim // 2
        inv_freq = ROPE_BASE ** (-2.0 * jnp.arange(half_dim, dtype=F32) / dim)
        positions = (lengths[:, None] + jnp.arange(new, dtype=jnp.int32)[None, :]).reshape(own_tok)
        angles = positions.astype(F32)[:, None] * inv_freq
        cos_t, sin_t = jnp.cos(angles), jnp.sin(angles)
        cos_t = jnp.concatenate([cos_t, cos_t], -1)
        sin_t = jnp.concatenate([-sin_t, sin_t], -1)
        o0, o1, o2, o3, k_next, v_next = attention(lengths, q_c, kv, cos_t, sin_t, k_cache, v_cache)

        keep = [o0, swap_c(o2)]
        send = swap_x(jnp.stack([o1, swap_c(o3)]))
        flip = lambda pair, i: jnp.where(i == 0, jnp.stack(pair), jnp.stack(pair[::-1]))
        o_rows = flip([flip(keep, ci), jnp.where(ci == 0, send, send[::-1])], xi)
        o_own = o_rows.reshape(half, -1)
        o_far = swap_c(o_own)

        chunks = 4
        cw = w_gate.shape[1] // chunks
        a_own, a_far = [], []
        for j in range(chunks):
            near_w = jnp.stack([w[:, j * cw : (j + 1) * cw] for w in (w_gate, w_up)])
            far_w = swap_y(near_w)
            if j == chunks - 1:
                last_w = near_w, far_w
                break
            if j > 0:
                far_w = tie(far_w, a_own[-1], o0)
            a_own.append(glu(h, near_w, far_w))
            a_far.append(swap_c(a_own[-1]))

        def block(xr, cr):
            col = (2 * (xi ^ xr) + (ci ^ cr)) * width
            return jnp.concatenate([lax.dynamic_slice_in_dim(w, col, width, 1) for w in (w_down, w_out)], 0)

        blocks = [[block(xr, cr) for cr in range(2)] for xr in range(2)]
        other_y = [[None, None], [None, None]]
        for xr, cr in BLOCK_ORDER:
            other_y[xr][cr] = swap_y(blocks[xr][cr])

        o_far = swap_c(o_own)

        def terms(near_w, far_w, which):
            out = []
            for a_part, o_part, w in ((a_own, o_own, near_w), (a_far, o_far, far_w)):
                if w is not None:
                    out += [(o_part, w, chunks * cw) if k == "o" else (a_part[k], w, k * cw) for k in which]
            return out

        early, late, every = [*range(chunks - 1), "o"], [chunks - 1], [*range(chunks), "o"]
        parts = 2
        size = half // parts

        cross_far, same_far = swap_c(blocks[1][1]), swap_c(blocks[0][1])
        pre_cross = mix(terms(blocks[1][0], cross_far, early))
        pre_same = mix(terms(tie(blocks[0][0], pre_cross), same_far, early), [mine])
        a_own.append(glu(h, last_w[0], tie(last_w[1], pre_same)))
        a_far.append(swap_c(a_own[-1]))
        p_own = mix(terms(blocks[1][0], cross_far, late), [pre_cross])
        r_own = swap_x(p_own)

        pre_far = mix(terms(None, swap_c(tie(other_y[1][1], p_own)), every))
        near_w = tie(other_y[1][0], pre_far)
        p_far = [mix(terms(near_w, None, every), [pre_far], F32, i * size, size) for i in range(parts)]
        r_far = [swap_x(p) for p in p_far]
        base = mix(terms(None, swap_c(tie(other_y[0][1], *p_far)), every), [from_y])
        out_own = mix(terms(blocks[0][0], same_far, late), [pre_same, tie(r_own, base)], BF16)
        last = tie(other_y[0][0], out_own)
        out_far = []
        for i in range(parts):
            out_far.append(mix(terms(last, None, every), [base, r_far[i]], BF16, i * size, size))
            out_far[i] = swap_y(out_far[i])
        out_far = jnp.concatenate(out_far, 0)
        out = jnp.where(yi == 0, jnp.stack([out_own, out_far]), jnp.stack([out_far, out_own]))
        return out.reshape(batch, new, width), k_next, v_next

    row_spec = P("dp", None, ("tx", "tyz"))
    batch_spec = P(("dp", "tx", "tyz"), None, None)
    in_specs = (row_spec, P(("dp", "tx", "tyz")), batch_spec, batch_spec, P(("tx", "tyz")), P("tx", "tyz"), P("tx", None), P("tx", None), P("tx", "tyz"), P("tx", "tyz"), P("tyz", "tx"), P("tyz", "tx"))
    out_specs = (row_spec, batch_spec, batch_spec)

    return jax.shard_map(local_layer, mesh=mesh, in_specs=in_specs, out_specs=out_specs, check_vma=False)
```

```python
import functools

import jax
import jax.numpy as jnp
from jax import lax
from jax.experimental import pallas as pl
from jax.experimental.pallas import tpu as pltpu
from jax.sharding import PartitionSpec as P

LN_EPS = 1e-6
ROPE_BASE = 10000.0
BF16 = jnp.bfloat16
F32 = jnp.float32


def swap(axis, pairs):
    return lambda a: lax.ppermute(a, axis, pairs)


swap_y = swap("tx", [(0, 1), (1, 0)])
swap_x = swap("tyz", [(0, 2), (2, 0), (1, 3), (3, 1)])
swap_c = swap("tyz", [(0, 1), (1, 0), (2, 3), (3, 2)])


def pick(arr, index):
    return lax.dynamic_index_in_dim(arr, index, axis=0, keepdims=False)


def norm_kernel(offs_ref, *refs):
    pieces, gain_ref, out_ref = refs[:8], refs[8], refs[9]
    width = pieces[0].shape[1]
    total = 8 * width
    xs = [p[...].astype(F32) for p in pieces]
    s1 = sum(jnp.sum(v, axis=-1, keepdims=True) for v in xs)
    s2 = sum(jnp.sum(v * v, axis=-1, keepdims=True) for v in xs)
    mean = s1 / total
    var = s2 / total - mean * mean
    inv = lax.rsqrt(var + LN_EPS)
    for i, v in enumerate(xs):
        off = pl.multiple_of(offs_ref[i], width)
        out_ref[:, pl.ds(off, width)] = ((v - mean) * inv * gain_ref[i : i + 1, :]).astype(BF16)


def layer_norm(pieces, gains, offs):
    tokens, width = pieces[0].shape
    blk = 256
    return pl.pallas_call(
        norm_kernel,
        grid_spec=pltpu.PrefetchScalarGridSpec(
            num_scalar_prefetch=1,
            grid=(tokens // blk,),
            in_specs=[pl.BlockSpec((blk, width), lambda i, o: (i, 0))] * 8 + [pl.BlockSpec((8, width), lambda i, o: (0, 0))],
            out_specs=pl.BlockSpec((blk, 8 * width), lambda i, o: (i, 0)),
        ),
        out_shape=jax.ShapeDtypeStruct((tokens, 8 * width), BF16),
        cost_estimate=pl.CostEstimate(flops=20 * tokens * 8 * width, bytes_accessed=32 * tokens * width, transcendentals=tokens),
        name="norm",
    )(offs, *pieces, gains)


def rope(t, cos_t, sin_t):
    t = t.astype(F32)
    return (t * cos_t + pltpu.roll(t, t.shape[-1] // 2, 1) * sin_t).astype(BF16)


def attn_kernel(len_ref, q0, q1, q2, q3, kv_ref, cos_ref, sin_ref, kc_ref, vc_ref, o0, o1, o2, o3, kn_ref, vn_ref, qs):
    new = kv_ref.shape[0]
    cache = kc_ref.shape[1]
    dim = kc_ref.shape[2]
    length = len_ref[pl.program_id(0)]
    cos_t, sin_t = cos_ref[...], sin_ref[...]
    win = new + 32
    kn_ref[...] = kc_ref[...]
    vn_ref[...] = vc_ref[...]
    base = pl.multiple_of(jnp.minimum((length // 16) * 16, cache - win), 16)
    rows = lax.broadcasted_iota(jnp.int32, (win, new), 0) + (base - length)
    hot = (rows == lax.broadcasted_iota(jnp.int32, (win, new), 1)).astype(BF16)
    key_rot = rope(kv_ref[:, :dim], cos_t, sin_t)
    r = lax.broadcasted_iota(jnp.int32, (win, dim), 0) + (base - length)
    fresh = (r >= 0) & (r < new)
    k_win = jnp.dot(hot, key_rot, preferred_element_type=F32)
    v_win = jnp.dot(hot, kv_ref[:, dim:], preferred_element_type=F32)
    sl = pl.ds(base, win)
    kn_ref[0, sl, :] = jnp.where(fresh, k_win, kc_ref[0, sl, :].astype(F32)).astype(BF16)
    vn_ref[0, sl, :] = jnp.where(fresh, v_win, vc_ref[0, sl, :].astype(F32)).astype(BF16)

    q_refs, o_refs = (q0, q1, q2, q3), (o0, o1, o2, o3)
    hpg = q0.shape[1] // dim
    for g in range(4):
        for h in range(hpg):
            qs[g * hpg * new + h * new : g * hpg * new + (h + 1) * new, :] = rope(q_refs[g][:, h * dim : (h + 1) * dim], cos_t, sin_t)

    def attend(keys):
        @pl.loop(0, 4)
        def _(g):
            group = pl.ds(pl.multiple_of(g * hpg * new, hpg * new), hpg * new)
            q = qs[group, :]
            s = lax.dot_general(q, kn_ref[0, :keys, :], (((1,), (1,)), ((), ())), preferred_element_type=F32)
            s = s * (dim ** -0.5)
            tok = lax.broadcasted_iota(jnp.int32, (hpg * new, keys), 0) % new
            pos = lax.broadcasted_iota(jnp.int32, (hpg * new, keys), 1)
            s = jnp.where(pos - tok <= length, s, -1e30)
            e = jnp.exp(s - jnp.max(s, axis=-1, keepdims=True))
            p = (e * (1.0 / jnp.sum(e, axis=-1, keepdims=True))).astype(BF16)
            qs[group, :] = jnp.dot(p, vn_ref[0, :keys, :], preferred_element_type=F32).astype(BF16)

    step = 256
    need = (length + new + step - 1) // step
    sizes = list(range(5, cache // step + 1))
    for n in sizes:
        cond = need <= n if n == sizes[0] else need == n
        pl.when(cond)(functools.partial(attend, n * step))
    for g in range(4):
        for h in range(hpg):
            o_refs[g][:, h * dim : (h + 1) * dim] = qs[(g * hpg + h) * new : (g * hpg + h + 1) * new, :]


def attention(lengths, qs, kv, cos_t, sin_t, k_cache, v_cache):
    rows, cache, dim = k_cache.shape
    new = kv.shape[0] // rows
    qw = qs[0].shape[1]
    tok = lambda w: pl.BlockSpec((new, w), lambda b, L: (b, 0))
    row = pl.BlockSpec((1, cache, dim), lambda b, L: (b, 0, 0))
    heads = 4 * qw // dim
    return pl.pallas_call(
        attn_kernel,
        grid_spec=pltpu.PrefetchScalarGridSpec(
            num_scalar_prefetch=1,
            grid=(rows,),
            in_specs=[tok(qw)] * 4 + [tok(2 * dim), tok(dim), tok(dim), row, row],
            out_specs=[tok(qw)] * 4 + [row, row],
            scratch_shapes=[pltpu.VMEM((heads * new, dim), BF16)],
        ),
        out_shape=[jax.ShapeDtypeStruct((rows * new, qw), BF16)] * 4 + [jax.ShapeDtypeStruct(k_cache.shape, BF16)] * 2,
        cost_estimate=pl.CostEstimate(
            flops=8 * rows * heads * new * cache * dim, bytes_accessed=8 * rows * cache * dim, transcendentals=rows * heads * new * cache
        ),
        name="attn",
    )(lengths, *qs, kv, cos_t, sin_t, k_cache, v_cache)


def glu_kernel(h_ref, near_w, far_w, a_ref):
    depth = near_w.shape[1]
    near, far = h_ref[:, :depth], h_ref[:, depth:]
    gate = jnp.dot(near, near_w[0], preferred_element_type=F32) + jnp.dot(far, far_w[0], preferred_element_type=F32)
    up = jnp.dot(near, near_w[1], preferred_element_type=F32) + jnp.dot(far, far_w[1], preferred_element_type=F32)
    a_ref[...] = (gate / (1.0 + jnp.exp(-gate)) * up).astype(BF16)


def glu(h, near_w, far_w):
    tokens, depth = h.shape
    cols = near_w.shape[2]
    blk = 512
    w = pl.BlockSpec(near_w.shape, lambda i: (0, 0, 0))
    return pl.pallas_call(
        glu_kernel,
        grid=(tokens // blk,),
        in_specs=[pl.BlockSpec((blk, depth), lambda i: (i, 0)), w, w],
        out_specs=pl.BlockSpec((blk, cols), lambda i: (i, 0)),
        out_shape=jax.ShapeDtypeStruct((tokens, cols), BF16),
        cost_estimate=pl.CostEstimate(flops=4 * tokens * depth * cols, bytes_accessed=2 * tokens * (depth + cols) + 4 * depth * cols, transcendentals=tokens * cols),
        name="glu",
    )(h, near_w, far_w)


def mix_kernel(plan, n_lhs, n_w, *refs):
    lhs, ws, adds, out_ref = refs[:n_lhs], refs[n_lhs : n_lhs + n_w], refs[n_lhs + n_w : -1], refs[-1]
    total = None
    for l, (w, row) in zip(lhs, plan):
        part = jnp.dot(l[...], ws[w][row : row + l.shape[1], :], preferred_element_type=F32)
        total = part if total is None else total + part
    for t in adds:
        total = total + t[...].astype(F32)
    out_ref[...] = total.astype(out_ref.dtype)


def mix(terms, adds=(), dtype=F32, start=0, tokens=None):
    ws, plan = [], []
    for _, w, row in terms:
        found = [i for i, v in enumerate(ws) if v is w]
        if not found:
            ws.append(w)
        plan.append((found[0] if found else len(ws) - 1, row))
    lhs = [t[0] for t in terms]
    tokens = lhs[0].shape[0] if tokens is None else tokens
    cols = ws[0].shape[1]
    blk = 512
    first = start // blk
    tok = lambda w: pl.BlockSpec((blk, w), lambda i: (i + first, 0))
    depth = sum(l.shape[1] for l in lhs)
    add_specs = [tok(cols) if t.shape[0] != tokens else pl.BlockSpec((blk, cols), lambda i: (i, 0)) for t in adds]
    return pl.pallas_call(
        functools.partial(mix_kernel, plan, len(lhs), len(ws)),
        grid=(tokens // blk,),
        in_specs=[tok(l.shape[1]) for l in lhs] + [pl.BlockSpec(w.shape, lambda i: (0, 0)) for w in ws] + add_specs,
        out_specs=pl.BlockSpec((blk, cols), lambda i: (i, 0)),
        out_shape=jax.ShapeDtypeStruct((tokens, cols), dtype),
        cost_estimate=pl.CostEstimate(flops=2 * tokens * depth * cols, bytes_accessed=2 * depth * (tokens + cols), transcendentals=0),
        name="mix",
    )(*lhs, *ws, *adds)


BLOCK_ORDER = [(1, 1), (1, 0), (0, 1), (0, 0)]


def tie(value, *others):
    return lax.optimization_barrier((value, *others))[0]


def solution(mesh):
    def local_layer(hidden, lengths, k_cache, v_cache, ln_gain, w_query, w_key, w_value, w_gate, w_up, w_down, w_out):
        batch, new, width = hidden.shape
        rows_own, _, dim = k_cache.shape
        yi = lax.axis_index("tx")
        ti = lax.axis_index("tyz")
        xi, ci = ti // 2, ti % 2
        half = batch * new // 2
        own_tok = rows_own * new

        g = ln_gain.reshape(1, width)
        g = jnp.concatenate([g, swap_y(g)], 0)
        g = jnp.concatenate([g, swap_x(g)], 0)
        g = jnp.concatenate([g, swap_c(g)], 0)
        hid2 = hidden.reshape(2, half, width)
        other = pick(hid2, 1 - yi)
        mine = pick(tie(hid2, other), yi)
        from_y = swap_y(other)
        mine_x = swap_x(mine)
        from_yx = swap_x(from_y)
        near = [mine, from_y, mine_x, from_yx]
        far = [swap_c(p) for p in near]
        offs = []
        for cr in range(2):
            for xr in range(2):
                for yr in range(2):
                    offs.append(width * (4 * yr + 2 * (xr ^ xi) + (cr ^ ci)))
        h = layer_norm(near + far, g, jnp.stack(offs).astype(jnp.int32))

        kv_rows = w_key.shape[0] // 2
        w_kv = jnp.concatenate([w_key, w_value], axis=1)
        kv_part = swap_y(lax.dynamic_slice_in_dim(w_kv, ci * kv_rows, kv_rows, 0))
        kv_pair = jnp.stack([kv_part, swap_c(kv_part)])
        kv_far = jnp.where(ci == 0, kv_pair, kv_pair[::-1]).reshape(w_kv.shape)
        q_far = swap_y(w_query)

        q = mix([(h, jnp.concatenate([w_query, q_far], 0), 0)], dtype=BF16)
        h_own = lax.dynamic_slice_in_dim(h, ti * own_tok, own_tok, 0)
        kv = jnp.dot(h_own, jnp.concatenate([w_kv, kv_far], 0), preferred_element_type=F32).astype(BF16)

        q4 = q.reshape(2, 2, own_tok, q.shape[1])
        q_x = [pick(q4, xi), swap_x(pick(q4, 1 - xi))]
        q_c = [pick(v, ci) for v in q_x] + [swap_c(pick(v, 1 - ci)) for v in q_x]

        chunks = 4
        cw = w_gate.shape[1] // chunks
        near_ws = [jnp.stack([w[:, j * cw : (j + 1) * cw] for w in (w_gate, w_up)]) for j in range(chunks)]
        far_ws = [swap_y(w) for w in near_ws]
        a_own = [glu(h, near_ws[0], far_ws[0])]
        half_dim = dim // 2
        inv_freq = ROPE_BASE ** (-2.0 * jnp.arange(half_dim, dtype=F32) / dim)
        positions = (lengths[:, None] + jnp.arange(new, dtype=jnp.int32)[None, :]).reshape(own_tok)
        angles = positions.astype(F32)[:, None] * inv_freq
        cos_t, sin_t = jnp.cos(angles), jnp.sin(angles)
        cos_t = jnp.concatenate([cos_t, cos_t], -1)
        sin_t = jnp.concatenate([-sin_t, sin_t], -1)
        o0, o1, o2, o3, k_next, v_next = attention(lengths, [tie(q_c[0], a_own[0]), *q_c[1:]], kv, cos_t, sin_t, k_cache, v_cache)

        keep = [o0, swap_c(o2)]
        send = swap_x(jnp.stack([o1, swap_c(o3)]))
        flip = lambda pair, i: jnp.where(i == 0, jnp.stack(pair), jnp.stack(pair[::-1]))
        o_rows = flip([flip(keep, ci), jnp.where(ci == 0, send, send[::-1])], xi)
        o_own = o_rows.reshape(half, -1)
        o_far = swap_c(o_own)
        o_far = swap_c(o_own)

        for j in range(1, chunks - 1):
            a_own.append(glu(h, near_ws[j], tie(far_ws[j], a_own[-1], o0)))
        a_far = [swap_c(v) for v in a_own]

        def block(xr, cr):
            col = (2 * (xi ^ xr) + (ci ^ cr)) * width
            return jnp.concatenate([lax.dynamic_slice_in_dim(w, col, width, 1) for w in (w_down, w_out)], 0)

        blocks = [[block(xr, cr) for cr in range(2)] for xr in range(2)]
        other_y = [[None, None], [None, None]]
        for xr, cr in BLOCK_ORDER:
            other_y[xr][cr] = swap_y(blocks[xr][cr])

        def terms(near_w, far_w, which):
            out = []
            for a_part, o_part, w in ((a_own, o_own, near_w), (a_far, o_far, far_w)):
                if w is not None:
                    out += [(o_part, w, chunks * cw) if k == "o" else (a_part[k], w, k * cw) for k in which]
            return out

        early, late, every = [*range(chunks - 1), "o"], [chunks - 1], [*range(chunks), "o"]
        parts = 2
        size = half // parts

        cross_far, same_far = swap_c(blocks[1][1]), swap_c(blocks[0][1])
        pre_cross = mix(terms(blocks[1][0], cross_far, early))
        pre_same = mix(terms(tie(blocks[0][0], pre_cross), same_far, early), [mine])
        a_own.append(glu(h, near_ws[-1], tie(far_ws[-1], pre_same)))
        a_far.append(swap_c(a_own[-1]))
        p_own = mix(terms(blocks[1][0], cross_far, late), [pre_cross])
        r_own = swap_x(p_own)

        pre_far = mix(terms(None, swap_c(tie(other_y[1][1], p_own)), every))
        near_w = tie(other_y[1][0], pre_far)
        p_far, r_far = [], []
        for i in range(parts):
            p_far.append(mix(terms(near_w, None, every), [pre_far], F32, i * size, size))
            r_far.append(swap_x(p_far[i]))
        out_own = mix(terms(blocks[0][0], same_far, late), [pre_same, tie(r_own, *p_far)], BF16)
        base = mix(terms(None, swap_c(tie(other_y[0][1], out_own)), every), [from_y])
        last = tie(other_y[0][0], base)
        out_far = []
        for i in range(parts):
            out_far.append(mix(terms(last, None, every), [base, r_far[i]], BF16, i * size, size))
            out_far[i] = swap_y(out_far[i])
        out_far = jnp.concatenate(out_far, 0)
        out = jnp.where(yi == 0, jnp.stack([out_own, out_far]), jnp.stack([out_far, out_own]))
        return out.reshape(batch, new, width), k_next, v_next

    row_spec = P("dp", None, ("tx", "tyz"))
    batch_spec = P(("dp", "tx", "tyz"), None, None)
    in_specs = (row_spec, P(("dp", "tx", "tyz")), batch_spec, batch_spec, P(("tx", "tyz")), P("tx", "tyz"), P("tx", None), P("tx", None), P("tx", "tyz"), P("tx", "tyz"), P("tyz", "tx"), P("tyz", "tx"))
    out_specs = (row_spec, batch_spec, batch_spec)

    return jax.shard_map(local_layer, mesh=mesh, in_specs=in_specs, out_specs=out_specs, check_vma=False)
```

```python
import functools

import jax
import jax.numpy as jnp
from jax import lax
from jax.experimental import pallas as pl
from jax.experimental.pallas import tpu as pltpu
from jax.sharding import PartitionSpec as P

LN_EPS = 1e-6
ROPE_BASE = 10000.0
BF16 = jnp.bfloat16
F32 = jnp.float32


def swap(axis, pairs):
    return lambda a: lax.ppermute(a, axis, pairs)


swap_y = swap("tx", [(0, 1), (1, 0)])
swap_x = swap("tyz", [(0, 2), (2, 0), (1, 3), (3, 1)])
swap_c = swap("tyz", [(0, 1), (1, 0), (2, 3), (3, 2)])


def pick(arr, index):
    return lax.dynamic_index_in_dim(arr, index, axis=0, keepdims=False)


def norm_kernel(offs_ref, *refs):
    pieces, gain_ref, out_ref = refs[:8], refs[8], refs[9]
    width = pieces[0].shape[1]
    total = 8 * width
    xs = [p[...].astype(F32) for p in pieces]
    s1 = sum(jnp.sum(v, axis=-1, keepdims=True) for v in xs)
    s2 = sum(jnp.sum(v * v, axis=-1, keepdims=True) for v in xs)
    mean = s1 / total
    var = s2 / total - mean * mean
    inv = lax.rsqrt(var + LN_EPS)
    for i, v in enumerate(xs):
        off = pl.multiple_of(offs_ref[i], width)
        out_ref[:, pl.ds(off, width)] = ((v - mean) * inv * gain_ref[i : i + 1, :]).astype(BF16)


def layer_norm(pieces, gains, offs):
    tokens, width = pieces[0].shape
    blk = 256
    return pl.pallas_call(
        norm_kernel,
        grid_spec=pltpu.PrefetchScalarGridSpec(
            num_scalar_prefetch=1,
            grid=(tokens // blk,),
            in_specs=[pl.BlockSpec((blk, width), lambda i, o: (i, 0))] * 8 + [pl.BlockSpec((8, width), lambda i, o: (0, 0))],
            out_specs=pl.BlockSpec((blk, 8 * width), lambda i, o: (i, 0)),
        ),
        out_shape=jax.ShapeDtypeStruct((tokens, 8 * width), BF16),
        cost_estimate=pl.CostEstimate(flops=20 * tokens * 8 * width, bytes_accessed=32 * tokens * width, transcendentals=tokens),
        name="norm",
    )(offs, *pieces, gains)


def rope(t, cos_t, sin_t):
    t = t.astype(F32)
    return (t * cos_t + pltpu.roll(t, t.shape[-1] // 2, 1) * sin_t).astype(BF16)


def attn_kernel(len_ref, q0, q1, q2, q3, kv_ref, cos_ref, sin_ref, kc_ref, vc_ref, o0, o1, o2, o3, kn_ref, vn_ref, qs):
    new = kv_ref.shape[0]
    cache = kc_ref.shape[1]
    dim = kc_ref.shape[2]
    length = len_ref[pl.program_id(0)]
    cos_t, sin_t = cos_ref[...], sin_ref[...]
    win = new + 32
    kn_ref[...] = kc_ref[...]
    vn_ref[...] = vc_ref[...]
    base = pl.multiple_of(jnp.minimum((length // 16) * 16, cache - win), 16)
    rows = lax.broadcasted_iota(jnp.int32, (win, new), 0) + (base - length)
    hot = (rows == lax.broadcasted_iota(jnp.int32, (win, new), 1)).astype(BF16)
    key_rot = rope(kv_ref[:, :dim], cos_t, sin_t)
    r = lax.broadcasted_iota(jnp.int32, (win, dim), 0) + (base - length)
    fresh = (r >= 0) & (r < new)
    k_win = jnp.dot(hot, key_rot, preferred_element_type=F32)
    v_win = jnp.dot(hot, kv_ref[:, dim:], preferred_element_type=F32)
    sl = pl.ds(base, win)
    kn_ref[0, sl, :] = jnp.where(fresh, k_win, kc_ref[0, sl, :].astype(F32)).astype(BF16)
    vn_ref[0, sl, :] = jnp.where(fresh, v_win, vc_ref[0, sl, :].astype(F32)).astype(BF16)

    q_refs, o_refs = (q0, q1, q2, q3), (o0, o1, o2, o3)
    hpg = q0.shape[1] // dim
    for g in range(4):
        for h in range(hpg):
            qs[g * hpg * new + h * new : g * hpg * new + (h + 1) * new, :] = rope(q_refs[g][:, h * dim : (h + 1) * dim], cos_t, sin_t)

    def attend(keys):
        @pl.loop(0, 4)
        def _(g):
            group = pl.ds(pl.multiple_of(g * hpg * new, hpg * new), hpg * new)
            q = qs[group, :]
            s = lax.dot_general(q, kn_ref[0, :keys, :], (((1,), (1,)), ((), ())), preferred_element_type=F32)
            s = s * (dim ** -0.5)
            tok = lax.broadcasted_iota(jnp.int32, (hpg * new, keys), 0) % new
            pos = lax.broadcasted_iota(jnp.int32, (hpg * new, keys), 1)
            s = jnp.where(pos - tok <= length, s, -1e30)
            e = jnp.exp(s - jnp.max(s, axis=-1, keepdims=True))
            p = (e * (1.0 / jnp.sum(e, axis=-1, keepdims=True))).astype(BF16)
            qs[group, :] = jnp.dot(p, vn_ref[0, :keys, :], preferred_element_type=F32).astype(BF16)

    step = 256
    need = (length + new + step - 1) // step
    sizes = list(range(5, cache // step + 1))
    for n in sizes:
        cond = need <= n if n == sizes[0] else need == n
        pl.when(cond)(functools.partial(attend, n * step))
    for g in range(4):
        for h in range(hpg):
            o_refs[g][:, h * dim : (h + 1) * dim] = qs[(g * hpg + h) * new : (g * hpg + h + 1) * new, :]


def attention(lengths, qs, kv, cos_t, sin_t, k_cache, v_cache):
    rows, cache, dim = k_cache.shape
    new = kv.shape[0] // rows
    qw = qs[0].shape[1]
    tok = lambda w: pl.BlockSpec((new, w), lambda b, L: (b, 0))
    row = pl.BlockSpec((1, cache, dim), lambda b, L: (b, 0, 0))
    heads = 4 * qw // dim
    return pl.pallas_call(
        attn_kernel,
        grid_spec=pltpu.PrefetchScalarGridSpec(
            num_scalar_prefetch=1,
            grid=(rows,),
            in_specs=[tok(qw)] * 4 + [tok(2 * dim), tok(dim), tok(dim), row, row],
            out_specs=[tok(qw)] * 4 + [row, row],
            scratch_shapes=[pltpu.VMEM((heads * new, dim), BF16)],
        ),
        out_shape=[jax.ShapeDtypeStruct((rows * new, qw), BF16)] * 4 + [jax.ShapeDtypeStruct(k_cache.shape, BF16)] * 2,
        cost_estimate=pl.CostEstimate(
            flops=8 * rows * heads * new * cache * dim, bytes_accessed=8 * rows * cache * dim, transcendentals=rows * heads * new * cache
        ),
        name="attn",
    )(lengths, *qs, kv, cos_t, sin_t, k_cache, v_cache)


def glu_kernel(h_ref, near_w, far_w, a_ref):
    depth = near_w.shape[1]
    near, far = h_ref[:, :depth], h_ref[:, depth:]
    gate = jnp.dot(near, near_w[0], preferred_element_type=F32) + jnp.dot(far, far_w[0], preferred_element_type=F32)
    up = jnp.dot(near, near_w[1], preferred_element_type=F32) + jnp.dot(far, far_w[1], preferred_element_type=F32)
    a_ref[...] = (gate / (1.0 + jnp.exp(-gate)) * up).astype(BF16)


def glu(h, near_w, far_w):
    tokens, depth = h.shape
    cols = near_w.shape[2]
    blk = 512
    w = pl.BlockSpec(near_w.shape, lambda i: (0, 0, 0))
    return pl.pallas_call(
        glu_kernel,
        grid=(tokens // blk,),
        in_specs=[pl.BlockSpec((blk, depth), lambda i: (i, 0)), w, w],
        out_specs=pl.BlockSpec((blk, cols), lambda i: (i, 0)),
        out_shape=jax.ShapeDtypeStruct((tokens, cols), BF16),
        cost_estimate=pl.CostEstimate(flops=4 * tokens * depth * cols, bytes_accessed=2 * tokens * (depth + cols) + 4 * depth * cols, transcendentals=tokens * cols),
        name="glu",
    )(h, near_w, far_w)


def mix_kernel(plan, n_lhs, n_w, *refs):
    lhs, ws, adds, out_ref = refs[:n_lhs], refs[n_lhs : n_lhs + n_w], refs[n_lhs + n_w : -1], refs[-1]
    total = None
    for l, (w, row) in zip(lhs, plan):
        part = jnp.dot(l[...], ws[w][row : row + l.shape[1], :], preferred_element_type=F32)
        total = part if total is None else total + part
    for t in adds:
        total = total + t[...].astype(F32)
    out_ref[...] = total.astype(out_ref.dtype)


def mix(terms, adds=(), dtype=F32, start=0, tokens=None, col=0):
    ws, plan = [], []
    for _, w, row in terms:
        found = [i for i, v in enumerate(ws) if v is w]
        if not found:
            ws.append(w)
        plan.append((found[0] if found else len(ws) - 1, row))
    lhs = [t[0] for t in terms]
    tokens = lhs[0].shape[0] if tokens is None else tokens
    cols = ws[0].shape[1]
    blk = 512
    first = start // blk
    tok = lambda w: pl.BlockSpec((blk, w), lambda i: (i + first, 0))
    depth = sum(l.shape[1] for l in lhs)
    add_specs = [pl.BlockSpec((blk, cols), lambda i, f=first * (t.shape[0] != tokens), c=col * (t.shape[1] != cols): (i + f, c)) for t in adds]
    return pl.pallas_call(
        functools.partial(mix_kernel, plan, len(lhs), len(ws)),
        grid=(tokens // blk,),
        in_specs=[tok(l.shape[1]) for l in lhs] + [pl.BlockSpec(w.shape, lambda i: (0, 0)) for w in ws] + add_specs,
        out_specs=pl.BlockSpec((blk, cols), lambda i: (i, 0)),
        out_shape=jax.ShapeDtypeStruct((tokens, cols), dtype),
        cost_estimate=pl.CostEstimate(flops=2 * tokens * depth * cols, bytes_accessed=2 * depth * (tokens + cols), transcendentals=0),
        name="mix",
    )(*lhs, *ws, *adds)


BLOCK_ORDER = ["11", "10A", "10B", "01", "00A", "00B"]


def tie(value, *others):
    return lax.optimization_barrier((value, *others))[0]


def solution(mesh):
    def local_layer(hidden, lengths, k_cache, v_cache, ln_gain, w_query, w_key, w_value, w_gate, w_up, w_down, w_out):
        batch, new, width = hidden.shape
        rows_own, _, dim = k_cache.shape
        yi = lax.axis_index("tx")
        ti = lax.axis_index("tyz")
        xi, ci = ti // 2, ti % 2
        half = batch * new // 2
        own_tok = rows_own * new

        g = ln_gain.reshape(1, width)
        g = jnp.concatenate([g, swap_y(g)], 0)
        g = jnp.concatenate([g, swap_x(g)], 0)
        g = jnp.concatenate([g, swap_c(g)], 0)
        hid2 = hidden.reshape(2, half, width)
        other = pick(hid2, 1 - yi)
        mine = pick(tie(hid2, other), yi)
        from_y = swap_y(other)
        mine_x = swap_x(mine)
        from_yx = swap_x(from_y)
        near = [mine, from_y, mine_x, from_yx]
        far = [swap_c(p) for p in near]
        offs = []
        for cr in range(2):
            for xr in range(2):
                for yr in range(2):
                    offs.append(width * (4 * yr + 2 * (xr ^ xi) + (cr ^ ci)))
        h = layer_norm(near + far, g, jnp.stack(offs).astype(jnp.int32))

        kv_rows = w_key.shape[0] // 2
        w_kv = jnp.concatenate([w_key, w_value], axis=1)
        kv_part = swap_y(lax.dynamic_slice_in_dim(w_kv, ci * kv_rows, kv_rows, 0))
        kv_pair = jnp.stack([kv_part, swap_c(kv_part)])
        kv_far = jnp.where(ci == 0, kv_pair, kv_pair[::-1]).reshape(w_kv.shape)
        q_far = swap_y(w_query)

        q = mix([(h, jnp.concatenate([w_query, q_far], 0), 0)], dtype=BF16)
        h_own = lax.dynamic_slice_in_dim(h, ti * own_tok, own_tok, 0)
        kv = jnp.dot(h_own, jnp.concatenate([w_kv, kv_far], 0), preferred_element_type=F32).astype(BF16)

        q4 = q.reshape(2, 2, own_tok, q.shape[1])
        q_x = [pick(q4, xi), swap_x(pick(q4, 1 - xi))]
        q_c = [pick(v, ci) for v in q_x] + [swap_c(pick(v, 1 - ci)) for v in q_x]

        chunks = 4
        cw = w_gate.shape[1] // chunks
        near_ws = [jnp.stack([w[:, j * cw : (j + 1) * cw] for w in (w_gate, w_up)]) for j in range(chunks)]
        far_ws = [swap_y(w) for w in near_ws]
        a_own = [glu(h, near_ws[0], far_ws[0])]
        half_dim = dim // 2
        inv_freq = ROPE_BASE ** (-2.0 * jnp.arange(half_dim, dtype=F32) / dim)
        positions = (lengths[:, None] + jnp.arange(new, dtype=jnp.int32)[None, :]).reshape(own_tok)
        angles = positions.astype(F32)[:, None] * inv_freq
        cos_t, sin_t = jnp.cos(angles), jnp.sin(angles)
        cos_t = jnp.concatenate([cos_t, cos_t], -1)
        sin_t = jnp.concatenate([-sin_t, sin_t], -1)
        o0, o1, o2, o3, k_next, v_next = attention(lengths, [tie(q_c[0], a_own[0]), *q_c[1:]], kv, cos_t, sin_t, k_cache, v_cache)

        keep = [o0, swap_c(o2)]
        send = swap_x(jnp.stack([o1, swap_c(o3)]))
        flip = lambda pair, i: jnp.where(i == 0, jnp.stack(pair), jnp.stack(pair[::-1]))
        o_rows = flip([flip(keep, ci), jnp.where(ci == 0, send, send[::-1])], xi)
        o_own = o_rows.reshape(half, -1)
        o_far = swap_c(o_own)
        o_far = swap_c(o_own)

        for j in range(1, chunks - 1):
            a_own.append(glu(h, near_ws[j], tie(far_ws[j], a_own[-1], o0)))
        a_far = [swap_c(v) for v in a_own]

        def block(xr, cr):
            col = (2 * (xi ^ xr) + (ci ^ cr)) * width
            return jnp.concatenate([lax.dynamic_slice_in_dim(w, col, width, 1) for w in (w_down, w_out)], 0)

        blocks = [[block(xr, cr) for cr in range(2)] for xr in range(2)]
        narrow = width // 2
        other_y = {}
        for name in BLOCK_ORDER:
            b = blocks[int(name[0])][int(name[1])]
            if name[2:]:
                col = "AB".index(name[2]) * narrow
                b = b[:, col : col + narrow]
            other_y[name] = swap_y(b)

        def terms(near_w, far_w, which):
            out = []
            for a_part, o_part, w in ((a_own, o_own, near_w), (a_far, o_far, far_w)):
                if w is not None:
                    out += [(o_part, w, chunks * cw) if k == "o" else (a_part[k], w, k * cw) for k in which]
            return out

        early, late, every = [*range(chunks - 1), "o"], [chunks - 1], [*range(chunks), "o"]
        split = (0, 3 * half // 4), (3 * half // 4, half // 4)

        cross_far, same_far = swap_c(blocks[1][1]), swap_c(blocks[0][1])
        pre_cross = mix(terms(blocks[1][0], cross_far, early))
        pre_same = mix(terms(tie(blocks[0][0], pre_cross), same_far, early), [mine])
        a_own.append(glu(h, near_ws[-1], tie(far_ws[-1], pre_same)))
        a_far.append(swap_c(a_own[-1]))
        p_own, r_own = [], []
        for i, span in enumerate(split):
            p_own.append(mix(terms(blocks[1][0], cross_far, late), [pre_cross], F32, *span))
            r_own.append(swap_x(p_own[i]))

        pre_far = mix(terms(None, swap_c(tie(other_y["11"], *p_own)), every))
        r_far = []
        held = pre_far
        for i, side in enumerate("AB"):
            held = mix(terms(tie(other_y["10" + side], held), None, every), [pre_far], col=i)
            r_far.append(swap_x(held))

        def finish_own(i):
            return mix(terms(blocks[0][0], same_far, late), [pre_same, r_own[i]], BF16, *split[i])

        out = jnp.zeros((2, half, width), BF16)
        r_own[0] = tie(r_own[0], held)
        held = finish_own(0)
        out = lax.dynamic_update_slice(out, held[None], (yi, 0, 0))
        base = held = mix(terms(None, swap_c(tie(other_y["01"], held)), every), [from_y])
        out_far = []
        for i, side in enumerate("AB"):
            held = mix(terms(tie(other_y["00" + side], held), None, every), [base, r_far[i]], BF16, col=i)
            out_far.append(swap_y(held))
        r_own[1] = tie(r_own[1], held)
        held = finish_own(1)
        out = lax.dynamic_update_slice(out, held[None], (yi, split[1][0], 0))
        for i, part in enumerate(out_far):
            out = lax.dynamic_update_slice(out, part[None], (1 - yi, 0, i * narrow))
        return out.reshape(batch, new, width), k_next, v_next

    row_spec = P("dp", None, ("tx", "tyz"))
    batch_spec = P(("dp", "tx", "tyz"), None, None)
    in_specs = (row_spec, P(("dp", "tx", "tyz")), batch_spec, batch_spec, P(("tx", "tyz")), P("tx", "tyz"), P("tx", None), P("tx", None), P("tx", "tyz"), P("tx", "tyz"), P("tyz", "tx"), P("tyz", "tx"))
    out_specs = (row_spec, batch_spec, batch_spec)

    return jax.shard_map(local_layer, mesh=mesh, in_specs=in_specs, out_specs=out_specs, check_vma=False)
```

```python
import functools

import jax
import jax.numpy as jnp
from jax import lax
from jax.experimental import pallas as pl
from jax.experimental.pallas import tpu as pltpu
from jax.sharding import PartitionSpec as P

LN_EPS = 1e-6
ROPE_BASE = 10000.0
BF16 = jnp.bfloat16
F32 = jnp.float32


def swap(axis, pairs):
    return lambda a: lax.ppermute(a, axis, pairs)


swap_y = swap("tx", [(0, 1), (1, 0)])
swap_x = swap("tyz", [(0, 2), (2, 0), (1, 3), (3, 1)])
swap_c = swap("tyz", [(0, 1), (1, 0), (2, 3), (3, 2)])


def pick(arr, index):
    return lax.dynamic_index_in_dim(arr, index, axis=0, keepdims=False)


def norm_kernel(offs_ref, *refs):
    pieces, gain_ref, out_ref = refs[:8], refs[8], refs[9]
    width = pieces[0].shape[1]
    total = 8 * width
    xs = [p[...].astype(F32) for p in pieces]
    s1 = sum(jnp.sum(v, axis=-1, keepdims=True) for v in xs)
    s2 = sum(jnp.sum(v * v, axis=-1, keepdims=True) for v in xs)
    mean = s1 / total
    var = s2 / total - mean * mean
    inv = lax.rsqrt(var + LN_EPS)
    for i, v in enumerate(xs):
        off = pl.multiple_of(offs_ref[i], width)
        out_ref[:, pl.ds(off, width)] = ((v - mean) * inv * gain_ref[i : i + 1, :]).astype(BF16)


def layer_norm(pieces, gains, offs):
    tokens, width = pieces[0].shape
    blk = 256
    return pl.pallas_call(
        norm_kernel,
        grid_spec=pltpu.PrefetchScalarGridSpec(
            num_scalar_prefetch=1,
            grid=(tokens // blk,),
            in_specs=[pl.BlockSpec((blk, width), lambda i, o: (i, 0))] * 8 + [pl.BlockSpec((8, width), lambda i, o: (0, 0))],
            out_specs=pl.BlockSpec((blk, 8 * width), lambda i, o: (i, 0)),
        ),
        out_shape=jax.ShapeDtypeStruct((tokens, 8 * width), BF16),
        cost_estimate=pl.CostEstimate(flops=20 * tokens * 8 * width, bytes_accessed=32 * tokens * width, transcendentals=tokens),
        name="norm",
    )(offs, *pieces, gains)


def rope(t, cos_t, sin_t):
    t = t.astype(F32)
    return (t * cos_t + pltpu.roll(t, t.shape[-1] // 2, 1) * sin_t).astype(BF16)


def attn_kernel(len_ref, q0, q1, q2, q3, kv_ref, cos_ref, sin_ref, kc_ref, vc_ref, o0, o1, o2, o3, kn_ref, vn_ref, qs):
    new = kv_ref.shape[0]
    cache = kc_ref.shape[1]
    dim = kc_ref.shape[2]
    length = len_ref[pl.program_id(0)]
    cos_t, sin_t = cos_ref[...], sin_ref[...]
    win = new + 32
    kn_ref[...] = kc_ref[...]
    vn_ref[...] = vc_ref[...]
    base = pl.multiple_of(jnp.minimum((length // 16) * 16, cache - win), 16)
    rows = lax.broadcasted_iota(jnp.int32, (win, new), 0) + (base - length)
    hot = (rows == lax.broadcasted_iota(jnp.int32, (win, new), 1)).astype(BF16)
    key_rot = rope(kv_ref[:, :dim], cos_t, sin_t)
    r = lax.broadcasted_iota(jnp.int32, (win, dim), 0) + (base - length)
    fresh = (r >= 0) & (r < new)
    k_win = jnp.dot(hot, key_rot, preferred_element_type=F32)
    v_win = jnp.dot(hot, kv_ref[:, dim:], preferred_element_type=F32)
    sl = pl.ds(base, win)
    kn_ref[0, sl, :] = jnp.where(fresh, k_win, kc_ref[0, sl, :].astype(F32)).astype(BF16)
    vn_ref[0, sl, :] = jnp.where(fresh, v_win, vc_ref[0, sl, :].astype(F32)).astype(BF16)

    q_refs, o_refs = (q0, q1, q2, q3), (o0, o1, o2, o3)
    hpg = q0.shape[1] // dim
    for g in range(4):
        for h in range(hpg):
            qs[g * hpg * new + h * new : g * hpg * new + (h + 1) * new, :] = rope(q_refs[g][:, h * dim : (h + 1) * dim], cos_t, sin_t)

    def attend(keys):
        @pl.loop(0, 4)
        def _(g):
            group = pl.ds(pl.multiple_of(g * hpg * new, hpg * new), hpg * new)
            q = qs[group, :]
            s = lax.dot_general(q, kn_ref[0, :keys, :], (((1,), (1,)), ((), ())), preferred_element_type=F32)
            s = s * (dim ** -0.5)
            tok = lax.broadcasted_iota(jnp.int32, (hpg * new, keys), 0) % new
            pos = lax.broadcasted_iota(jnp.int32, (hpg * new, keys), 1)
            s = jnp.where(pos - tok <= length, s, -1e30)
            e = jnp.exp(s - jnp.max(s, axis=-1, keepdims=True))
            p = (e * (1.0 / jnp.sum(e, axis=-1, keepdims=True))).astype(BF16)
            qs[group, :] = jnp.dot(p, vn_ref[0, :keys, :], preferred_element_type=F32).astype(BF16)

    step = 256
    need = (length + new + step - 1) // step
    sizes = list(range(5, cache // step + 1))
    for n in sizes:
        cond = need <= n if n == sizes[0] else need == n
        pl.when(cond)(functools.partial(attend, n * step))
    for g in range(4):
        for h in range(hpg):
            o_refs[g][:, h * dim : (h + 1) * dim] = qs[(g * hpg + h) * new : (g * hpg + h + 1) * new, :]


def attention(lengths, qs, kv, cos_t, sin_t, k_cache, v_cache):
    rows, cache, dim = k_cache.shape
    new = kv.shape[0] // rows
    qw = qs[0].shape[1]
    tok = lambda w: pl.BlockSpec((new, w), lambda b, L: (b, 0))
    row = pl.BlockSpec((1, cache, dim), lambda b, L: (b, 0, 0))
    heads = 4 * qw // dim
    return pl.pallas_call(
        attn_kernel,
        grid_spec=pltpu.PrefetchScalarGridSpec(
            num_scalar_prefetch=1,
            grid=(rows,),
            in_specs=[tok(qw)] * 4 + [tok(2 * dim), tok(dim), tok(dim), row, row],
            out_specs=[tok(qw)] * 4 + [row, row],
            scratch_shapes=[pltpu.VMEM((heads * new, dim), BF16)],
        ),
        out_shape=[jax.ShapeDtypeStruct((rows * new, qw), BF16)] * 4 + [jax.ShapeDtypeStruct(k_cache.shape, BF16)] * 2,
        cost_estimate=pl.CostEstimate(
            flops=8 * rows * heads * new * cache * dim, bytes_accessed=8 * rows * cache * dim, transcendentals=rows * heads * new * cache
        ),
        name="attn",
    )(lengths, *qs, kv, cos_t, sin_t, k_cache, v_cache)


def glu_kernel(h_ref, near_w, far_w, a_ref):
    depth = near_w.shape[1]
    near, far = h_ref[:, :depth], h_ref[:, depth:]
    gate = jnp.dot(near, near_w[0], preferred_element_type=F32) + jnp.dot(far, far_w[0], preferred_element_type=F32)
    up = jnp.dot(near, near_w[1], preferred_element_type=F32) + jnp.dot(far, far_w[1], preferred_element_type=F32)
    a_ref[...] = (gate / (1.0 + jnp.exp(-gate)) * up).astype(BF16)


def glu(h, near_w, far_w):
    tokens, depth = h.shape
    cols = near_w.shape[2]
    blk = 512
    w = pl.BlockSpec(near_w.shape, lambda i: (0, 0, 0))
    return pl.pallas_call(
        glu_kernel,
        grid=(tokens // blk,),
        in_specs=[pl.BlockSpec((blk, depth), lambda i: (i, 0)), w, w],
        out_specs=pl.BlockSpec((blk, cols), lambda i: (i, 0)),
        out_shape=jax.ShapeDtypeStruct((tokens, cols), BF16),
        cost_estimate=pl.CostEstimate(flops=4 * tokens * depth * cols, bytes_accessed=2 * tokens * (depth + cols) + 4 * depth * cols, transcendentals=tokens * cols),
        name="glu",
    )(h, near_w, far_w)


def mix_kernel(plan, n_lhs, n_w, *refs):
    lhs, ws, adds, out_ref = refs[:n_lhs], refs[n_lhs : n_lhs + n_w], refs[n_lhs + n_w : -1], refs[-1]
    total = None
    for l, (w, row) in zip(lhs, plan):
        part = jnp.dot(l[...], ws[w][row : row + l.shape[1], :], preferred_element_type=F32)
        total = part if total is None else total + part
    for t in adds:
        total = total + t[...].astype(F32)
    out_ref[...] = total.astype(out_ref.dtype)


def mix(terms, adds=(), dtype=F32, start=0, tokens=None, col=0):
    ws, plan = [], []
    for _, w, row in terms:
        found = [i for i, v in enumerate(ws) if v is w]
        if not found:
            ws.append(w)
        plan.append((found[0] if found else len(ws) - 1, row))
    lhs = [t[0] for t in terms]
    tokens = lhs[0].shape[0] if tokens is None else tokens
    cols = ws[0].shape[1]
    blk = 512
    first = start // blk
    tok = lambda w: pl.BlockSpec((blk, w), lambda i: (i + first, 0))
    depth = sum(l.shape[1] for l in lhs)
    add_specs = [pl.BlockSpec((blk, cols), lambda i, f=first * (t.shape[0] != tokens), c=col * (t.shape[1] != cols): (i + f, c)) for t in adds]
    return pl.pallas_call(
        functools.partial(mix_kernel, plan, len(lhs), len(ws)),
        grid=(tokens // blk,),
        in_specs=[tok(l.shape[1]) for l in lhs] + [pl.BlockSpec(w.shape, lambda i: (0, 0)) for w in ws] + add_specs,
        out_specs=pl.BlockSpec((blk, cols), lambda i: (i, 0)),
        out_shape=jax.ShapeDtypeStruct((tokens, cols), dtype),
        cost_estimate=pl.CostEstimate(flops=2 * tokens * depth * cols, bytes_accessed=2 * depth * (tokens + cols), transcendentals=0),
        name="mix",
    )(*lhs, *ws, *adds)


BLOCK_ORDER = ["11", "10A", "10B", "01", "00A", "00B"]


def tie(value, *others):
    return lax.optimization_barrier((value, *others))[0]


def solution(mesh):
    def local_layer(hidden, lengths, k_cache, v_cache, ln_gain, w_query, w_key, w_value, w_gate, w_up, w_down, w_out):
        batch, new, width = hidden.shape
        rows_own, _, dim = k_cache.shape
        yi = lax.axis_index("tx")
        ti = lax.axis_index("tyz")
        xi, ci = ti // 2, ti % 2
        half = batch * new // 2
        own_tok = rows_own * new

        g = ln_gain.reshape(1, width)
        g = jnp.concatenate([g, swap_y(g)], 0)
        g = jnp.concatenate([g, swap_x(g)], 0)
        g = jnp.concatenate([g, swap_c(g)], 0)
        hid2 = hidden.reshape(2, half, width)
        other = pick(hid2, 1 - yi)
        mine = pick(tie(hid2, other), yi)
        from_y = swap_y(other)
        mine_x = swap_x(mine)
        from_yx = swap_x(from_y)
        near = [mine, from_y, mine_x, from_yx]
        far = [swap_c(near[0])] + [swap_c(p) for p in near[1:]]
        offs = []
        for cr in range(2):
            for xr in range(2):
                for yr in range(2):
                    offs.append(width * (4 * yr + 2 * (xr ^ xi) + (cr ^ ci)))
        h = layer_norm(near + far, g, jnp.stack(offs).astype(jnp.int32))

        kv_rows = w_key.shape[0] // 4
        w_kv = jnp.concatenate([w_key, w_value], axis=1)
        ordered = lambda pair, i, axis: jnp.where(i == 0, jnp.stack(pair, axis), jnp.stack(pair[::-1], axis))
        kv_part = swap_y(lax.dynamic_slice_in_dim(w_kv, ti * kv_rows, kv_rows, 0))
        kv_pair = ordered([kv_part, swap_x(kv_part)], xi, 0)
        kv_far = ordered([kv_pair, swap_c(kv_pair)], ci, 1).reshape(w_kv.shape)
        q_far = swap_y(w_query)

        q = mix([(h, jnp.concatenate([w_query, q_far], 0), 0)], dtype=BF16)
        h_own = lax.dynamic_slice_in_dim(h, ti * own_tok, own_tok, 0)
        kv = jnp.dot(h_own, jnp.concatenate([w_kv, kv_far], 0), preferred_element_type=F32).astype(BF16)

        q4 = q.reshape(2, 2, own_tok, q.shape[1])
        q_back = swap_x(pick(q4, 1 - xi))

        chunks = 4
        cw = w_gate.shape[1] // chunks
        near_ws = [jnp.stack([w[:, j * cw : (j + 1) * cw] for w in (w_gate, w_up)]) for j in range(chunks)]
        far_ws = [swap_y(w) for w in near_ws]
        a_own = [glu(h, near_ws[0], far_ws[0])]
        q_back = tie(q_back, a_own[0])
        q_x = [pick(q4, xi), q_back]
        q_c = [pick(v, ci) for v in q_x] + [swap_c(pick(v, 1 - ci)) for v in q_x]

        half_dim = dim // 2
        inv_freq = ROPE_BASE ** (-2.0 * jnp.arange(half_dim, dtype=F32) / dim)
        positions = (lengths[:, None] + jnp.arange(new, dtype=jnp.int32)[None, :]).reshape(own_tok)
        angles = positions.astype(F32)[:, None] * inv_freq
        cos_t, sin_t = jnp.cos(angles), jnp.sin(angles)
        cos_t = jnp.concatenate([cos_t, cos_t], -1)
        sin_t = jnp.concatenate([-sin_t, sin_t], -1)
        o0, o1, o2, o3, k_next, v_next = attention(lengths, q_c, kv, cos_t, sin_t, k_cache, v_cache)

        keep = [o0, swap_c(o2)]
        send = swap_x(jnp.stack([o1, swap_c(o3)]))
        flip = lambda pair, i: jnp.where(i == 0, jnp.stack(pair), jnp.stack(pair[::-1]))
        o_rows = flip([flip(keep, ci), jnp.where(ci == 0, send, send[::-1])], xi)
        o_own = o_rows.reshape(half, -1)
        o_far = swap_c(o_own)
        o_far = swap_c(o_own)

        for j in range(1, chunks - 1):
            a_own.append(glu(h, near_ws[j], tie(far_ws[j], a_own[-1], o0)))
        a_far = [swap_c(v) for v in a_own]

        def block(xr, cr):
            col = (2 * (xi ^ xr) + (ci ^ cr)) * width
            return jnp.concatenate([lax.dynamic_slice_in_dim(w, col, width, 1) for w in (w_down, w_out)], 0)

        blocks = [[block(xr, cr) for cr in range(2)] for xr in range(2)]
        narrow = width // 2
        other_y = {}
        for name in BLOCK_ORDER:
            b = blocks[int(name[0])][int(name[1])]
            if name[2:]:
                col = "AB".index(name[2]) * narrow
                b = b[:, col : col + narrow]
            other_y[name] = swap_y(b)

        def terms(near_w, far_w, which):
            out = []
            for a_part, o_part, w in ((a_own, o_own, near_w), (a_far, o_far, far_w)):
                if w is not None:
                    out += [(o_part, w, chunks * cw) if k == "o" else (a_part[k], w, k * cw) for k in which]
            return out

        early, late, every = [*range(chunks - 1), "o"], [chunks - 1], [*range(chunks), "o"]
        split = (0, 3 * half // 4), (3 * half // 4, half // 4)

        cross_far, same_far = swap_c(blocks[1][1]), swap_c(blocks[0][1])
        pre_cross = mix(terms(blocks[1][0], cross_far, early))
        pre_same = mix(terms(tie(blocks[0][0], pre_cross), same_far, early), [mine])
        a_own.append(glu(h, near_ws[-1], tie(far_ws[-1], pre_same)))
        a_far.append(swap_c(a_own[-1]))
        p_own, r_own = [], []
        for i, span in enumerate(split):
            p_own.append(mix(terms(blocks[1][0], cross_far, late), [pre_cross], F32, *span))
            r_own.append(swap_x(p_own[i]))

        pre_far = mix(terms(None, swap_c(tie(other_y["11"], *p_own)), every))
        r_far = []
        held = pre_far
        for i, side in enumerate("AB"):
            held = mix(terms(tie(other_y["10" + side], held), None, every), [pre_far], col=i)
            r_far.append(swap_x(held))

        def finish_own(i):
            return mix(terms(blocks[0][0], same_far, late), [pre_same, r_own[i]], BF16, *split[i])

        out = jnp.zeros((2, half, width), BF16)
        r_own[0] = tie(r_own[0], held)
        held = finish_own(0)
        out = lax.dynamic_update_slice(out, held[None], (yi, 0, 0))
        base = held = mix(terms(None, swap_c(tie(other_y["01"], held)), every), [from_y])
        out_far = []
        for i, side in enumerate("AB"):
            held = mix(terms(tie(other_y["00" + side], held), None, every), [base, r_far[i]], BF16, col=i)
            out_far.append(swap_y(held))
        r_own[1] = tie(r_own[1], held)
        held = finish_own(1)
        out = lax.dynamic_update_slice(out, held[None], (yi, split[1][0], 0))
        for i, part in enumerate(out_far):
            out = lax.dynamic_update_slice(out, part[None], (1 - yi, 0, i * narrow))
        return out.reshape(batch, new, width), k_next, v_next

    row_spec = P("dp", None, ("tx", "tyz"))
    batch_spec = P(("dp", "tx", "tyz"), None, None)
    in_specs = (row_spec, P(("dp", "tx", "tyz")), batch_spec, batch_spec, P(("tx", "tyz")), P("tx", "tyz"), P("tx", None), P("tx", None), P("tx", "tyz"), P("tx", "tyz"), P("tyz", "tx"), P("tyz", "tx"))
    out_specs = (row_spec, batch_spec, batch_spec)

    return jax.shard_map(local_layer, mesh=mesh, in_specs=in_specs, out_specs=out_specs, check_vma=False)
```

```python
import functools

import jax
import jax.numpy as jnp
from jax import lax
from jax.experimental import pallas as pl
from jax.experimental.pallas import tpu as pltpu
from jax.sharding import PartitionSpec as P

LN_EPS = 1e-6
ROPE_BASE = 10000.0
BF16 = jnp.bfloat16
F32 = jnp.float32


def swap(axis, pairs):
    return lambda a: lax.ppermute(a, axis, pairs)


swap_y = swap("tx", [(0, 1), (1, 0)])
swap_x = swap("tyz", [(0, 2), (2, 0), (1, 3), (3, 1)])
swap_c = swap("tyz", [(0, 1), (1, 0), (2, 3), (3, 2)])


def pick(arr, index):
    return lax.dynamic_index_in_dim(arr, index, axis=0, keepdims=False)


def norm_kernel(offs_ref, *refs):
    pieces, gain_ref, out_ref = refs[:8], refs[8], refs[9]
    width = pieces[0].shape[1]
    total = 8 * width
    xs = [p[...].astype(F32) for p in pieces]
    s1 = sum(jnp.sum(v, axis=-1, keepdims=True) for v in xs)
    s2 = sum(jnp.sum(v * v, axis=-1, keepdims=True) for v in xs)
    mean = s1 / total
    var = s2 / total - mean * mean
    inv = lax.rsqrt(var + LN_EPS)
    for i, v in enumerate(xs):
        off = pl.multiple_of(offs_ref[i], width)
        out_ref[:, pl.ds(off, width)] = ((v - mean) * inv * gain_ref[i : i + 1, :]).astype(BF16)


def layer_norm(pieces, gains, offs):
    tokens, width = pieces[0].shape
    blk = 256
    return pl.pallas_call(
        norm_kernel,
        grid_spec=pltpu.PrefetchScalarGridSpec(
            num_scalar_prefetch=1,
            grid=(tokens // blk,),
            in_specs=[pl.BlockSpec((blk, width), lambda i, o: (i, 0))] * 8 + [pl.BlockSpec((8, width), lambda i, o: (0, 0))],
            out_specs=pl.BlockSpec((blk, 8 * width), lambda i, o: (i, 0)),
        ),
        out_shape=jax.ShapeDtypeStruct((tokens, 8 * width), BF16),
        cost_estimate=pl.CostEstimate(flops=20 * tokens * 8 * width, bytes_accessed=32 * tokens * width, transcendentals=tokens),
        name="norm",
    )(offs, *pieces, gains)


def rope(t, cos_t, sin_t):
    t = t.astype(F32)
    return (t * cos_t + pltpu.roll(t, t.shape[-1] // 2, 1) * sin_t).astype(BF16)


def attn_kernel(len_ref, q0, q1, q2, q3, kv_ref, cos_ref, sin_ref, kc_ref, vc_ref, o0, o1, o2, o3, kn_ref, vn_ref, qs):
    new = kv_ref.shape[0]
    cache = kc_ref.shape[1]
    dim = kc_ref.shape[2]
    length = len_ref[pl.program_id(0)]
    cos_t, sin_t = cos_ref[...], sin_ref[...]
    win = new + 32
    kn_ref[...] = kc_ref[...]
    vn_ref[...] = vc_ref[...]
    base = pl.multiple_of(jnp.minimum((length // 16) * 16, cache - win), 16)
    rows = lax.broadcasted_iota(jnp.int32, (win, new), 0) + (base - length)
    hot = (rows == lax.broadcasted_iota(jnp.int32, (win, new), 1)).astype(BF16)
    key_rot = rope(kv_ref[:, :dim], cos_t, sin_t)
    r = lax.broadcasted_iota(jnp.int32, (win, dim), 0) + (base - length)
    fresh = (r >= 0) & (r < new)
    k_win = jnp.dot(hot, key_rot, preferred_element_type=F32)
    v_win = jnp.dot(hot, kv_ref[:, dim:], preferred_element_type=F32)
    sl = pl.ds(base, win)
    kn_ref[0, sl, :] = jnp.where(fresh, k_win, kc_ref[0, sl, :].astype(F32)).astype(BF16)
    vn_ref[0, sl, :] = jnp.where(fresh, v_win, vc_ref[0, sl, :].astype(F32)).astype(BF16)

    q_refs, o_refs = (q0, q1, q2, q3), (o0, o1, o2, o3)
    hpg = q0.shape[1] // dim
    for g in range(4):
        for h in range(hpg):
            qs[g * hpg * new + h * new : g * hpg * new + (h + 1) * new, :] = rope(q_refs[g][:, h * dim : (h + 1) * dim], cos_t, sin_t)

    def attend(keys):
        @pl.loop(0, 4)
        def _(g):
            group = pl.ds(pl.multiple_of(g * hpg * new, hpg * new), hpg * new)
            q = qs[group, :]
            s = lax.dot_general(q, kn_ref[0, :keys, :], (((1,), (1,)), ((), ())), preferred_element_type=F32)
            s = s * (dim ** -0.5)
            tok = lax.broadcasted_iota(jnp.int32, (hpg * new, keys), 0) % new
            pos = lax.broadcasted_iota(jnp.int32, (hpg * new, keys), 1)
            s = jnp.where(pos - tok <= length, s, -1e30)
            e = jnp.exp(s - jnp.max(s, axis=-1, keepdims=True))
            p = (e * (1.0 / jnp.sum(e, axis=-1, keepdims=True))).astype(BF16)
            qs[group, :] = jnp.dot(p, vn_ref[0, :keys, :], preferred_element_type=F32).astype(BF16)

    step = 256
    need = (length + new + step - 1) // step
    sizes = list(range(5, cache // step + 1))
    for n in sizes:
        cond = need <= n if n == sizes[0] else need == n
        pl.when(cond)(functools.partial(attend, n * step))
    for g in range(4):
        for h in range(hpg):
            o_refs[g][:, h * dim : (h + 1) * dim] = qs[(g * hpg + h) * new : (g * hpg + h + 1) * new, :]


def attention(lengths, qs, kv, cos_t, sin_t, k_cache, v_cache):
    rows, cache, dim = k_cache.shape
    new = kv.shape[0] // rows
    qw = qs[0].shape[1]
    tok = lambda w: pl.BlockSpec((new, w), lambda b, L: (b, 0))
    row = pl.BlockSpec((1, cache, dim), lambda b, L: (b, 0, 0))
    heads = 4 * qw // dim
    return pl.pallas_call(
        attn_kernel,
        grid_spec=pltpu.PrefetchScalarGridSpec(
            num_scalar_prefetch=1,
            grid=(rows,),
            in_specs=[tok(qw)] * 4 + [tok(2 * dim), tok(dim), tok(dim), row, row],
            out_specs=[tok(qw)] * 4 + [row, row],
            scratch_shapes=[pltpu.VMEM((heads * new, dim), BF16)],
        ),
        out_shape=[jax.ShapeDtypeStruct((rows * new, qw), BF16)] * 4 + [jax.ShapeDtypeStruct(k_cache.shape, BF16)] * 2,
        cost_estimate=pl.CostEstimate(
            flops=8 * rows * heads * new * cache * dim, bytes_accessed=8 * rows * cache * dim, transcendentals=rows * heads * new * cache
        ),
        name="attn",
    )(lengths, *qs, kv, cos_t, sin_t, k_cache, v_cache)


def glu_kernel(h_ref, near_w, far_w, a_ref):
    depth = near_w.shape[1]
    near, far = h_ref[:, :depth], h_ref[:, depth:]
    gate = jnp.dot(near, near_w[0], preferred_element_type=F32) + jnp.dot(far, far_w[0], preferred_element_type=F32)
    up = jnp.dot(near, near_w[1], preferred_element_type=F32) + jnp.dot(far, far_w[1], preferred_element_type=F32)
    a_ref[...] = (gate / (1.0 + jnp.exp(-gate)) * up).astype(BF16)


def glu(h, near_w, far_w):
    tokens, depth = h.shape
    cols = near_w.shape[2]
    blk = 512
    w = pl.BlockSpec(near_w.shape, lambda i: (0, 0, 0))
    return pl.pallas_call(
        glu_kernel,
        grid=(tokens // blk,),
        in_specs=[pl.BlockSpec((blk, depth), lambda i: (i, 0)), w, w],
        out_specs=pl.BlockSpec((blk, cols), lambda i: (i, 0)),
        out_shape=jax.ShapeDtypeStruct((tokens, cols), BF16),
        cost_estimate=pl.CostEstimate(flops=4 * tokens * depth * cols, bytes_accessed=2 * tokens * (depth + cols) + 4 * depth * cols, transcendentals=tokens * cols),
        name="glu",
    )(h, near_w, far_w)


def project_kernel(h_ref, *refs):
    total, row = None, 0
    for w in refs[:-1]:
        part = jnp.dot(h_ref[:, row : row + w.shape[0]], w[...], preferred_element_type=F32)
        total = part if total is None else total + part
        row += w.shape[0]
    refs[-1][...] = total.astype(BF16)


def project(h, ws):
    tokens, depth = h.shape
    cols = ws[0].shape[1]
    blk = 512
    return pl.pallas_call(
        project_kernel,
        grid=(tokens // blk,),
        in_specs=[pl.BlockSpec((blk, depth), lambda i: (i, 0))] + [pl.BlockSpec(w.shape, lambda i: (0, 0)) for w in ws],
        out_specs=pl.BlockSpec((blk, cols), lambda i: (i, 0)),
        out_shape=jax.ShapeDtypeStruct((tokens, cols), BF16),
        cost_estimate=pl.CostEstimate(flops=2 * tokens * depth * cols, bytes_accessed=2 * depth * (tokens + cols), transcendentals=0),
        name="project",
    )(h, *ws)


def mix_kernel(plan, n_lhs, n_w, *refs):
    lhs, ws, adds, out_ref = refs[:n_lhs], refs[n_lhs : n_lhs + n_w], refs[n_lhs + n_w : -1], refs[-1]
    total = None
    for l, (w, row) in zip(lhs, plan):
        part = jnp.dot(l[...], ws[w][row : row + l.shape[1], :], preferred_element_type=F32)
        total = part if total is None else total + part
    for t in adds:
        total = total + t[...].astype(F32)
    out_ref[...] = total.astype(out_ref.dtype)


def mix(terms, adds=(), dtype=F32, start=0, tokens=None, col=0):
    ws, plan = [], []
    for _, w, row in terms:
        found = [i for i, v in enumerate(ws) if v is w]
        if not found:
            ws.append(w)
        plan.append((found[0] if found else len(ws) - 1, row))
    lhs = [t[0] for t in terms]
    tokens = lhs[0].shape[0] if tokens is None else tokens
    cols = ws[0].shape[1]
    blk = 512
    first = start // blk
    tok = lambda w: pl.BlockSpec((blk, w), lambda i: (i + first, 0))
    depth = sum(l.shape[1] for l in lhs)
    add_specs = [pl.BlockSpec((blk, cols), lambda i, f=first * (t.shape[0] != tokens), c=col * (t.shape[1] != cols): (i + f, c)) for t in adds]
    return pl.pallas_call(
        functools.partial(mix_kernel, plan, len(lhs), len(ws)),
        grid=(tokens // blk,),
        in_specs=[tok(l.shape[1]) for l in lhs] + [pl.BlockSpec(w.shape, lambda i: (0, 0)) for w in ws] + add_specs,
        out_specs=pl.BlockSpec((blk, cols), lambda i: (i, 0)),
        out_shape=jax.ShapeDtypeStruct((tokens, cols), dtype),
        cost_estimate=pl.CostEstimate(flops=2 * tokens * depth * cols, bytes_accessed=2 * depth * (tokens + cols), transcendentals=0),
        name="mix",
    )(*lhs, *ws, *adds)


BLOCK_ORDER = ["11", "10A", "10B", "01", "00A", "00B"]


def tie(value, *others):
    return lax.optimization_barrier((value, *others))[0]


def solution(mesh):
    def local_layer(hidden, lengths, k_cache, v_cache, ln_gain, w_query, w_key, w_value, w_gate, w_up, w_down, w_out):
        batch, new, width = hidden.shape
        rows_own, _, dim = k_cache.shape
        yi = lax.axis_index("tx")
        ti = lax.axis_index("tyz")
        xi, ci = ti // 2, ti % 2
        half = batch * new // 2
        own_tok = rows_own * new

        g = ln_gain.reshape(1, width)
        g = jnp.concatenate([g, swap_y(g)], 0)
        g = jnp.concatenate([g, swap_x(g)], 0)
        g = jnp.concatenate([g, swap_c(g)], 0)
        hid2 = hidden.reshape(2, half, width)
        other = pick(hid2, 1 - yi)
        mine = pick(tie(hid2, other), yi)
        from_y = swap_y(other)
        mine_x = swap_x(mine)
        from_yx = swap_x(from_y)
        near = [mine, from_y, mine_x, from_yx]
        far = [swap_c(near[0])] + [swap_c(p) for p in near[1:]]
        offs = []
        for cr in range(2):
            for xr in range(2):
                for yr in range(2):
                    offs.append(width * (4 * yr + 2 * (xr ^ xi) + (cr ^ ci)))
        h = layer_norm(near + far, g, jnp.stack(offs).astype(jnp.int32))

        kv_rows = w_key.shape[0] // 4
        w_kv = jnp.concatenate([w_key, w_value], axis=1)
        ordered = lambda pair, i, axis: jnp.where(i == 0, jnp.stack(pair, axis), jnp.stack(pair[::-1], axis))
        kv_part = swap_y(lax.dynamic_slice_in_dim(w_kv, ti * kv_rows, kv_rows, 0))
        kv_pair = ordered([kv_part, swap_x(kv_part)], xi, 0)
        kv_far = ordered([kv_pair, swap_c(kv_pair)], ci, 1).reshape(w_kv.shape)
        lead = 256
        q_far = [swap_y(w_query[:lead]), swap_y(w_query[lead:])]

        q = project(h, [w_query, *q_far])
        h_own = lax.dynamic_slice_in_dim(h, ti * own_tok, own_tok, 0)
        kv = jnp.dot(h_own, jnp.concatenate([w_kv, kv_far], 0), preferred_element_type=F32).astype(BF16)

        q4 = q.reshape(2, 2, own_tok, q.shape[1])
        q_back = swap_x(pick(q4, 1 - xi))

        chunks = 4
        cw = w_gate.shape[1] // chunks
        near_ws = [jnp.stack([w[:, j * cw : (j + 1) * cw] for w in (w_gate, w_up)]) for j in range(chunks)]
        far_ws = [swap_y(w) for w in near_ws]
        a_own = [glu(h, near_ws[0], far_ws[0])]
        q_back = tie(q_back, a_own[0])
        q_x = [pick(q4, xi), q_back]
        q_c = [pick(v, ci) for v in q_x] + [swap_c(pick(v, 1 - ci)) for v in q_x]

        half_dim = dim // 2
        inv_freq = ROPE_BASE ** (-2.0 * jnp.arange(half_dim, dtype=F32) / dim)
        positions = (lengths[:, None] + jnp.arange(new, dtype=jnp.int32)[None, :]).reshape(own_tok)
        angles = positions.astype(F32)[:, None] * inv_freq
        cos_t, sin_t = jnp.cos(angles), jnp.sin(angles)
        cos_t = jnp.concatenate([cos_t, cos_t], -1)
        sin_t = jnp.concatenate([-sin_t, sin_t], -1)
        o0, o1, o2, o3, k_next, v_next = attention(lengths, q_c, kv, cos_t, sin_t, k_cache, v_cache)

        keep = [o0, swap_c(o2)]
        send = swap_x(jnp.stack([o1, swap_c(o3)]))
        flip = lambda pair, i: jnp.where(i == 0, jnp.stack(pair), jnp.stack(pair[::-1]))
        o_rows = flip([flip(keep, ci), jnp.where(ci == 0, send, send[::-1])], xi)
        o_own = o_rows.reshape(half, -1)
        o_far = swap_c(o_own)
        o_far = swap_c(o_own)

        for j in range(1, chunks - 1):
            a_own.append(glu(h, near_ws[j], tie(far_ws[j], a_own[-1], o0)))
        a_far = [swap_c(v) for v in a_own]

        def block(xr, cr):
            col = (2 * (xi ^ xr) + (ci ^ cr)) * width
            return jnp.concatenate([lax.dynamic_slice_in_dim(w, col, width, 1) for w in (w_down, w_out)], 0)

        blocks = [[block(xr, cr) for cr in range(2)] for xr in range(2)]
        narrow = width // 2
        other_y = {}
        for name in BLOCK_ORDER:
            b = blocks[int(name[0])][int(name[1])]
            if name[2:]:
                col = "AB".index(name[2]) * narrow
                b = b[:, col : col + narrow]
            other_y[name] = swap_y(b)

        def terms(near_w, far_w, which):
            out = []
            for a_part, o_part, w in ((a_own, o_own, near_w), (a_far, o_far, far_w)):
                if w is not None:
                    out += [(o_part, w, chunks * cw) if k == "o" else (a_part[k], w, k * cw) for k in which]
            return out

        early, late, every = [*range(chunks - 1), "o"], [chunks - 1], [*range(chunks), "o"]
        split = (0, 3 * half // 4), (3 * half // 4, half // 4)

        cross_far, same_far = swap_c(blocks[1][1]), swap_c(blocks[0][1])
        pre_cross = mix(terms(blocks[1][0], cross_far, early))
        pre_same = mix(terms(tie(blocks[0][0], pre_cross), same_far, early), [mine])
        a_own.append(glu(h, near_ws[-1], tie(far_ws[-1], pre_same)))
        a_far.append(swap_c(a_own[-1]))
        p_own, r_own = [], []
        for i, span in enumerate(split):
            p_own.append(mix(terms(blocks[1][0], cross_far, late), [pre_cross], F32, *span))
            r_own.append(swap_x(p_own[i]))

        pre_far = mix(terms(None, swap_c(tie(other_y["11"], *p_own)), every))
        r_far = []
        held = pre_far
        for i, side in enumerate("AB"):
            held = mix(terms(tie(other_y["10" + side], held), None, every), [pre_far], col=i)
            r_far.append(swap_x(held))

        def finish_own(i):
            return mix(terms(blocks[0][0], same_far, late), [pre_same, r_own[i]], BF16, *split[i])

        out = jnp.zeros((2, half, width), BF16)
        r_own[0] = tie(r_own[0], held)
        held = finish_own(0)
        out = lax.dynamic_update_slice(out, held[None], (yi, 0, 0))
        base = held = mix(terms(None, swap_c(tie(other_y["01"], held)), every), [from_y])
        out_far = []
        for i, side in enumerate("AB"):
            held = mix(terms(tie(other_y["00" + side], held), None, every), [base, r_far[i]], BF16, col=i)
            out_far.append(swap_y(held))
        r_own[1] = tie(r_own[1], held)
        held = finish_own(1)
        out = lax.dynamic_update_slice(out, held[None], (yi, split[1][0], 0))
        for i, part in enumerate(out_far):
            out = lax.dynamic_update_slice(out, part[None], (1 - yi, 0, i * narrow))
        return out.reshape(batch, new, width), k_next, v_next

    row_spec = P("dp", None, ("tx", "tyz"))
    batch_spec = P(("dp", "tx", "tyz"), None, None)
    in_specs = (row_spec, P(("dp", "tx", "tyz")), batch_spec, batch_spec, P(("tx", "tyz")), P("tx", "tyz"), P("tx", None), P("tx", None), P("tx", "tyz"), P("tx", "tyz"), P("tyz", "tx"), P("tyz", "tx"))
    out_specs = (row_spec, batch_spec, batch_spec)

    return jax.shard_map(local_layer, mesh=mesh, in_specs=in_specs, out_specs=out_specs, check_vma=False)
```

```python
import functools

import jax
import jax.numpy as jnp
from jax import lax
from jax.experimental import pallas as pl
from jax.experimental.pallas import tpu as pltpu
from jax.sharding import PartitionSpec as P

LN_EPS = 1e-6
ROPE_BASE = 10000.0
BF16 = jnp.bfloat16
F32 = jnp.float32


def swap(axis, pairs):
    return lambda a: lax.ppermute(a, axis, pairs)


swap_y = swap("tx", [(0, 1), (1, 0)])
swap_x = swap("tyz", [(0, 2), (2, 0), (1, 3), (3, 1)])
swap_c = swap("tyz", [(0, 1), (1, 0), (2, 3), (3, 2)])


def pick(arr, index):
    return lax.dynamic_index_in_dim(arr, index, axis=0, keepdims=False)


def norm_kernel(offs_ref, *refs):
    pieces, gain_ref, out_ref = refs[:8], refs[8], refs[9]
    width = pieces[0].shape[1]
    total = 8 * width
    xs = [p[...].astype(F32) for p in pieces]
    s1 = sum(jnp.sum(v, axis=-1, keepdims=True) for v in xs)
    s2 = sum(jnp.sum(v * v, axis=-1, keepdims=True) for v in xs)
    mean = s1 / total
    var = s2 / total - mean * mean
    inv = lax.rsqrt(var + LN_EPS)
    for i, v in enumerate(xs):
        off = pl.multiple_of(offs_ref[i], width)
        out_ref[:, pl.ds(off, width)] = ((v - mean) * inv * gain_ref[i : i + 1, :]).astype(BF16)


def layer_norm(pieces, gains, offs):
    tokens, width = pieces[0].shape
    blk = 256
    return pl.pallas_call(
        norm_kernel,
        grid_spec=pltpu.PrefetchScalarGridSpec(
            num_scalar_prefetch=1,
            grid=(tokens // blk,),
            in_specs=[pl.BlockSpec((blk, width), lambda i, o: (i, 0))] * 8 + [pl.BlockSpec((8, width), lambda i, o: (0, 0))],
            out_specs=pl.BlockSpec((blk, 8 * width), lambda i, o: (i, 0)),
        ),
        out_shape=jax.ShapeDtypeStruct((tokens, 8 * width), BF16),
        cost_estimate=pl.CostEstimate(flops=20 * tokens * 8 * width, bytes_accessed=32 * tokens * width, transcendentals=tokens),
        name="norm",
    )(offs, *pieces, gains)


def rope(t, cos_t, sin_t):
    t = t.astype(F32)
    return (t * cos_t + pltpu.roll(t, t.shape[-1] // 2, 1) * sin_t).astype(BF16)


def attn_kernel(len_ref, q0, q1, q2, q3, kv_ref, cos_ref, sin_ref, kc_ref, vc_ref, o0, o1, o2, o3, kn_ref, vn_ref, qs):
    new = kv_ref.shape[0]
    cache = kc_ref.shape[1]
    dim = kc_ref.shape[2]
    length = len_ref[pl.program_id(0)]
    cos_t, sin_t = cos_ref[...], sin_ref[...]
    win = new + 32
    kn_ref[...] = kc_ref[...]
    vn_ref[...] = vc_ref[...]
    base = pl.multiple_of(jnp.minimum((length // 16) * 16, cache - win), 16)
    rows = lax.broadcasted_iota(jnp.int32, (win, new), 0) + (base - length)
    hot = (rows == lax.broadcasted_iota(jnp.int32, (win, new), 1)).astype(BF16)
    key_rot = rope(kv_ref[:, :dim], cos_t, sin_t)
    r = lax.broadcasted_iota(jnp.int32, (win, dim), 0) + (base - length)
    fresh = (r >= 0) & (r < new)
    k_win = jnp.dot(hot, key_rot, preferred_element_type=F32)
    v_win = jnp.dot(hot, kv_ref[:, dim:], preferred_element_type=F32)
    sl = pl.ds(base, win)
    kn_ref[0, sl, :] = jnp.where(fresh, k_win, kc_ref[0, sl, :].astype(F32)).astype(BF16)
    vn_ref[0, sl, :] = jnp.where(fresh, v_win, vc_ref[0, sl, :].astype(F32)).astype(BF16)

    q_refs, o_refs = (q0, q1, q2, q3), (o0, o1, o2, o3)
    hpg = q0.shape[1] // dim
    for g in range(4):
        for h in range(hpg):
            qs[g * hpg * new + h * new : g * hpg * new + (h + 1) * new, :] = rope(q_refs[g][:, h * dim : (h + 1) * dim], cos_t, sin_t)

    def attend(keys):
        @pl.loop(0, 4)
        def _(g):
            group = pl.ds(pl.multiple_of(g * hpg * new, hpg * new), hpg * new)
            q = qs[group, :]
            s = lax.dot_general(q, kn_ref[0, :keys, :], (((1,), (1,)), ((), ())), preferred_element_type=F32)
            s = s * (dim ** -0.5)
            tok = lax.broadcasted_iota(jnp.int32, (hpg * new, keys), 0) % new
            pos = lax.broadcasted_iota(jnp.int32, (hpg * new, keys), 1)
            s = jnp.where(pos - tok <= length, s, -1e30)
            e = jnp.exp(s - jnp.max(s, axis=-1, keepdims=True))
            p = (e * (1.0 / jnp.sum(e, axis=-1, keepdims=True))).astype(BF16)
            qs[group, :] = jnp.dot(p, vn_ref[0, :keys, :], preferred_element_type=F32).astype(BF16)

    step = 256
    need = (length + new + step - 1) // step
    sizes = list(range(5, cache // step + 1))
    for n in sizes:
        cond = need <= n if n == sizes[0] else need == n
        pl.when(cond)(functools.partial(attend, n * step))
    for g in range(4):
        for h in range(hpg):
            o_refs[g][:, h * dim : (h + 1) * dim] = qs[(g * hpg + h) * new : (g * hpg + h + 1) * new, :]


def attention(lengths, qs, kv, cos_t, sin_t, k_cache, v_cache):
    rows, cache, dim = k_cache.shape
    new = kv.shape[0] // rows
    qw = qs[0].shape[1]
    tok = lambda w: pl.BlockSpec((new, w), lambda b, L: (b, 0))
    row = pl.BlockSpec((1, cache, dim), lambda b, L: (b, 0, 0))
    heads = 4 * qw // dim
    return pl.pallas_call(
        attn_kernel,
        grid_spec=pltpu.PrefetchScalarGridSpec(
            num_scalar_prefetch=1,
            grid=(rows,),
            in_specs=[tok(qw)] * 4 + [tok(2 * dim), tok(dim), tok(dim), row, row],
            out_specs=[tok(qw)] * 4 + [row, row],
            scratch_shapes=[pltpu.VMEM((heads * new, dim), BF16)],
        ),
        out_shape=[jax.ShapeDtypeStruct((rows * new, qw), BF16)] * 4 + [jax.ShapeDtypeStruct(k_cache.shape, BF16)] * 2,
        cost_estimate=pl.CostEstimate(
            flops=8 * rows * heads * new * cache * dim, bytes_accessed=8 * rows * cache * dim, transcendentals=rows * heads * new * cache
        ),
        name="attn",
    )(lengths, *qs, kv, cos_t, sin_t, k_cache, v_cache)


def glu_kernel(h_ref, near_w, far_w, a_ref):
    depth = near_w.shape[1]
    near, far = h_ref[:, :depth], h_ref[:, depth:]
    gate = jnp.dot(near, near_w[0], preferred_element_type=F32) + jnp.dot(far, far_w[0], preferred_element_type=F32)
    up = jnp.dot(near, near_w[1], preferred_element_type=F32) + jnp.dot(far, far_w[1], preferred_element_type=F32)
    a_ref[...] = (gate / (1.0 + jnp.exp(-gate)) * up).astype(BF16)


def glu(h, near_w, far_w):
    tokens, depth = h.shape
    cols = near_w.shape[2]
    blk = 512
    w = pl.BlockSpec(near_w.shape, lambda i: (0, 0, 0))
    return pl.pallas_call(
        glu_kernel,
        grid=(tokens // blk,),
        in_specs=[pl.BlockSpec((blk, depth), lambda i: (i, 0)), w, w],
        out_specs=pl.BlockSpec((blk, cols), lambda i: (i, 0)),
        out_shape=jax.ShapeDtypeStruct((tokens, cols), BF16),
        cost_estimate=pl.CostEstimate(flops=4 * tokens * depth * cols, bytes_accessed=2 * tokens * (depth + cols) + 4 * depth * cols, transcendentals=tokens * cols),
        name="glu",
    )(h, near_w, far_w)


def project_kernel(h_ref, *refs):
    total, row = None, 0
    for w in refs[:-1]:
        part = jnp.dot(h_ref[:, row : row + w.shape[0]], w[...], preferred_element_type=F32)
        total = part if total is None else total + part
        row += w.shape[0]
    refs[-1][...] = total.astype(BF16)


def project(h, ws):
    tokens, depth = h.shape
    cols = ws[0].shape[1]
    blk = 512
    return pl.pallas_call(
        project_kernel,
        grid=(tokens // blk,),
        in_specs=[pl.BlockSpec((blk, depth), lambda i: (i, 0))] + [pl.BlockSpec(w.shape, lambda i: (0, 0)) for w in ws],
        out_specs=pl.BlockSpec((blk, cols), lambda i: (i, 0)),
        out_shape=jax.ShapeDtypeStruct((tokens, cols), BF16),
        cost_estimate=pl.CostEstimate(flops=2 * tokens * depth * cols, bytes_accessed=2 * depth * (tokens + cols), transcendentals=0),
        name="project",
    )(h, *ws)


def mix_kernel(plan, n_lhs, n_w, *refs):
    lhs, ws, adds, out_ref = refs[:n_lhs], refs[n_lhs : n_lhs + n_w], refs[n_lhs + n_w : -1], refs[-1]
    total = None
    for l, (w, row) in zip(lhs, plan):
        part = jnp.dot(l[...], ws[w][row : row + l.shape[1], :], preferred_element_type=F32)
        total = part if total is None else total + part
    for t in adds:
        total = total + t[...].astype(F32)
    out_ref[...] = total.astype(out_ref.dtype)


def mix(terms, adds=(), dtype=F32, start=0, tokens=None, col=0):
    ws, plan = [], []
    for _, w, row in terms:
        found = [i for i, v in enumerate(ws) if v is w]
        if not found:
            ws.append(w)
        plan.append((found[0] if found else len(ws) - 1, row))
    lhs = [t[0] for t in terms]
    tokens = lhs[0].shape[0] if tokens is None else tokens
    cols = ws[0].shape[1]
    blk = 512
    first = start // blk
    tok = lambda w: pl.BlockSpec((blk, w), lambda i: (i + first, 0))
    depth = sum(l.shape[1] for l in lhs)
    add_specs = [pl.BlockSpec((blk, cols), lambda i, f=first * (t.shape[0] != tokens), c=col * (t.shape[1] != cols): (i + f, c)) for t in adds]
    return pl.pallas_call(
        functools.partial(mix_kernel, plan, len(lhs), len(ws)),
        grid=(tokens // blk,),
        in_specs=[tok(l.shape[1]) for l in lhs] + [pl.BlockSpec(w.shape, lambda i: (0, 0)) for w in ws] + add_specs,
        out_specs=pl.BlockSpec((blk, cols), lambda i: (i, 0)),
        out_shape=jax.ShapeDtypeStruct((tokens, cols), dtype),
        cost_estimate=pl.CostEstimate(flops=2 * tokens * depth * cols, bytes_accessed=2 * depth * (tokens + cols), transcendentals=0),
        name="mix",
    )(*lhs, *ws, *adds)


BLOCK_ORDER = ["11", "10A", "10B", "01", "00A", "00B"]


def tie(value, *others):
    return lax.optimization_barrier((value, *others))[0]


def solution(mesh):
    def local_layer(hidden, lengths, k_cache, v_cache, ln_gain, w_query, w_key, w_value, w_gate, w_up, w_down, w_out):
        batch, new, width = hidden.shape
        rows_own, _, dim = k_cache.shape
        yi = lax.axis_index("tx")
        ti = lax.axis_index("tyz")
        xi, ci = ti // 2, ti % 2
        half = batch * new // 2
        own_tok = rows_own * new

        g = ln_gain.reshape(1, width)
        g = jnp.concatenate([g, swap_y(g)], 0)
        g = jnp.concatenate([g, swap_x(g)], 0)
        g = jnp.concatenate([g, swap_c(g)], 0)
        hid2 = hidden.reshape(2, half, width)
        other = pick(hid2, 1 - yi)
        mine = pick(tie(hid2, other), yi)
        from_y = swap_y(other)
        mine_x = swap_x(mine)
        from_yx = swap_x(from_y)
        near = [mine, from_y, mine_x, from_yx]
        far = [swap_c(near[0])] + [swap_c(p) for p in near[1:]]
        offs = []
        for cr in range(2):
            for xr in range(2):
                for yr in range(2):
                    offs.append(width * (4 * yr + 2 * (xr ^ xi) + (cr ^ ci)))
        h = layer_norm(near + far, g, jnp.stack(offs).astype(jnp.int32))

        kv_rows = w_key.shape[0] // 4
        w_kv = jnp.concatenate([w_key, w_value], axis=1)
        ordered = lambda pair, i, axis: jnp.where(i == 0, jnp.stack(pair, axis), jnp.stack(pair[::-1], axis))
        kv_part = swap_y(lax.dynamic_slice_in_dim(w_kv, ti * kv_rows, kv_rows, 0))
        kv_pair = ordered([kv_part, swap_x(kv_part)], xi, 0)
        kv_far = ordered([kv_pair, swap_c(kv_pair)], ci, 1).reshape(w_kv.shape)
        q_far = swap_y(w_query)

        q = project(h, [w_query, q_far])
        h_own = lax.dynamic_slice_in_dim(h, ti * own_tok, own_tok, 0)
        kv = jnp.dot(h_own, jnp.concatenate([w_kv, kv_far], 0), preferred_element_type=F32).astype(BF16)

        q4 = q.reshape(2, 2, own_tok, q.shape[1])
        q_back = swap_x(pick(q4, 1 - xi))

        chunks = 4
        cw = w_gate.shape[1] // chunks
        near_ws = [jnp.stack([w[:, j * cw : (j + 1) * cw] for w in (w_gate, w_up)]) for j in range(chunks)]
        far_ws = [swap_y(w) for w in near_ws]
        a_own = [glu(h, near_ws[0], far_ws[0])]
        q_back = tie(q_back, a_own[0])
        q_x = [pick(q4, xi), q_back]
        q_c = [pick(v, ci) for v in q_x] + [swap_c(pick(v, 1 - ci)) for v in q_x]

        half_dim = dim // 2
        inv_freq = ROPE_BASE ** (-2.0 * jnp.arange(half_dim, dtype=F32) / dim)
        positions = (lengths[:, None] + jnp.arange(new, dtype=jnp.int32)[None, :]).reshape(own_tok)
        angles = positions.astype(F32)[:, None] * inv_freq
        cos_t, sin_t = jnp.cos(angles), jnp.sin(angles)
        cos_t = jnp.concatenate([cos_t, cos_t], -1)
        sin_t = jnp.concatenate([-sin_t, sin_t], -1)
        o0, o1, o2, o3, k_next, v_next = attention(lengths, q_c, kv, cos_t, sin_t, k_cache, v_cache)

        keep = [o0, swap_c(o2)]
        send = swap_x(jnp.stack([o1, swap_c(o3)]))
        flip = lambda pair, i: jnp.where(i == 0, jnp.stack(pair), jnp.stack(pair[::-1]))
        o_rows = flip([flip(keep, ci), jnp.where(ci == 0, send, send[::-1])], xi)
        o_own = o_rows.reshape(half, -1)
        o_far = swap_c(o_own)
        o_far = swap_c(o_own)

        for j in range(1, chunks - 1):
            a_own.append(glu(h, near_ws[j], tie(far_ws[j], a_own[-1], o0)))
        a_far = [swap_c(v) for v in a_own]

        def block(xr, cr):
            col = (2 * (xi ^ xr) + (ci ^ cr)) * width
            pair = (w_down, w_out) if xr and cr else (tie(w_down, h), tie(w_out, h))
            return jnp.concatenate([lax.dynamic_slice_in_dim(w, col, width, 1) for w in pair], 0)

        blocks = [[block(xr, cr) for cr in range(2)] for xr in range(2)]
        narrow = width // 2
        other_y = {}
        for name in BLOCK_ORDER:
            b = blocks[int(name[0])][int(name[1])]
            if name[2:]:
                col = "AB".index(name[2]) * narrow
                b = b[:, col : col + narrow]
            other_y[name] = swap_y(b)

        def terms(near_w, far_w, which):
            out = []
            for a_part, o_part, w in ((a_own, o_own, near_w), (a_far, o_far, far_w)):
                if w is not None:
                    out += [(o_part, w, chunks * cw) if k == "o" else (a_part[k], w, k * cw) for k in which]
            return out

        early, late, every = [*range(chunks - 1), "o"], [chunks - 1], [*range(chunks), "o"]
        split = (0, 3 * half // 4), (3 * half // 4, half // 4)

        cross_far, same_far = swap_c(blocks[1][1]), swap_c(blocks[0][1])
        pre_cross = mix(terms(blocks[1][0], cross_far, early))
        pre_same = mix(terms(tie(blocks[0][0], pre_cross), same_far, early), [mine])
        a_own.append(glu(h, near_ws[-1], tie(far_ws[-1], pre_same)))
        a_far.append(swap_c(a_own[-1]))
        p_own, r_own = [], []
        for i, span in enumerate(split):
            p_own.append(mix(terms(blocks[1][0], cross_far, late), [pre_cross], F32, *span))
            r_own.append(swap_x(p_own[i]))

        pre_far = mix(terms(None, swap_c(tie(other_y["11"], *p_own)), every))
        r_far = []
        held = pre_far
        for i, side in enumerate("AB"):
            held = mix(terms(tie(other_y["10" + side], held), None, every), [pre_far], col=i)
            r_far.append(swap_x(held))

        def finish_own(i):
            return mix(terms(blocks[0][0], same_far, late), [pre_same, r_own[i]], BF16, *split[i])

        out = jnp.zeros((2, half, width), BF16)
        r_own[0] = tie(r_own[0], held)
        held = finish_own(0)
        out = lax.dynamic_update_slice(out, held[None], (yi, 0, 0))
        base = held = mix(terms(None, swap_c(tie(other_y["01"], held)), every), [from_y])
        out_far = []
        for i, side in enumerate("AB"):
            held = mix(terms(tie(other_y["00" + side], held), None, every), [base, r_far[i]], BF16, col=i)
            out_far.append(swap_y(held))
        r_own[1] = tie(r_own[1], held)
        held = finish_own(1)
        out = lax.dynamic_update_slice(out, held[None], (yi, split[1][0], 0))
        for i, part in enumerate(out_far):
            out = lax.dynamic_update_slice(out, part[None], (1 - yi, 0, i * narrow))
        return out.reshape(batch, new, width), k_next, v_next

    row_spec = P("dp", None, ("tx", "tyz"))
    batch_spec = P(("dp", "tx", "tyz"), None, None)
    in_specs = (row_spec, P(("dp", "tx", "tyz")), batch_spec, batch_spec, P(("tx", "tyz")), P("tx", "tyz"), P("tx", None), P("tx", None), P("tx", "tyz"), P("tx", "tyz"), P("tyz", "tx"), P("tyz", "tx"))
    out_specs = (row_spec, batch_spec, batch_spec)

    return jax.shard_map(local_layer, mesh=mesh, in_specs=in_specs, out_specs=out_specs, check_vma=False)
```

```python
import functools

import jax
import jax.numpy as jnp
from jax import lax
from jax.experimental import pallas as pl
from jax.experimental.pallas import tpu as pltpu
from jax.sharding import PartitionSpec as P

LN_EPS = 1e-6
ROPE_BASE = 10000.0
BF16 = jnp.bfloat16
F32 = jnp.float32


def swap(axis, pairs):
    return lambda a: lax.ppermute(a, axis, pairs)


swap_y = swap("tx", [(0, 1), (1, 0)])
swap_x = swap("tyz", [(0, 2), (2, 0), (1, 3), (3, 1)])
swap_c = swap("tyz", [(0, 1), (1, 0), (2, 3), (3, 2)])


def pick(arr, index):
    return lax.dynamic_index_in_dim(arr, index, axis=0, keepdims=False)


def norm_kernel(offs_ref, *refs):
    pieces, gain_ref, out_ref = refs[:8], refs[8], refs[9]
    width = pieces[0].shape[1]
    total = 8 * width
    xs = [p[...].astype(F32) for p in pieces]
    s1 = sum(jnp.sum(v, axis=-1, keepdims=True) for v in xs)
    s2 = sum(jnp.sum(v * v, axis=-1, keepdims=True) for v in xs)
    mean = s1 / total
    var = s2 / total - mean * mean
    inv = lax.rsqrt(var + LN_EPS)
    for i, v in enumerate(xs):
        off = pl.multiple_of(offs_ref[i], width)
        out_ref[:, pl.ds(off, width)] = ((v - mean) * inv * gain_ref[i : i + 1, :]).astype(BF16)


def layer_norm(pieces, gains, offs):
    tokens, width = pieces[0].shape
    blk = 256
    return pl.pallas_call(
        norm_kernel,
        grid_spec=pltpu.PrefetchScalarGridSpec(
            num_scalar_prefetch=1,
            grid=(tokens // blk,),
            in_specs=[pl.BlockSpec((blk, width), lambda i, o: (i, 0))] * 8 + [pl.BlockSpec((8, width), lambda i, o: (0, 0))],
            out_specs=pl.BlockSpec((blk, 8 * width), lambda i, o: (i, 0)),
        ),
        out_shape=jax.ShapeDtypeStruct((tokens, 8 * width), BF16),
        cost_estimate=pl.CostEstimate(flops=20 * tokens * 8 * width, bytes_accessed=32 * tokens * width, transcendentals=tokens),
        name="norm",
    )(offs, *pieces, gains)


def rope(t, cos_t, sin_t):
    t = t.astype(F32)
    return (t * cos_t + pltpu.roll(t, t.shape[-1] // 2, 1) * sin_t).astype(BF16)


def attn_kernel(len_ref, q0, q1, q2, q3, kv_ref, cos_ref, sin_ref, kc_ref, vc_ref, o0, o1, o2, o3, kn_ref, vn_ref, qs):
    new = kv_ref.shape[0]
    cache = kc_ref.shape[1]
    dim = kc_ref.shape[2]
    length = len_ref[pl.program_id(0)]
    cos_t, sin_t = cos_ref[...], sin_ref[...]
    win = new + 32
    kn_ref[...] = kc_ref[...]
    vn_ref[...] = vc_ref[...]
    base = pl.multiple_of(jnp.minimum((length // 16) * 16, cache - win), 16)
    rows = lax.broadcasted_iota(jnp.int32, (win, new), 0) + (base - length)
    hot = (rows == lax.broadcasted_iota(jnp.int32, (win, new), 1)).astype(BF16)
    key_rot = rope(kv_ref[:, :dim], cos_t, sin_t)
    r = lax.broadcasted_iota(jnp.int32, (win, dim), 0) + (base - length)
    fresh = (r >= 0) & (r < new)
    k_win = jnp.dot(hot, key_rot, preferred_element_type=F32)
    v_win = jnp.dot(hot, kv_ref[:, dim:], preferred_element_type=F32)
    sl = pl.ds(base, win)
    kn_ref[0, sl, :] = jnp.where(fresh, k_win, kc_ref[0, sl, :].astype(F32)).astype(BF16)
    vn_ref[0, sl, :] = jnp.where(fresh, v_win, vc_ref[0, sl, :].astype(F32)).astype(BF16)

    q_refs, o_refs = (q0, q1, q2, q3), (o0, o1, o2, o3)
    hpg = q0.shape[1] // dim
    for g in range(4):
        for h in range(hpg):
            qs[g * hpg * new + h * new : g * hpg * new + (h + 1) * new, :] = rope(q_refs[g][:, h * dim : (h + 1) * dim], cos_t, sin_t)

    fold = dim ** -0.5 * 1.4426950408889634

    def attend(keys, edge):
        @pl.loop(0, 4)
        def _(g):
            group = pl.ds(pl.multiple_of(g * hpg * new, hpg * new), hpg * new)
            q = qs[group, :]
            nt = (((1,), (1,)), ((), ()))
            sure = lax.dot_general(q, kn_ref[0, :edge, :], nt, preferred_element_type=F32) * fold
            rest = lax.dot_general(q, kn_ref[0, edge:keys, :], nt, preferred_element_type=F32) * fold
            tok = lax.broadcasted_iota(jnp.int32, rest.shape, 0) % new
            pos = lax.broadcasted_iota(jnp.int32, rest.shape, 1)
            rest = jnp.where(pos - tok <= length - edge, rest, -1e30)
            top = jnp.maximum(jnp.max(sure, axis=-1, keepdims=True), jnp.max(rest, axis=-1, keepdims=True))
            sure, rest = jnp.exp2(sure - top), jnp.exp2(rest - top)
            scale = 1.0 / (jnp.sum(sure, axis=-1, keepdims=True) + jnp.sum(rest, axis=-1, keepdims=True))
            o = jnp.dot((sure * scale).astype(BF16), vn_ref[0, :edge, :], preferred_element_type=F32)
            o = o + jnp.dot((rest * scale).astype(BF16), vn_ref[0, edge:keys, :], preferred_element_type=F32)
            qs[group, :] = o.astype(BF16)

    step = 256
    need = (length + new + step - 1) // step
    sizes = list(range(5, cache // step + 1))
    for n in sizes:
        cond = need <= n if n == sizes[0] else need == n
        pl.when(cond)(functools.partial(attend, n * step, (n - 1) * step - 128))
    for g in range(4):
        for h in range(hpg):
            o_refs[g][:, h * dim : (h + 1) * dim] = qs[(g * hpg + h) * new : (g * hpg + h + 1) * new, :]


def attention(lengths, qs, kv, cos_t, sin_t, k_cache, v_cache):
    rows, cache, dim = k_cache.shape
    new = kv.shape[0] // rows
    qw = qs[0].shape[1]
    tok = lambda w: pl.BlockSpec((new, w), lambda b, L: (b, 0))
    row = pl.BlockSpec((1, cache, dim), lambda b, L: (b, 0, 0))
    heads = 4 * qw // dim
    return pl.pallas_call(
        attn_kernel,
        grid_spec=pltpu.PrefetchScalarGridSpec(
            num_scalar_prefetch=1,
            grid=(rows,),
            in_specs=[tok(qw)] * 4 + [tok(2 * dim), tok(dim), tok(dim), row, row],
            out_specs=[tok(qw)] * 4 + [row, row],
            scratch_shapes=[pltpu.VMEM((heads * new, dim), BF16)],
        ),
        out_shape=[jax.ShapeDtypeStruct((rows * new, qw), BF16)] * 4 + [jax.ShapeDtypeStruct(k_cache.shape, BF16)] * 2,
        cost_estimate=pl.CostEstimate(
            flops=8 * rows * heads * new * cache * dim, bytes_accessed=8 * rows * cache * dim, transcendentals=rows * heads * new * cache
        ),
        name="attn",
    )(lengths, *qs, kv, cos_t, sin_t, k_cache, v_cache)


def glu_kernel(h_ref, near_w, far_w, a_ref):
    depth = near_w.shape[1]
    near, far = h_ref[:, :depth], h_ref[:, depth:]
    gate = jnp.dot(near, near_w[0], preferred_element_type=F32) + jnp.dot(far, far_w[0], preferred_element_type=F32)
    up = jnp.dot(near, near_w[1], preferred_element_type=F32) + jnp.dot(far, far_w[1], preferred_element_type=F32)
    a_ref[...] = (gate / (1.0 + jnp.exp(-gate)) * up).astype(BF16)


def glu(h, near_w, far_w):
    tokens, depth = h.shape
    cols = near_w.shape[2]
    blk = 512
    w = pl.BlockSpec(near_w.shape, lambda i: (0, 0, 0))
    return pl.pallas_call(
        glu_kernel,
        grid=(tokens // blk,),
        in_specs=[pl.BlockSpec((blk, depth), lambda i: (i, 0)), w, w],
        out_specs=pl.BlockSpec((blk, cols), lambda i: (i, 0)),
        out_shape=jax.ShapeDtypeStruct((tokens, cols), BF16),
        cost_estimate=pl.CostEstimate(flops=4 * tokens * depth * cols, bytes_accessed=2 * tokens * (depth + cols) + 4 * depth * cols, transcendentals=tokens * cols),
        name="glu",
    )(h, near_w, far_w)


def project_kernel(h_ref, *refs):
    total, row = None, 0
    for w in refs[:-1]:
        part = jnp.dot(h_ref[:, row : row + w.shape[0]], w[...], preferred_element_type=F32)
        total = part if total is None else total + part
        row += w.shape[0]
    refs[-1][...] = total.astype(BF16)


def project(h, ws):
    tokens, depth = h.shape
    cols = ws[0].shape[1]
    blk = 512
    return pl.pallas_call(
        project_kernel,
        grid=(tokens // blk,),
        in_specs=[pl.BlockSpec((blk, depth), lambda i: (i, 0))] + [pl.BlockSpec(w.shape, lambda i: (0, 0)) for w in ws],
        out_specs=pl.BlockSpec((blk, cols), lambda i: (i, 0)),
        out_shape=jax.ShapeDtypeStruct((tokens, cols), BF16),
        cost_estimate=pl.CostEstimate(flops=2 * tokens * depth * cols, bytes_accessed=2 * depth * (tokens + cols), transcendentals=0),
        name="project",
    )(h, *ws)


def mix_kernel(plan, n_lhs, n_w, *refs):
    lhs, ws, adds, out_ref = refs[:n_lhs], refs[n_lhs : n_lhs + n_w], refs[n_lhs + n_w : -1], refs[-1]
    total = None
    for l, (w, row) in zip(lhs, plan):
        part = jnp.dot(l[...], ws[w][row : row + l.shape[1], :], preferred_element_type=F32)
        total = part if total is None else total + part
    for t in adds:
        total = total + t[...].astype(F32)
    out_ref[...] = total.astype(out_ref.dtype)


def mix(terms, adds=(), dtype=F32, start=0, tokens=None, col=0):
    ws, plan = [], []
    for _, w, row in terms:
        found = [i for i, v in enumerate(ws) if v is w]
        if not found:
            ws.append(w)
        plan.append((found[0] if found else len(ws) - 1, row))
    lhs = [t[0] for t in terms]
    tokens = lhs[0].shape[0] if tokens is None else tokens
    cols = ws[0].shape[1]
    blk = 512
    first = start // blk
    tok = lambda w: pl.BlockSpec((blk, w), lambda i: (i + first, 0))
    depth = sum(l.shape[1] for l in lhs)
    add_specs = [pl.BlockSpec((blk, cols), lambda i, f=first * (t.shape[0] != tokens), c=col * (t.shape[1] != cols): (i + f, c)) for t in adds]
    return pl.pallas_call(
        functools.partial(mix_kernel, plan, len(lhs), len(ws)),
        grid=(tokens // blk,),
        in_specs=[tok(l.shape[1]) for l in lhs] + [pl.BlockSpec(w.shape, lambda i: (0, 0)) for w in ws] + add_specs,
        out_specs=pl.BlockSpec((blk, cols), lambda i: (i, 0)),
        out_shape=jax.ShapeDtypeStruct((tokens, cols), dtype),
        cost_estimate=pl.CostEstimate(flops=2 * tokens * depth * cols, bytes_accessed=2 * depth * (tokens + cols), transcendentals=0),
        name="mix",
    )(*lhs, *ws, *adds)


BLOCK_ORDER = ["11", "10A", "10B", "01", "00A", "00B"]


def tie(value, *others):
    return lax.optimization_barrier((value, *others))[0]


def solution(mesh):
    def local_layer(hidden, lengths, k_cache, v_cache, ln_gain, w_query, w_key, w_value, w_gate, w_up, w_down, w_out):
        batch, new, width = hidden.shape
        rows_own, _, dim = k_cache.shape
        yi = lax.axis_index("tx")
        ti = lax.axis_index("tyz")
        xi, ci = ti // 2, ti % 2
        half = batch * new // 2
        own_tok = rows_own * new

        g = ln_gain.reshape(1, width)
        g = jnp.concatenate([g, swap_y(g)], 0)
        g = jnp.concatenate([g, swap_x(g)], 0)
        g = jnp.concatenate([g, swap_c(g)], 0)
        hid2 = hidden.reshape(2, half, width)
        other = pick(hid2, 1 - yi)
        mine = pick(tie(hid2, other), yi)
        from_y = swap_y(other)
        mine_x = swap_x(mine)
        from_yx = swap_x(from_y)
        near = [mine, from_y, mine_x, from_yx]
        far = [swap_c(near[0])] + [swap_c(p) for p in near[1:]]
        offs = []
        for cr in range(2):
            for xr in range(2):
                for yr in range(2):
                    offs.append(width * (4 * yr + 2 * (xr ^ xi) + (cr ^ ci)))
        half_dim = dim // 2
        inv_freq = ROPE_BASE ** (-2.0 * jnp.arange(half_dim, dtype=F32) / dim)
        positions = (lengths[:, None] + jnp.arange(new, dtype=jnp.int32)[None, :]).reshape(own_tok)
        angles = positions.astype(F32)[:, None] * inv_freq
        cos_t, sin_t = jnp.cos(angles), jnp.sin(angles)
        cos_t = jnp.concatenate([cos_t, cos_t], -1)
        sin_t = jnp.concatenate([-sin_t, sin_t], -1)
        g = tie(g, cos_t, sin_t)
        h = layer_norm(near + far, g, jnp.stack(offs).astype(jnp.int32))

        kv_rows = w_key.shape[0] // 4
        w_kv = jnp.concatenate([w_key, w_value], axis=1)
        ordered = lambda pair, i, axis: jnp.where(i == 0, jnp.stack(pair, axis), jnp.stack(pair[::-1], axis))
        kv_part = swap_y(lax.dynamic_slice_in_dim(w_kv, ti * kv_rows, kv_rows, 0))
        kv_pair = ordered([kv_part, swap_x(kv_part)], xi, 0)
        kv_far = ordered([kv_pair, swap_c(kv_pair)], ci, 1).reshape(w_kv.shape)
        q_far = swap_y(w_query)

        q = project(h, [w_query, q_far])
        h_own = lax.dynamic_slice_in_dim(h, ti * own_tok, own_tok, 0)
        kv = jnp.dot(h_own, jnp.concatenate([w_kv, kv_far], 0), preferred_element_type=F32).astype(BF16)

        q4 = q.reshape(2, 2, own_tok, q.shape[1])
        q_back = swap_x(pick(q4, 1 - xi))

        chunks = 4
        cw = w_gate.shape[1] // chunks
        near_ws = [jnp.stack([w[:, j * cw : (j + 1) * cw] for w in (w_gate, w_up)]) for j in range(chunks)]
        far_ws = [swap_y(w) for w in near_ws]
        a_own = [glu(h, near_ws[0], far_ws[0])]
        q_back = tie(q_back, a_own[0])
        q_x = [pick(q4, xi), q_back]
        q_c = [pick(v, ci) for v in q_x] + [swap_c(pick(v, 1 - ci)) for v in q_x]

        o0, o1, o2, o3, k_next, v_next = attention(lengths, q_c, kv, cos_t, sin_t, k_cache, v_cache)

        keep = [o0, swap_c(o2)]
        send = swap_x(jnp.stack([o1, swap_c(o3)]))
        flip = lambda pair, i: jnp.where(i == 0, jnp.stack(pair), jnp.stack(pair[::-1]))
        o_rows = flip([flip(keep, ci), jnp.where(ci == 0, send, send[::-1])], xi)
        o_own = o_rows.reshape(half, -1)
        o_far = swap_c(o_own)
        o_far = swap_c(o_own)

        for j in range(1, chunks - 1):
            a_own.append(glu(h, near_ws[j], tie(far_ws[j], a_own[-1], o0)))
        a_far = [swap_c(v) for v in a_own]

        def block(xr, cr):
            col = (2 * (xi ^ xr) + (ci ^ cr)) * width
            pair = (w_down, w_out) if xr and cr else (tie(w_down, h), tie(w_out, h))
            return jnp.concatenate([lax.dynamic_slice_in_dim(w, col, width, 1) for w in pair], 0)

        blocks = [[block(xr, cr) for cr in range(2)] for xr in range(2)]
        narrow = width // 2
        other_y = {}
        for name in BLOCK_ORDER:
            b = blocks[int(name[0])][int(name[1])]
            if name[2:]:
                col = "AB".index(name[2]) * narrow
                b = b[:, col : col + narrow]
            other_y[name] = swap_y(b)

        def terms(near_w, far_w, which):
            out = []
            for a_part, o_part, w in ((a_own, o_own, near_w), (a_far, o_far, far_w)):
                if w is not None:
                    out += [(o_part, w, chunks * cw) if k == "o" else (a_part[k], w, k * cw) for k in which]
            return out

        early, late, every = [*range(chunks - 1), "o"], [chunks - 1], [*range(chunks), "o"]
        split = (0, 3 * half // 4), (3 * half // 4, half // 4)

        cross_far, same_far = swap_c(blocks[1][1]), swap_c(blocks[0][1])
        pre_cross = mix(terms(blocks[1][0], cross_far, early))
        pre_same = mix(terms(tie(blocks[0][0], pre_cross), same_far, early), [mine])
        a_own.append(glu(h, near_ws[-1], tie(far_ws[-1], pre_same)))
        a_far.append(swap_c(a_own[-1]))
        p_own, r_own = [], []
        for i, span in enumerate(split):
            p_own.append(mix(terms(blocks[1][0], cross_far, late), [pre_cross], F32, *span))
            r_own.append(swap_x(p_own[i]))

        pre_far = mix(terms(None, swap_c(tie(other_y["11"], *p_own)), every))
        r_far = []
        held = pre_far
        for i, side in enumerate("AB"):
            held = mix(terms(tie(other_y["10" + side], held), None, every), [pre_far], col=i)
            r_far.append(swap_x(held))

        def finish_own(i):
            return mix(terms(blocks[0][0], same_far, late), [pre_same, r_own[i]], BF16, *split[i])

        out = jnp.zeros((2, half, width), BF16)
        r_own[0] = tie(r_own[0], held)
        held = finish_own(0)
        out = lax.dynamic_update_slice(out, held[None], (yi, 0, 0))
        base = held = mix(terms(None, swap_c(tie(other_y["01"], held)), every), [from_y])
        out_far = []
        for i, side in enumerate("AB"):
            held = mix(terms(tie(other_y["00" + side], held), None, every), [base, r_far[i]], BF16, col=i)
            out_far.append(swap_y(held))
        r_own[1] = tie(r_own[1], held)
        held = finish_own(1)
        out = lax.dynamic_update_slice(out, held[None], (yi, split[1][0], 0))
        for i, part in enumerate(out_far):
            out = lax.dynamic_update_slice(out, part[None], (1 - yi, 0, i * narrow))
        return out.reshape(batch, new, width), k_next, v_next

    row_spec = P("dp", None, ("tx", "tyz"))
    batch_spec = P(("dp", "tx", "tyz"), None, None)
    in_specs = (row_spec, P(("dp", "tx", "tyz")), batch_spec, batch_spec, P(("tx", "tyz")), P("tx", "tyz"), P("tx", None), P("tx", None), P("tx", "tyz"), P("tx", "tyz"), P("tyz", "tx"), P("tyz", "tx"))
    out_specs = (row_spec, batch_spec, batch_spec)

    return jax.shard_map(local_layer, mesh=mesh, in_specs=in_specs, out_specs=out_specs, check_vma=False)
```

```python
import functools

import jax
import jax.numpy as jnp
from jax import lax
from jax.experimental import pallas as pl
from jax.experimental.pallas import tpu as pltpu
from jax.sharding import PartitionSpec as P

LN_EPS = 1e-6
ROPE_BASE = 10000.0
BF16 = jnp.bfloat16
F32 = jnp.float32


def swap(axis, pairs):
    return lambda a: lax.ppermute(a, axis, pairs)


swap_y = swap("tx", [(0, 1), (1, 0)])
swap_x = swap("tyz", [(0, 2), (2, 0), (1, 3), (3, 1)])
swap_c = swap("tyz", [(0, 1), (1, 0), (2, 3), (3, 2)])


def pick(arr, index):
    return lax.dynamic_index_in_dim(arr, index, axis=0, keepdims=False)


def norm_kernel(offs_ref, *refs):
    pieces, gain_ref, out_ref = refs[:8], refs[8], refs[9]
    width = pieces[0].shape[1]
    total = 8 * width
    xs = [p[...].astype(F32) for p in pieces]
    s1 = sum(jnp.sum(v, axis=-1, keepdims=True) for v in xs)
    s2 = sum(jnp.sum(v * v, axis=-1, keepdims=True) for v in xs)
    mean = s1 / total
    var = s2 / total - mean * mean
    inv = lax.rsqrt(var + LN_EPS)
    for i, v in enumerate(xs):
        off = pl.multiple_of(offs_ref[i], width)
        out_ref[:, pl.ds(off, width)] = ((v - mean) * inv * gain_ref[i : i + 1, :]).astype(BF16)


def layer_norm(pieces, gains, offs):
    tokens, width = pieces[0].shape
    blk = 256
    return pl.pallas_call(
        norm_kernel,
        grid_spec=pltpu.PrefetchScalarGridSpec(
            num_scalar_prefetch=1,
            grid=(tokens // blk,),
            in_specs=[pl.BlockSpec((blk, width), lambda i, o: (i, 0))] * 8 + [pl.BlockSpec((8, width), lambda i, o: (0, 0))],
            out_specs=pl.BlockSpec((blk, 8 * width), lambda i, o: (i, 0)),
        ),
        out_shape=jax.ShapeDtypeStruct((tokens, 8 * width), BF16),
        cost_estimate=pl.CostEstimate(flops=20 * tokens * 8 * width, bytes_accessed=32 * tokens * width, transcendentals=tokens),
        name="norm",
    )(offs, *pieces, gains)


def rope(t, cos_t, sin_t):
    t = t.astype(F32)
    return (t * cos_t + pltpu.roll(t, t.shape[-1] // 2, 1) * sin_t).astype(BF16)


def attn_kernel(len_ref, q0, q1, q2, q3, kv_ref, cos_ref, sin_ref, kc_ref, vc_ref, o0, o1, o2, o3, kn_ref, vn_ref, qs):
    new = kv_ref.shape[0]
    cache = kc_ref.shape[1]
    dim = kc_ref.shape[2]
    length = len_ref[pl.program_id(0)]
    cos_t, sin_t = cos_ref[...], sin_ref[...]
    win = new + 32
    kn_ref[...] = kc_ref[...]
    vn_ref[...] = vc_ref[...]
    base = pl.multiple_of(jnp.minimum((length // 16) * 16, cache - win), 16)
    rows = lax.broadcasted_iota(jnp.int32, (win, new), 0) + (base - length)
    hot = (rows == lax.broadcasted_iota(jnp.int32, (win, new), 1)).astype(BF16)
    key_rot = rope(kv_ref[:, :dim], cos_t, sin_t)
    r = lax.broadcasted_iota(jnp.int32, (win, dim), 0) + (base - length)
    fresh = (r >= 0) & (r < new)
    k_win = jnp.dot(hot, key_rot, preferred_element_type=F32)
    v_win = jnp.dot(hot, kv_ref[:, dim:], preferred_element_type=F32)
    sl = pl.ds(base, win)
    kn_ref[0, sl, :] = jnp.where(fresh, k_win, kc_ref[0, sl, :].astype(F32)).astype(BF16)
    vn_ref[0, sl, :] = jnp.where(fresh, v_win, vc_ref[0, sl, :].astype(F32)).astype(BF16)

    q_refs, o_refs = (q0, q1, q2, q3), (o0, o1, o2, o3)
    hpg = q0.shape[1] // dim
    for g in range(4):
        for h in range(hpg):
            qs[g * hpg * new + h * new : g * hpg * new + (h + 1) * new, :] = rope(q_refs[g][:, h * dim : (h + 1) * dim], cos_t, sin_t)

    fold = dim ** -0.5 * 1.4426950408889634

    def attend(keys, edge):
        @pl.loop(0, 4)
        def _(g):
            group = pl.ds(pl.multiple_of(g * hpg * new, hpg * new), hpg * new)
            q = qs[group, :]
            nt = (((1,), (1,)), ((), ()))
            sure = lax.dot_general(q, kn_ref[0, :edge, :], nt, preferred_element_type=F32) * fold
            rest = lax.dot_general(q, kn_ref[0, edge:keys, :], nt, preferred_element_type=F32) * fold
            tok = lax.broadcasted_iota(jnp.int32, rest.shape, 0) % new
            pos = lax.broadcasted_iota(jnp.int32, rest.shape, 1)
            rest = jnp.where(pos - tok <= length - edge, rest, -1e30)
            top = jnp.maximum(jnp.max(sure, axis=-1, keepdims=True), jnp.max(rest, axis=-1, keepdims=True))
            sure, rest = jnp.exp2(sure - top), jnp.exp2(rest - top)
            scale = 1.0 / (jnp.sum(sure, axis=-1, keepdims=True) + jnp.sum(rest, axis=-1, keepdims=True))
            o = jnp.dot((sure * scale).astype(BF16), vn_ref[0, :edge, :], preferred_element_type=F32)
            o = o + jnp.dot((rest * scale).astype(BF16), vn_ref[0, edge:keys, :], preferred_element_type=F32)
            qs[group, :] = o.astype(BF16)

    step = 256
    need = (length + new + step - 1) // step
    sizes = list(range(5, cache // step + 1))
    for n in sizes:
        cond = need <= n if n == sizes[0] else need == n
        pl.when(cond)(functools.partial(attend, n * step, (n - 1) * step - 128))
    for g in range(4):
        for h in range(hpg):
            o_refs[g][:, h * dim : (h + 1) * dim] = qs[(g * hpg + h) * new : (g * hpg + h + 1) * new, :]


def attention(lengths, qs, kv, cos_t, sin_t, k_cache, v_cache):
    rows, cache, dim = k_cache.shape
    new = kv.shape[0] // rows
    qw = qs[0].shape[1]
    tok = lambda w: pl.BlockSpec((new, w), lambda b, L: (b, 0))
    row = pl.BlockSpec((1, cache, dim), lambda b, L: (b, 0, 0))
    heads = 4 * qw // dim
    return pl.pallas_call(
        attn_kernel,
        grid_spec=pltpu.PrefetchScalarGridSpec(
            num_scalar_prefetch=1,
            grid=(rows,),
            in_specs=[tok(qw)] * 4 + [tok(2 * dim), tok(dim), tok(dim), row, row],
            out_specs=[tok(qw)] * 4 + [row, row],
            scratch_shapes=[pltpu.VMEM((heads * new, dim), BF16)],
        ),
        out_shape=[jax.ShapeDtypeStruct((rows * new, qw), BF16)] * 4 + [jax.ShapeDtypeStruct(k_cache.shape, BF16)] * 2,
        cost_estimate=pl.CostEstimate(
            flops=8 * rows * heads * new * cache * dim, bytes_accessed=8 * rows * cache * dim, transcendentals=rows * heads * new * cache
        ),
        name="attn",
    )(lengths, *qs, kv, cos_t, sin_t, k_cache, v_cache)


def glu_kernel(h_ref, near_w, far_w, a_ref):
    depth = near_w.shape[1]
    near, far = h_ref[:, :depth], h_ref[:, depth:]
    gate = jnp.dot(near, near_w[0], preferred_element_type=F32) + jnp.dot(far, far_w[0], preferred_element_type=F32)
    up = jnp.dot(near, near_w[1], preferred_element_type=F32) + jnp.dot(far, far_w[1], preferred_element_type=F32)
    a_ref[...] = (gate / (1.0 + jnp.exp(-gate)) * up).astype(BF16)


def glu(h, near_w, far_w):
    tokens, depth = h.shape
    cols = near_w.shape[2]
    blk = 512
    w = pl.BlockSpec(near_w.shape, lambda i: (0, 0, 0))
    return pl.pallas_call(
        glu_kernel,
        grid=(tokens // blk,),
        in_specs=[pl.BlockSpec((blk, depth), lambda i: (i, 0)), w, w],
        out_specs=pl.BlockSpec((blk, cols), lambda i: (i, 0)),
        out_shape=jax.ShapeDtypeStruct((tokens, cols), BF16),
        cost_estimate=pl.CostEstimate(flops=4 * tokens * depth * cols, bytes_accessed=2 * tokens * (depth + cols) + 4 * depth * cols, transcendentals=tokens * cols),
        name="glu",
    )(h, near_w, far_w)


def project_kernel(h_ref, *refs):
    total, row = None, 0
    for w in refs[:-1]:
        part = jnp.dot(h_ref[:, row : row + w.shape[0]], w[...], preferred_element_type=F32)
        total = part if total is None else total + part
        row += w.shape[0]
    refs[-1][...] = total.astype(BF16)


def project(h, ws):
    tokens, depth = h.shape
    cols = ws[0].shape[1]
    blk = 512
    return pl.pallas_call(
        project_kernel,
        grid=(tokens // blk,),
        in_specs=[pl.BlockSpec((blk, depth), lambda i: (i, 0))] + [pl.BlockSpec(w.shape, lambda i: (0, 0)) for w in ws],
        out_specs=pl.BlockSpec((blk, cols), lambda i: (i, 0)),
        out_shape=jax.ShapeDtypeStruct((tokens, cols), BF16),
        cost_estimate=pl.CostEstimate(flops=2 * tokens * depth * cols, bytes_accessed=2 * depth * (tokens + cols), transcendentals=0),
        name="project",
    )(h, *ws)


def mix_kernel(plan, n_lhs, n_w, *refs):
    lhs, ws, adds, out_ref = refs[:n_lhs], refs[n_lhs : n_lhs + n_w], refs[n_lhs + n_w : -1], refs[-1]
    total = None
    for l, (w, row) in zip(lhs, plan):
        part = jnp.dot(l[...], ws[w][row : row + l.shape[1], :], preferred_element_type=F32)
        total = part if total is None else total + part
    for t in adds:
        total = total + t[...].astype(F32)
    out_ref[...] = total.astype(out_ref.dtype)


def mix(terms, adds=(), dtype=F32, start=0, tokens=None, col=0):
    ws, plan = [], []
    for _, w, row in terms:
        found = [i for i, v in enumerate(ws) if v is w]
        if not found:
            ws.append(w)
        plan.append((found[0] if found else len(ws) - 1, row))
    lhs = [t[0] for t in terms]
    tokens = lhs[0].shape[0] if tokens is None else tokens
    cols = ws[0].shape[1]
    blk = 512
    first = start // blk
    tok = lambda w: pl.BlockSpec((blk, w), lambda i: (i + first, 0))
    depth = sum(l.shape[1] for l in lhs)
    add_specs = [pl.BlockSpec((blk, cols), lambda i, f=first * (t.shape[0] != tokens), c=col * (t.shape[1] != cols): (i + f, c)) for t in adds]
    return pl.pallas_call(
        functools.partial(mix_kernel, plan, len(lhs), len(ws)),
        grid=(tokens // blk,),
        in_specs=[tok(l.shape[1]) for l in lhs] + [pl.BlockSpec(w.shape, lambda i: (0, 0)) for w in ws] + add_specs,
        out_specs=pl.BlockSpec((blk, cols), lambda i: (i, 0)),
        out_shape=jax.ShapeDtypeStruct((tokens, cols), dtype),
        cost_estimate=pl.CostEstimate(flops=2 * tokens * depth * cols, bytes_accessed=2 * depth * (tokens + cols), transcendentals=0),
        compiler_params=pltpu.CompilerParams(vmem_limit_bytes=67043328),
        name="mix",
    )(*lhs, *ws, *adds)


BLOCK_ORDER = ["11", "10A", "10B", "01", "00A", "00B"]


def tie(value, *others):
    return lax.optimization_barrier((value, *others))[0]


def solution(mesh):
    def local_layer(hidden, lengths, k_cache, v_cache, ln_gain, w_query, w_key, w_value, w_gate, w_up, w_down, w_out):
        batch, new, width = hidden.shape
        rows_own, _, dim = k_cache.shape
        yi = lax.axis_index("tx")
        ti = lax.axis_index("tyz")
        xi, ci = ti // 2, ti % 2
        half = batch * new // 2
        own_tok = rows_own * new

        g = ln_gain.reshape(1, width)
        g = jnp.concatenate([g, swap_y(g)], 0)
        g = jnp.concatenate([g, swap_x(g)], 0)
        g = jnp.concatenate([g, swap_c(g)], 0)
        offs = []
        for cr in range(2):
            for xr in range(2):
                for yr in range(2):
                    offs.append(width * (4 * yr + 2 * (xr ^ xi) + (cr ^ ci)))
        offs = jnp.stack(offs).astype(jnp.int32)
        half_dim = dim // 2
        inv_freq = ROPE_BASE ** (-2.0 * jnp.arange(half_dim, dtype=F32) / dim)
        positions = (lengths[:, None] + jnp.arange(new, dtype=jnp.int32)[None, :]).reshape(own_tok)
        angles = positions.astype(F32)[:, None] * inv_freq
        cos_t, sin_t = jnp.cos(angles), jnp.sin(angles)
        cos_t = jnp.concatenate([cos_t, cos_t], -1)
        sin_t = jnp.concatenate([-sin_t, sin_t], -1)

        kv_rows = w_key.shape[0] // 4
        w_kv = jnp.concatenate([w_key, w_value], axis=1)
        ordered = lambda pair, i, axis: jnp.where(i == 0, jnp.stack(pair, axis), jnp.stack(pair[::-1], axis))
        kv_part = swap_y(lax.dynamic_slice_in_dim(w_kv, ti * kv_rows, kv_rows, 0))
        kv_pair = ordered([kv_part, swap_x(kv_part)], xi, 0)
        kv_far = ordered([kv_pair, swap_c(kv_pair)], ci, 1).reshape(w_kv.shape)

        hid2 = hidden.reshape(2, half, width)
        other = pick(hid2, 1 - yi)
        mine = pick(tie(hid2, other), yi)
        mine_x = swap_x(mine)
        over = [swap_y(other[i * half // 2 : (i + 1) * half // 2]) for i in range(2)]
        over[0] = tie(over[0], cos_t, sin_t, offs)
        forward = [swap_x(p) for p in over]
        from_y = jnp.concatenate(over, 0)
        far = [swap_c(mine), swap_c(from_y), swap_c(mine_x)]
        from_yx = jnp.concatenate(forward, 0)
        near = [mine, from_y, mine_x, from_yx]
        far.append(swap_c(from_yx))
        h = layer_norm(near + far, g, offs)

        q_far = swap_y(w_query)

        q = project(h, [w_query, q_far])
        h_own = lax.dynamic_slice_in_dim(h, ti * own_tok, own_tok, 0)
        kv = jnp.dot(h_own, jnp.concatenate([w_kv, kv_far], 0), preferred_element_type=F32).astype(BF16)

        q4 = q.reshape(2, 2, own_tok, q.shape[1])
        q_back = swap_x(pick(q4, 1 - xi))

        chunks = 4
        cw = w_gate.shape[1] // chunks
        near_ws = [jnp.stack([w[:, j * cw : (j + 1) * cw] for w in (w_gate, w_up)]) for j in range(chunks)]
        far_ws = [swap_y(w) for w in near_ws]
        a_own = [glu(h, near_ws[0], far_ws[0])]
        q_back = tie(q_back, a_own[0])
        q_x = [pick(q4, xi), q_back]
        q_c = [pick(v, ci) for v in q_x] + [swap_c(pick(v, 1 - ci)) for v in q_x]

        o0, o1, o2, o3, k_next, v_next = attention(lengths, q_c, kv, cos_t, sin_t, k_cache, v_cache)

        keep = [o0, swap_c(o2)]
        send = swap_x(jnp.stack([o1, swap_c(o3)]))
        flip = lambda pair, i: jnp.where(i == 0, jnp.stack(pair), jnp.stack(pair[::-1]))
        o_rows = flip([flip(keep, ci), jnp.where(ci == 0, send, send[::-1])], xi)
        o_own = o_rows.reshape(half, -1)
        o_far = swap_c(o_own)
        o_far = swap_c(o_own)

        for j in range(1, chunks - 1):
            a_own.append(glu(h, near_ws[j], tie(far_ws[j], a_own[-1], o0)))
        a_far = [swap_c(v) for v in a_own]

        def block(xr, cr):
            col = (2 * (xi ^ xr) + (ci ^ cr)) * width
            pair = (w_down, w_out) if xr and cr else (tie(w_down, h), tie(w_out, h))
            return jnp.concatenate([lax.dynamic_slice_in_dim(w, col, width, 1) for w in pair], 0)

        blocks = [[block(xr, cr) for cr in range(2)] for xr in range(2)]
        narrow = width // 2
        other_y = {}
        for name in BLOCK_ORDER:
            b = blocks[int(name[0])][int(name[1])]
            if name[2:]:
                col = "AB".index(name[2]) * narrow
                b = b[:, col : col + narrow]
            other_y[name] = swap_y(b)

        def terms(near_w, far_w, which):
            out = []
            for a_part, o_part, w in ((a_own, o_own, near_w), (a_far, o_far, far_w)):
                if w is not None:
                    out += [(o_part, w, chunks * cw) if k == "o" else (a_part[k], w, k * cw) for k in which]
            return out

        early, late, every = [*range(chunks - 1), "o"], [chunks - 1], [*range(chunks), "o"]
        split = (0, half // 2), (half // 2, half // 2)

        cross_far, same_far = swap_c(blocks[1][1]), swap_c(blocks[0][1])
        pre_cross = mix(terms(blocks[1][0], cross_far, early))
        pre_same = mix(terms(tie(blocks[0][0], pre_cross), same_far, early), [mine])
        a_own.append(glu(h, near_ws[-1], tie(far_ws[-1], pre_same)))
        a_far.append(swap_c(a_own[-1]))
        p_own, r_own = [], []
        for i, span in enumerate(split):
            p_own.append(mix(terms(blocks[1][0], cross_far, late), [pre_cross], F32, *span))
            r_own.append(swap_x(p_own[i]))

        pre_far = mix(terms(None, swap_c(tie(other_y["11"], *p_own)), every))
        r_far = []
        held = pre_far
        for i, side in enumerate("AB"):
            held = mix(terms(tie(other_y["10" + side], held), None, every), [pre_far], col=i)
            r_far.append(swap_x(held))

        def finish_own(i):
            return mix(terms(blocks[0][0], same_far, late), [pre_same, r_own[i]], BF16, *split[i])

        out = jnp.zeros((2, half, width), BF16)
        r_own[0] = tie(r_own[0], held)
        held = finish_own(0)
        out = lax.dynamic_update_slice(out, held[None], (yi, 0, 0))
        base = held = mix(terms(None, swap_c(tie(other_y["01"], held)), every), [from_y])
        out_far = []
        for i, side in enumerate("AB"):
            held = mix(terms(tie(other_y["00" + side], held), None, every), [base, r_far[i]], BF16, col=i)
            out_far.append(swap_y(held))
        r_own[1] = tie(r_own[1], held)
        held = finish_own(1)
        out = lax.dynamic_update_slice(out, held[None], (yi, split[1][0], 0))
        for i, part in enumerate(out_far):
            out = lax.dynamic_update_slice(out, part[None], (1 - yi, 0, i * narrow))
        return out.reshape(batch, new, width), k_next, v_next

    row_spec = P("dp", None, ("tx", "tyz"))
    batch_spec = P(("dp", "tx", "tyz"), None, None)
    in_specs = (row_spec, P(("dp", "tx", "tyz")), batch_spec, batch_spec, P(("tx", "tyz")), P("tx", "tyz"), P("tx", None), P("tx", None), P("tx", "tyz"), P("tx", "tyz"), P("tyz", "tx"), P("tyz", "tx"))
    out_specs = (row_spec, batch_spec, batch_spec)

    return jax.shard_map(local_layer, mesh=mesh, in_specs=in_specs, out_specs=out_specs, check_vma=False)
```

```python
import functools

import jax
import jax.numpy as jnp
from jax import lax
from jax.experimental import pallas as pl
from jax.experimental.pallas import tpu as pltpu
from jax.sharding import PartitionSpec as P

LN_EPS = 1e-6
ROPE_BASE = 10000.0
BF16 = jnp.bfloat16
F32 = jnp.float32


def swap(axis, pairs):
    return lambda a: lax.ppermute(a, axis, pairs)


swap_y = swap("tx", [(0, 1), (1, 0)])
swap_x = swap("tyz", [(0, 2), (2, 0), (1, 3), (3, 1)])
swap_c = swap("tyz", [(0, 1), (1, 0), (2, 3), (3, 2)])


def pick(arr, index):
    return lax.dynamic_index_in_dim(arr, index, axis=0, keepdims=False)


def norm_kernel(offs_ref, *refs):
    pieces, gain_ref, out_ref = refs[:8], refs[8], refs[9]
    width = pieces[0].shape[1]
    total = 8 * width
    xs = [p[...].astype(F32) for p in pieces]
    s1 = sum(jnp.sum(v, axis=-1, keepdims=True) for v in xs)
    s2 = sum(jnp.sum(v * v, axis=-1, keepdims=True) for v in xs)
    mean = s1 / total
    var = s2 / total - mean * mean
    inv = lax.rsqrt(var + LN_EPS)
    for i, v in enumerate(xs):
        off = pl.multiple_of(offs_ref[i], width)
        out_ref[:, pl.ds(off, width)] = ((v - mean) * inv * gain_ref[i : i + 1, :]).astype(BF16)


def layer_norm(pieces, gains, offs):
    tokens, width = pieces[0].shape
    blk = 256
    return pl.pallas_call(
        norm_kernel,
        grid_spec=pltpu.PrefetchScalarGridSpec(
            num_scalar_prefetch=1,
            grid=(tokens // blk,),
            in_specs=[pl.BlockSpec((blk, width), lambda i, o: (i, 0))] * 8 + [pl.BlockSpec((8, width), lambda i, o: (0, 0))],
            out_specs=pl.BlockSpec((blk, 8 * width), lambda i, o: (i, 0)),
        ),
        out_shape=jax.ShapeDtypeStruct((tokens, 8 * width), BF16),
        cost_estimate=pl.CostEstimate(flops=20 * tokens * 8 * width, bytes_accessed=32 * tokens * width, transcendentals=tokens),
        name="norm",
    )(offs, *pieces, gains)


def rope(t, cos_t, sin_t):
    t = t.astype(F32)
    return (t * cos_t + pltpu.roll(t, t.shape[-1] // 2, 1) * sin_t).astype(BF16)


def attn_kernel(len_ref, q0, q1, q2, q3, kv_ref, cos_ref, sin_ref, kc_ref, vc_ref, o0, o1, o2, o3, kn_ref, vn_ref, qs):
    new = kv_ref.shape[0]
    cache = kc_ref.shape[1]
    dim = kc_ref.shape[2]
    length = len_ref[pl.program_id(0)]
    cos_t, sin_t = cos_ref[...], sin_ref[...]
    win = new + 32
    kn_ref[...] = kc_ref[...]
    vn_ref[...] = vc_ref[...]
    base = pl.multiple_of(jnp.minimum((length // 16) * 16, cache - win), 16)
    rows = lax.broadcasted_iota(jnp.int32, (win, new), 0) + (base - length)
    hot = (rows == lax.broadcasted_iota(jnp.int32, (win, new), 1)).astype(BF16)
    key_rot = rope(kv_ref[:, :dim], cos_t, sin_t)
    r = lax.broadcasted_iota(jnp.int32, (win, dim), 0) + (base - length)
    fresh = (r >= 0) & (r < new)
    k_win = jnp.dot(hot, key_rot, preferred_element_type=F32)
    v_win = jnp.dot(hot, kv_ref[:, dim:], preferred_element_type=F32)
    sl = pl.ds(base, win)
    kn_ref[0, sl, :] = jnp.where(fresh, k_win, kc_ref[0, sl, :].astype(F32)).astype(BF16)
    vn_ref[0, sl, :] = jnp.where(fresh, v_win, vc_ref[0, sl, :].astype(F32)).astype(BF16)

    q_refs, o_refs = (q0, q1, q2, q3), (o0, o1, o2, o3)
    hpg = q0.shape[1] // dim
    for g in range(4):
        for h in range(hpg):
            qs[g * hpg * new + h * new : g * hpg * new + (h + 1) * new, :] = rope(q_refs[g][:, h * dim : (h + 1) * dim], cos_t, sin_t)

    fold = dim ** -0.5 * 1.4426950408889634

    def attend(keys, edge):
        @pl.loop(0, 4)
        def _(g):
            group = pl.ds(pl.multiple_of(g * hpg * new, hpg * new), hpg * new)
            q = qs[group, :]
            nt = (((1,), (1,)), ((), ()))
            sure = lax.dot_general(q, kn_ref[0, :edge, :], nt, preferred_element_type=F32) * fold
            rest = lax.dot_general(q, kn_ref[0, edge:keys, :], nt, preferred_element_type=F32) * fold
            tok = lax.broadcasted_iota(jnp.int32, rest.shape, 0) % new
            pos = lax.broadcasted_iota(jnp.int32, rest.shape, 1)
            rest = jnp.where(pos - tok <= length - edge, rest, -1e30)
            top = jnp.maximum(jnp.max(sure, axis=-1, keepdims=True), jnp.max(rest, axis=-1, keepdims=True))
            sure, rest = jnp.exp2(sure - top), jnp.exp2(rest - top)
            scale = 1.0 / (jnp.sum(sure, axis=-1, keepdims=True) + jnp.sum(rest, axis=-1, keepdims=True))
            o = jnp.dot((sure * scale).astype(BF16), vn_ref[0, :edge, :], preferred_element_type=F32)
            o = o + jnp.dot((rest * scale).astype(BF16), vn_ref[0, edge:keys, :], preferred_element_type=F32)
            qs[group, :] = o.astype(BF16)

    step = 256
    need = (length + new + step - 1) // step
    sizes = list(range(5, cache // step + 1))
    for n in sizes:
        cond = need <= n if n == sizes[0] else need == n
        pl.when(cond)(functools.partial(attend, n * step, (n - 1) * step - 128))
    for g in range(4):
        for h in range(hpg):
            o_refs[g][:, h * dim : (h + 1) * dim] = qs[(g * hpg + h) * new : (g * hpg + h + 1) * new, :]


def attention(lengths, qs, kv, cos_t, sin_t, k_cache, v_cache):
    rows, cache, dim = k_cache.shape
    new = kv.shape[0] // rows
    qw = qs[0].shape[1]
    tok = lambda w: pl.BlockSpec((new, w), lambda b, L: (b, 0))
    row = pl.BlockSpec((1, cache, dim), lambda b, L: (b, 0, 0))
    heads = 4 * qw // dim
    return pl.pallas_call(
        attn_kernel,
        grid_spec=pltpu.PrefetchScalarGridSpec(
            num_scalar_prefetch=1,
            grid=(rows,),
            in_specs=[tok(qw)] * 4 + [tok(2 * dim), tok(dim), tok(dim), row, row],
            out_specs=[tok(qw)] * 4 + [row, row],
            scratch_shapes=[pltpu.VMEM((heads * new, dim), BF16)],
        ),
        out_shape=[jax.ShapeDtypeStruct((rows * new, qw), BF16)] * 4 + [jax.ShapeDtypeStruct(k_cache.shape, BF16)] * 2,
        cost_estimate=pl.CostEstimate(
            flops=8 * rows * heads * new * cache * dim, bytes_accessed=8 * rows * cache * dim, transcendentals=rows * heads * new * cache
        ),
        name="attn",
    )(lengths, *qs, kv, cos_t, sin_t, k_cache, v_cache)


def glu_kernel(h_ref, near_w, far_w, a_ref):
    depth = near_w.shape[1]
    near, far = h_ref[:, :depth], h_ref[:, depth:]
    gate = jnp.dot(near, near_w[0], preferred_element_type=F32) + jnp.dot(far, far_w[0], preferred_element_type=F32)
    up = jnp.dot(near, near_w[1], preferred_element_type=F32) + jnp.dot(far, far_w[1], preferred_element_type=F32)
    a_ref[...] = (gate / (1.0 + jnp.exp(-gate)) * up).astype(BF16)


def glu(h, near_w, far_w):
    tokens, depth = h.shape
    cols = near_w.shape[2]
    blk = 512
    w = pl.BlockSpec(near_w.shape, lambda i: (0, 0, 0))
    return pl.pallas_call(
        glu_kernel,
        grid=(tokens // blk,),
        in_specs=[pl.BlockSpec((blk, depth), lambda i: (i, 0)), w, w],
        out_specs=pl.BlockSpec((blk, cols), lambda i: (i, 0)),
        out_shape=jax.ShapeDtypeStruct((tokens, cols), BF16),
        cost_estimate=pl.CostEstimate(flops=4 * tokens * depth * cols, bytes_accessed=2 * tokens * (depth + cols) + 4 * depth * cols, transcendentals=tokens * cols),
        name="glu",
    )(h, near_w, far_w)


def project_kernel(h_ref, *refs):
    total, row = None, 0
    for w in refs[:-1]:
        part = jnp.dot(h_ref[:, row : row + w.shape[0]], w[...], preferred_element_type=F32)
        total = part if total is None else total + part
        row += w.shape[0]
    refs[-1][...] = total.astype(BF16)


def project(h, ws):
    tokens, depth = h.shape
    cols = ws[0].shape[1]
    blk = 512
    return pl.pallas_call(
        project_kernel,
        grid=(tokens // blk,),
        in_specs=[pl.BlockSpec((blk, depth), lambda i: (i, 0))] + [pl.BlockSpec(w.shape, lambda i: (0, 0)) for w in ws],
        out_specs=pl.BlockSpec((blk, cols), lambda i: (i, 0)),
        out_shape=jax.ShapeDtypeStruct((tokens, cols), BF16),
        cost_estimate=pl.CostEstimate(flops=2 * tokens * depth * cols, bytes_accessed=2 * depth * (tokens + cols), transcendentals=0),
        name="project",
    )(h, *ws)


def mix_kernel(plan, n_lhs, n_w, *refs):
    lhs, ws, adds, out_ref = refs[:n_lhs], refs[n_lhs : n_lhs + n_w], refs[n_lhs + n_w : -1], refs[-1]
    total = None
    for l, (w, row) in zip(lhs, plan):
        part = jnp.dot(l[...], ws[w][row : row + l.shape[1], :], preferred_element_type=F32)
        total = part if total is None else total + part
    for t in adds:
        total = total + t[...].astype(F32)
    out_ref[...] = total.astype(out_ref.dtype)


def mix(terms, adds=(), dtype=F32, start=0, tokens=None, col=0, room=0):
    ws, plan = [], []
    for _, w, row in terms:
        found = [i for i, v in enumerate(ws) if v is w]
        if not found:
            ws.append(w)
        plan.append((found[0] if found else len(ws) - 1, row))
    lhs = [t[0] for t in terms]
    tokens = lhs[0].shape[0] if tokens is None else tokens
    cols = ws[0].shape[1]
    blk = 512
    first = start // blk
    tok = lambda w: pl.BlockSpec((blk, w), lambda i: (i + first, 0))
    depth = sum(l.shape[1] for l in lhs)
    add_specs = [pl.BlockSpec((blk, cols), lambda i, f=first * (t.shape[0] != tokens), c=col * (t.shape[1] != cols): (i + f, c)) for t in adds]
    return pl.pallas_call(
        functools.partial(mix_kernel, plan, len(lhs), len(ws)),
        grid=(tokens // blk,),
        in_specs=[tok(l.shape[1]) for l in lhs] + [pl.BlockSpec(w.shape, lambda i: (0, 0)) for w in ws] + add_specs,
        out_specs=pl.BlockSpec((blk, cols), lambda i: (i, 0)),
        out_shape=jax.ShapeDtypeStruct((tokens, cols), dtype),
        cost_estimate=pl.CostEstimate(flops=2 * tokens * depth * cols, bytes_accessed=2 * depth * (tokens + cols), transcendentals=0),
        compiler_params=pltpu.CompilerParams(vmem_limit_bytes=67043328 - room),
        name="mix",
    )(*lhs, *ws, *adds)


BLOCK_ORDER = ["11", "10A", "10B", "01", "00A", "00B"]


def tie(value, *others):
    return lax.optimization_barrier((value, *others))[0]


def solution(mesh):
    def local_layer(hidden, lengths, k_cache, v_cache, ln_gain, w_query, w_key, w_value, w_gate, w_up, w_down, w_out):
        batch, new, width = hidden.shape
        rows_own, _, dim = k_cache.shape
        yi = lax.axis_index("tx")
        ti = lax.axis_index("tyz")
        xi, ci = ti // 2, ti % 2
        half = batch * new // 2
        own_tok = rows_own * new

        g = ln_gain.reshape(1, width)
        g = jnp.concatenate([g, swap_y(g)], 0)
        g = jnp.concatenate([g, swap_x(g)], 0)
        g = jnp.concatenate([g, swap_c(g)], 0)
        offs = []
        for cr in range(2):
            for xr in range(2):
                for yr in range(2):
                    offs.append(width * (4 * yr + 2 * (xr ^ xi) + (cr ^ ci)))
        offs = jnp.stack(offs).astype(jnp.int32)
        half_dim = dim // 2
        inv_freq = ROPE_BASE ** (-2.0 * jnp.arange(half_dim, dtype=F32) / dim)
        positions = (lengths[:, None] + jnp.arange(new, dtype=jnp.int32)[None, :]).reshape(own_tok)
        angles = positions.astype(F32)[:, None] * inv_freq
        cos_t, sin_t = jnp.cos(angles), jnp.sin(angles)
        cos_t = jnp.concatenate([cos_t, cos_t], -1)
        sin_t = jnp.concatenate([-sin_t, sin_t], -1)

        kv_rows = w_key.shape[0] // 4
        w_kv = jnp.concatenate([w_key, w_value], axis=1)
        ordered = lambda pair, i, axis: jnp.where(i == 0, jnp.stack(pair, axis), jnp.stack(pair[::-1], axis))
        kv_part = swap_y(lax.dynamic_slice_in_dim(w_kv, ti * kv_rows, kv_rows, 0))
        kv_pair = ordered([kv_part, swap_x(kv_part)], xi, 0)
        kv_far = ordered([kv_pair, swap_c(kv_pair)], ci, 1).reshape(w_kv.shape)

        hid2 = hidden.reshape(2, half, width)
        other = pick(hid2, 1 - yi)
        mine = pick(tie(hid2, other), yi)
        mine_x = swap_x(mine)
        over = [swap_y(other[i * half // 2 : (i + 1) * half // 2]) for i in range(2)]
        over[0] = tie(over[0], cos_t, sin_t, offs)
        forward = [swap_x(p) for p in over]
        from_y = jnp.concatenate(over, 0)
        far = [swap_c(mine), swap_c(from_y), swap_c(mine_x)]
        from_yx = jnp.concatenate(forward, 0)
        near = [mine, from_y, mine_x, from_yx]
        far.append(swap_c(from_yx))
        h = layer_norm(near + far, g, offs)

        q_far = swap_y(w_query)

        q = project(h, [w_query, q_far])
        h_own = lax.dynamic_slice_in_dim(h, ti * own_tok, own_tok, 0)
        kv = jnp.dot(h_own, jnp.concatenate([w_kv, kv_far], 0), preferred_element_type=F32).astype(BF16)

        q4 = q.reshape(2, 2, own_tok, q.shape[1])
        q_back = swap_x(pick(q4, 1 - xi))

        chunks = 4
        cw = w_gate.shape[1] // chunks
        near_ws = [jnp.stack([w[:, j * cw : (j + 1) * cw] for w in (w_gate, w_up)]) for j in range(chunks)]
        far_ws = [swap_y(w) for w in near_ws]
        a_own = [glu(h, near_ws[0], far_ws[0])]
        q_back = tie(q_back, a_own[0])
        q_x = [pick(q4, xi), q_back]
        q_c = [pick(v, ci) for v in q_x] + [swap_c(pick(v, 1 - ci)) for v in q_x]

        o0, o1, o2, o3, k_next, v_next = attention(lengths, q_c, kv, cos_t, sin_t, k_cache, v_cache)

        keep = [o0, swap_c(o2)]
        send = swap_x(jnp.stack([o1, swap_c(o3)]))
        flip = lambda pair, i: jnp.where(i == 0, jnp.stack(pair), jnp.stack(pair[::-1]))
        o_rows = flip([flip(keep, ci), jnp.where(ci == 0, send, send[::-1])], xi)
        o_own = o_rows.reshape(half, -1)
        o_far = swap_c(o_own)
        o_far = swap_c(o_own)

        for j in range(1, chunks - 1):
            a_own.append(glu(h, near_ws[j], tie(far_ws[j], a_own[-1], o0)))
        a_far = [swap_c(v) for v in a_own]

        def block(xr, cr):
            col = (2 * (xi ^ xr) + (ci ^ cr)) * width
            pair = (w_down, w_out) if xr and cr else (tie(w_down, h), tie(w_out, h))
            return jnp.concatenate([lax.dynamic_slice_in_dim(w, col, width, 1) for w in pair], 0)

        blocks = [[block(xr, cr) for cr in range(2)] for xr in range(2)]
        narrow = width // 2
        other_y = {}
        for name in BLOCK_ORDER:
            b = blocks[int(name[0])][int(name[1])]
            if name[2:]:
                col = "AB".index(name[2]) * narrow
                b = b[:, col : col + narrow]
            other_y[name] = swap_y(b)

        def terms(near_w, far_w, which):
            out = []
            for a_part, o_part, w in ((a_own, o_own, near_w), (a_far, o_far, far_w)):
                if w is not None:
                    out += [(o_part, w, chunks * cw) if k == "o" else (a_part[k], w, k * cw) for k in which]
            return out

        early, late, every = [*range(chunks - 1), "o"], [chunks - 1], [*range(chunks), "o"]
        split = (0, half // 2), (half // 2, half // 2)

        cross_far, same_far = swap_c(blocks[1][1]), swap_c(blocks[0][1])
        pre_cross = mix(terms(blocks[1][0], cross_far, early))
        pre_same = mix(terms(tie(blocks[0][0], pre_cross), same_far, early), [mine])
        a_own.append(glu(h, near_ws[-1], tie(far_ws[-1], pre_same)))
        a_far.append(swap_c(a_own[-1]))
        p_own, r_own = [], []
        for i, span in enumerate(split):
            p_own.append(mix(terms(blocks[1][0], cross_far, late), [pre_cross], F32, *span))
            r_own.append(swap_x(p_own[i]))

        pre_far = mix(terms(None, swap_c(tie(other_y["11"], *p_own)), every))
        r_far = []
        held = pre_far
        for i, side in enumerate("AB"):
            held = mix(terms(tie(other_y["10" + side], held), None, every), [pre_far], col=i)
            r_far.append(swap_x(held))

        def finish_own(i):
            return mix(terms(blocks[0][0], same_far, late), [pre_same, r_own[i]], BF16, *split[i], room=i * 640 * 1024)

        out = jnp.zeros((2, half, width), BF16)
        r_own[0] = tie(r_own[0], held)
        held = finish_own(0)
        out = lax.dynamic_update_slice(out, held[None], (yi, 0, 0))
        base = held = mix(terms(None, swap_c(tie(other_y["01"], held)), every), [from_y])
        out_far = []
        for i, side in enumerate("AB"):
            held = mix(terms(tie(other_y["00" + side], held), None, every), [base, r_far[i]], BF16, col=i)
            out_far.append(swap_y(held))
        r_own[1] = tie(r_own[1], held)
        held = finish_own(1)
        out = lax.dynamic_update_slice(out, out_far[0][None], (1 - yi, 0, 0))
        out = lax.dynamic_update_slice(out, held[None], (yi, split[1][0], 0))
        out = lax.dynamic_update_slice(out, out_far[1][None], (1 - yi, 0, narrow))
        return out.reshape(batch, new, width), k_next, v_next

    row_spec = P("dp", None, ("tx", "tyz"))
    batch_spec = P(("dp", "tx", "tyz"), None, None)
    in_specs = (row_spec, P(("dp", "tx", "tyz")), batch_spec, batch_spec, P(("tx", "tyz")), P("tx", "tyz"), P("tx", None), P("tx", None), P("tx", "tyz"), P("tx", "tyz"), P("tyz", "tx"), P("tyz", "tx"))
    out_specs = (row_spec, batch_spec, batch_spec)

    return jax.shard_map(local_layer, mesh=mesh, in_specs=in_specs, out_specs=out_specs, check_vma=False)
```
